8 devices in a mesh: dp: 2 (over z, y), tp: 4 (over x, core).
Axes of the slice: x: 2, y: 2, z: 1, core: 2. Of those that a mesh axis runs over, the one named last changes fastest.
Arguments:
- hidden: bfloat16 [120, 768], P('dp'), parts along dimension 0
- positions: int32 [120], P('dp'), parts along dimension 0
- self_keys: bfloat16 [2, 120, 448, 12, 64], P(None, 'dp', None, 'tp'), parts along dimension 1
- self_vals: bfloat16 [2, 120, 448, 12, 64], P(None, 'dp', None, 'tp'), parts along dimension 1
- cross_keys: bfloat16 [2, 24, 1500, 12, 64], P(None, 'dp', None, 'tp'), parts along dimension 1
- cross_vals: bfloat16 [2, 24, 1500, 12, 64], P(None, 'dp', None, 'tp'), parts along dimension 1
- ln_gain: bfloat16 [2, 3, 768], replicated
- ln_bias: bfloat16 [2, 3, 768], replicated
- w_query: bfloat16 [2, 768, 768], P(None, None, 'tp')
- b_query: bfloat16 [2, 768], P(None, 'tp')
- w_key: bfloat16 [2, 768, 768], P(None, None, 'tp')
- w_value: bfloat16 [2, 768, 768], P(None, None, 'tp')
- b_value: bfloat16 [2, 768], P(None, 'tp')
- w_out: bfloat16 [2, 768, 768], P(None, 'tp')
- b_out: bfloat16 [2, 768], replicated
- w_cquery: bfloat16 [2, 768, 768], P(None, None, 'tp')
- b_cquery: bfloat16 [2, 768], P(None, 'tp')
- w_cout: bfloat16 [2, 768, 768], P(None, 'tp')
- b_cout: bfloat16 [2, 768], replicated
- w_fc1: bfloat16 [2, 768, 3072], P(None, None, 'tp')
- b_fc1: bfloat16 [2, 3072], P(None, 'tp')
- w_fc2: bfloat16 [2, 3072, 768], P(None, 'tp')
- b_fc2: bfloat16 [2, 768], replicated
Outputs:
- output 1: bfloat16 [120, 768], P('dp'), parts along dimension 0
- output 2: bfloat16 [2, 120, 448, 12, 64], P(None, 'dp', None, 'tp'), parts along dimension 1
- output 3: bfloat16 [2, 120, 448, 12, 64], P(None, 'dp', None, 'tp'), parts along dimension 1
There are 2 independent parts. The reference program is written for one: setup_inputs(seed, part) draws one part's arguments, and reference() takes and returns one part's arrays. A program takes and returns all parts, laid end to end along the dimension named above; an argument that names none is the same for every part.
All inputs are finite; a program needn't handle non-finite values.
Results may differ from the reference program's by a relative error of at most 0.02.
Values are sent between devices in bfloat16 or wider.
A program may use at most 1 GiB of HBM per device.

```python
import jax
import jax.numpy as jnp
from jax import lax

D = 768
HEADS = 12
HEAD = 64
FF = 3072
FRAMES = 1500
CTX = 448
BEAMS = 5
AUDIOS = 12
LAYERS = 2

BATCH = AUDIOS * BEAMS
QK_SCALE = HEAD ** -0.25
EPS = 1e-5


def setup_inputs(seed: int = 0, part: int = 0) -> dict:
    part_keys = jax.random.split(jax.random.fold_in(jax.random.key(seed), part), 6)
    shared_keys = jax.random.split(jax.random.key(seed + 1), 17)

    def draw_array(key, shape, scale, offset=0.0):
        return (offset + scale * jax.random.normal(key, shape, jnp.float32)).astype(jnp.bfloat16)

    audio_pos = jax.random.randint(part_keys[1], (AUDIOS,), 3, CTX - 7)
    positions = jnp.repeat(audio_pos, BEAMS).astype(jnp.int32)
    cache_shape = (LAYERS, BATCH, CTX, HEADS, HEAD)
    cross_shape = (LAYERS, AUDIOS, FRAMES, HEADS, HEAD)
    width_scale = D ** -0.5
    return {
        'hidden': draw_array(part_keys[0], (BATCH, D), 1.0),
        'positions': positions,
        'self_keys': draw_array(part_keys[2], cache_shape, 0.3),
        'self_vals': draw_array(part_keys[3], cache_shape, 1.0),
        'cross_keys': draw_array(part_keys[4], cross_shape, 1.0),
        'cross_vals': draw_array(part_keys[5], cross_shape, 1.0),
        'ln_gain': draw_array(shared_keys[0], (LAYERS, 3, D), 0.3, 1.0),
        'ln_bias': draw_array(shared_keys[1], (LAYERS, 3, D), 0.3),
        'w_query': draw_array(shared_keys[2], (LAYERS, D, D), width_scale),
        'b_query': draw_array(shared_keys[3], (LAYERS, D), 0.3),
        'w_key': draw_array(shared_keys[4], (LAYERS, D, D), 2.0 * width_scale),
        'w_value': draw_array(shared_keys[5], (LAYERS, D, D), width_scale),
        'b_value': draw_array(shared_keys[6], (LAYERS, D), 1.0),
        'w_out': draw_array(shared_keys[7], (LAYERS, D, D), width_scale),
        'b_out': draw_array(shared_keys[8], (LAYERS, D), 0.3),
        'w_cquery': draw_array(shared_keys[9], (LAYERS, D, D), width_scale),
        'b_cquery': draw_array(shared_keys[10], (LAYERS, D), 0.3),
        'w_cout': draw_array(shared_keys[11], (LAYERS, D, D), width_scale),
        'b_cout': draw_array(shared_keys[12], (LAYERS, D), 0.3),
        'w_fc1': draw_array(shared_keys[13], (LAYERS, D, FF), width_scale),
        'b_fc1': draw_array(shared_keys[14], (LAYERS, FF), 0.3),
        'w_fc2': draw_array(shared_keys[15], (LAYERS, FF, D), FF ** -0.5),
        'b_fc2': draw_array(shared_keys[16], (LAYERS, D), 0.3),
    }


def layer_norm(values, gain_row, bias_row):
    wide_vals = values.astype(jnp.float32)
    center = wide_vals - jnp.mean(wide_vals, axis=-1, keepdims=True)
    var_est = jnp.mean(center * center, axis=-1, keepdims=True)
    return (center * lax.rsqrt(var_est + EPS) * gain_row.astype(jnp.float32) + bias_row.astype(jnp.float32)).astype(jnp.bfloat16)


def project(normed, weight, bias_row):
    return jnp.dot(normed, weight, preferred_element_type=jnp.float32) + bias_row.astype(jnp.float32)


def reference(hidden, positions, self_keys, self_vals, cross_keys, cross_vals, ln_gain, ln_bias, w_query, b_query, w_key, w_value, b_value, w_out, b_out, w_cquery, b_cquery, w_cout, b_cout, w_fc1, b_fc1, w_fc2, b_fc2):
    slot_ids = jnp.arange(CTX)[None, :]
    slot_hit = (slot_ids == positions[:, None])[:, :, None, None]
    slot_mask = (slot_ids <= positions[:, None])[:, None, :]

    def one_layer(hidden_in, layer_w):
        normed = layer_norm(hidden_in, layer_w['ln_gain'][0], layer_w['ln_bias'][0])
        query_heads = (project(normed, layer_w['w_query'], layer_w['b_query']) * QK_SCALE).astype(jnp.bfloat16).reshape(BATCH, HEADS, HEAD)
        new_key = (jnp.dot(normed, layer_w['w_key'], preferred_element_type=jnp.float32) * QK_SCALE).astype(jnp.bfloat16).reshape(BATCH, 1, HEADS, HEAD)
        new_val = project(normed, layer_w['w_value'], layer_w['b_value']).astype(jnp.bfloat16).reshape(BATCH, 1, HEADS, HEAD)
        cache_k = jnp.where(slot_hit, new_key, layer_w['cache_k'])
        cache_v = jnp.where(slot_hit, new_val, layer_w['cache_v'])
        raw_scores = jnp.einsum('bhd,bshd->bhs', query_heads.astype(jnp.float32), cache_k.astype(jnp.float32))
        attn_probs = jax.nn.softmax(jnp.where(slot_mask, raw_scores, -1e30), axis=-1).astype(jnp.bfloat16)
        attn_out = jnp.einsum('bhs,bshd->bhd', attn_probs.astype(jnp.float32), cache_v.astype(jnp.float32)).astype(jnp.bfloat16).reshape(BATCH, HEADS * HEAD)
        hidden_mid = (hidden_in.astype(jnp.float32) + project(attn_out, layer_w['w_out'], layer_w['b_out'])).astype(jnp.bfloat16)

        normed = layer_norm(hidden_mid, layer_w['ln_gain'][1], layer_w['ln_bias'][1])
        cross_query = (project(normed, layer_w['w_cquery'], layer_w['b_cquery']) * QK_SCALE).astype(jnp.bfloat16).reshape(AUDIOS, BEAMS, HEADS, HEAD)
        cross_scores = jnp.einsum('abhd,afhd->abhf', cross_query.astype(jnp.float32), layer_w['cross_k'].astype(jnp.float32))
        cross_probs = jax.nn.softmax(cross_scores, axis=-1).astype(jnp.bfloat16)
        cross_out = jnp.einsum('abhf,afhd->abhd', cross_probs.astype(jnp.float32), layer_w['cross_v'].astype(jnp.float32)).astype(jnp.bfloat16).reshape(BATCH, HEADS * HEAD)
        hidden_mid = (hidden_mid.astype(jnp.float32) + project(cross_out, layer_w['w_cout'], layer_w['b_cout'])).astype(jnp.bfloat16)

        normed = layer_norm(hidden_mid, layer_w['ln_gain'][2], layer_w['ln_bias'][2])
        mlp_inner = jax.nn.gelu(project(normed, layer_w['w_fc1'], layer_w['b_fc1']), approximate=False).astype(jnp.bfloat16)
        hidden_next = (hidden_mid.astype(jnp.float32) + project(mlp_inner, layer_w['w_fc2'], layer_w['b_fc2'])).astype(jnp.bfloat16)
        return hidden_next, (cache_k, cache_v)

    layer_stack = {'cache_k': self_keys, 'cache_v': self_vals, 'cross_k': cross_keys, 'cross_v': cross_vals, 'ln_gain': ln_gain, 'ln_bias': ln_bias, 'w_query': w_query, 'b_query': b_query, 'w_key': w_key, 'w_value': w_value, 'b_value': b_value, 'w_out': w_out, 'b_out': b_out, 'w_cquery': w_cquery, 'b_cquery': b_cquery, 'w_cout': w_cout, 'b_cout': b_cout, 'w_fc1': w_fc1, 'b_fc1': b_fc1, 'w_fc2': w_fc2, 'b_fc2': b_fc2}
    hidden_out, cache_pair = lax.scan(one_layer, hidden, layer_stack)
    return hidden_out, cache_pair[0], cache_pair[1]
```

```python
import functools

import jax
import jax.numpy as jnp
from jax import lax
from jax.experimental import pallas as pl
from jax.experimental.pallas import tpu as pltpu
from jax.sharding import PartitionSpec as P

EPS = 1e-5
BF = jnp.bfloat16
F32 = jnp.float32
MESH = pl.DeviceIdType.MESH
ANY = pl.BlockSpec(memory_space=pl.ANY)
VM = pl.BlockSpec(memory_space=pltpu.VMEM)
NT = (((1,), (1,)), ((), ()))
VMEM_LIMIT = 60 * 1024 * 1024


def layer_norm(wide, gain_row, bias_row):
    center = wide - jnp.mean(wide, axis=-1, keepdims=True)
    var_est = jnp.mean(center * center, axis=-1, keepdims=True)
    return (center * lax.rsqrt(var_est + EPS) * gain_row.astype(F32) + bias_row.astype(F32)).astype(BF)


def dot(a, b):
    return jnp.dot(a, b, preferred_element_type=F32)


def dot_nt(a, b):
    return lax.dot_general(a, b, NT, preferred_element_type=F32)


def iota(shape, dim):
    return lax.broadcasted_iota(jnp.int32, shape, dim)


def self_kernel(layer, n_in, beams, *refs):
    h_hbm, pos_ref, g_hbm, b_hbm, wq_hbm, wk_hbm, wv_hbm, bq_hbm, bv_hbm, k_hbm, v_hbm = refs[:11]
    o_ref, ko_hbm, vo_hbm = refs[n_in:n_in + 3]
    h, g, b, wq, wk, wv, bq, bv, kbuf, vbuf, qs, kt, vt, os, psem, ksem, vsem, kosem, vosem = refs[n_in + 3:]
    rows = h.shape[0]
    audios = rows // beams
    slots = kbuf.shape[-1]
    scale = 64 ** -0.25

    small = [(h_hbm, h), (g_hbm, g), (b_hbm, b), (wq_hbm.at[layer], wq), (wk_hbm.at[layer], wk), (wv_hbm.at[layer], wv), (bq_hbm, bq), (bv_hbm, bv)]
    small = [pltpu.make_async_copy(s, d, psem.at[i]) for i, (s, d) in enumerate(small)]
    for c in small:
        c.start()

    def k_in(a):
        r = pl.ds(a * beams, beams)
        return pltpu.make_async_copy(k_hbm.at[layer, r], kbuf.at[r], ksem.at[a])

    def v_in(a):
        r = pl.ds(a * beams, beams)
        return pltpu.make_async_copy(v_hbm.at[layer, r], vbuf.at[r], vsem.at[a])

    def k_out(a):
        r = pl.ds(a * beams, beams)
        return pltpu.make_async_copy(kbuf.at[r], ko_hbm.at[layer, r], kosem.at[a])

    def v_out(a):
        r = pl.ds(a * beams, beams)
        return pltpu.make_async_copy(vbuf.at[r], vo_hbm.at[layer, r], vosem.at[a])

    @pl.loop(0, audios)
    def _(a):
        k_in(a).start()
        v_in(a).start()

    for c in small:
        c.wait()
    normed = layer_norm(h[...].astype(F32), g[layer, 0:1, :], b[layer, 0:1, :])
    q = ((dot_nt(normed, wq[...]) + bq[layer:layer + 1, :].astype(F32)) * scale).astype(BF)
    k = (dot_nt(normed, wk[...]) * scale).astype(BF).astype(F32)
    v = (dot_nt(normed, wv[...]) + bv[layer:layer + 1, :].astype(F32)).astype(BF).astype(F32)
    pad = jnp.zeros((128 - rows, k.shape[1]), F32)
    kt[...] = jnp.concatenate([k, pad], axis=0).T
    vt[...] = jnp.concatenate([v, pad], axis=0).T
    spread = (iota((rows * 8, rows), 0) // 8 == iota((rows * 8, rows), 1)).astype(F32).astype(BF)
    q8 = dot(spread, q)
    own = iota(q8.shape, 1) // 64 == iota(q8.shape, 0) % 8
    qs[...] = jnp.where(own, q8, 0.0)

    width = kbuf.shape[1]
    last = (slots // 128) * 128

    @pl.loop(0, audios)
    def _(a):
        k_in(a).wait()
        v_in(a).wait()
        pos = pos_ref[a * beams]
        tile = pos // 128

        def insert(start, size):
            hit = iota((width, size), 1) == pos - start
            for i in range(beams):
                r = a * beams + i
                pick = jnp.full((width, 128), r, jnp.int32)
                for buf, cols in ((kbuf, kt), (vbuf, vt)):
                    col = jnp.take_along_axis(cols[...], pick, axis=1)[:, :size]
                    old = buf[r, :, pl.ds(start, size)].astype(F32)
                    buf[r, :, pl.ds(start, size)] = jnp.where(hit, col, old).astype(BF)

        @pl.when(tile * 128 < last)
        def _():
            insert(pl.multiple_of(tile * 128, 128), 128)

        if slots > last:
            @pl.when(tile * 128 >= last)
            def _():
                insert(last, slots - last)

        k_out(a).start()
        v_out(a).start()
        scores = []
        for i in range(beams):
            r = a * beams + i
            scores.append(dot(qs[pl.ds(pl.multiple_of(r * 8, 8), 8), :].astype(BF), kbuf[r]))
        scores = jnp.concatenate(scores, axis=0)
        scores = jnp.where(iota(scores.shape, 1) <= pos, scores, -1e30)
        e = jnp.exp(scores - jnp.max(scores, axis=-1, keepdims=True))
        probs = (e * (1.0 / jnp.sum(e, axis=-1, keepdims=True))).astype(F32)
        for i in range(beams):
            r = a * beams + i
            out = dot_nt(probs[i * 8:i * 8 + 8].astype(BF), vbuf[r])
            mine = iota(out.shape, 1) // 64 == iota(out.shape, 0)
            os[pl.ds(r, 1), :] = jnp.sum(jnp.where(mine, out, 0.0), axis=0, keepdims=True)

    o_ref[...] = os[...].astype(BF)

    @pl.loop(0, audios)
    def _(a):
        k_out(a).wait()
        v_out(a).wait()


def self_call(layer, beams, h, pos, g, b, wq, wk, wv, bq, bv, k, v, outs):
    rows = h.shape[0]
    audios = rows // beams
    _, _, width, slots = k.shape
    args = (h, pos, g, b, wq, wk, wv, bq, bv, k, v) + outs
    n_in = len(args)
    return pl.pallas_call(
        functools.partial(self_kernel, layer, n_in, beams),
        out_shape=(jax.ShapeDtypeStruct((rows, width), BF), jax.ShapeDtypeStruct(k.shape, BF), jax.ShapeDtypeStruct(v.shape, BF)),
        in_specs=[ANY, pl.BlockSpec(memory_space=pltpu.SMEM)] + [ANY] * (n_in - 2),
        out_specs=(VM, ANY, ANY),
        input_output_aliases={11: 1, 12: 2} if outs else {},
        scratch_shapes=[
            pltpu.VMEM(h.shape, BF), pltpu.VMEM(g.shape, BF), pltpu.VMEM(b.shape, BF),
            pltpu.VMEM(wq.shape[1:], BF), pltpu.VMEM(wk.shape[1:], BF), pltpu.VMEM(wv.shape[1:], BF),
            pltpu.VMEM(bq.shape, BF), pltpu.VMEM(bv.shape, BF),
            pltpu.VMEM((rows, width, slots), BF), pltpu.VMEM((rows, width, slots), BF),
            pltpu.VMEM((rows * 8, width), F32), pltpu.VMEM((width, 128), F32), pltpu.VMEM((width, 128), F32), pltpu.VMEM((rows, width), F32),
            pltpu.SemaphoreType.DMA((8,)), pltpu.SemaphoreType.DMA((audios,)), pltpu.SemaphoreType.DMA((audios,)),
            pltpu.SemaphoreType.DMA((audios,)), pltpu.SemaphoreType.DMA((audios,)),
        ],
        compiler_params=pltpu.CompilerParams(vmem_limit_bytes=VMEM_LIMIT),
        name=f"self_{layer}",
    )(*args)


def rest_kernel(layer, beams, o_hbm, h_hbm, g_hbm, b_hbm, wo_hbm, bo_hbm, wc_hbm, bc_hbm, wco_hbm, bco_hbm, w1_hbm, b1_hbm, w2_hbm, b2_hbm, k_hbm, v_hbm, out_ref,
                o, h, g, b, wo, bo, wc, bc, wco, bco, w1, b1, w2, b2, kbuf, vbuf, qpad, opad, near, near_in, far, far_in, psem, ksem, vsem, near_s, near_r, far_s, far_r):
    rows = h.shape[0]
    audios = rows // beams
    width = o.shape[1]
    scale = 64 ** -0.25
    dp = lax.axis_index('dp')
    me = lax.axis_index('tp')
    core = me % 2
    mate = me + 1 - 2 * core
    others = ((me + 2) % 4, (mate + 2) % 4)

    small = [(o_hbm, o), (h_hbm, h), (g_hbm, g), (b_hbm, b), (wo_hbm.at[layer], wo), (bo_hbm, bo), (wc_hbm.at[layer], wc), (bc_hbm, bc),
             (wco_hbm.at[layer], wco), (bco_hbm, bco), (w1_hbm.at[layer], w1), (b1_hbm, b1), (w2_hbm.at[layer], w2), (b2_hbm, b2)]
    small = [pltpu.make_async_copy(s, d, psem.at[i]) for i, (s, d) in enumerate(small)]
    for c in small[:8]:
        c.start()

    def k_in(a):
        return pltpu.make_async_copy(k_hbm.at[layer, a], kbuf.at[a], ksem.at[a])

    def v_in(a):
        return pltpu.make_async_copy(v_hbm.at[layer, a], vbuf.at[a], vsem.at[a])

    @pl.loop(0, audios)
    def _(a):
        k_in(a).start()
        v_in(a).start()

    for c in small[8:]:
        c.start()
    barrier = pltpu.get_barrier_semaphore()
    for peer in (mate,) + others:
        pl.semaphore_signal(barrier, inc=1, device_id=(dp, peer), device_id_type=MESH)
    pl.semaphore_wait(barrier, 3)

    half = h.shape[1] // 2

    def all_sum(step, part):
        near[step] = part.astype(BF)
        c = pltpu.make_async_remote_copy(near.at[step], near_in.at[step], near_s.at[step], near_r.at[step], device_id=(dp, mate), device_id_type=MESH)
        c.start()
        c.wait()
        chip = (near[step].astype(F32) + near_in[step].astype(F32)).astype(BF)
        far[step, 0] = chip[:, :half]
        far[step, 1] = chip[:, half:]
        sends = [pltpu.make_async_remote_copy(far.at[step, core], far_in.at[step, core], far_s.at[step, j], far_r.at[step, core], device_id=(dp, others[j]), device_id_type=MESH) for j in range(2)]
        for c in sends:
            c.start()
        for j in range(2):
            pltpu.make_async_remote_copy(far.at[step, j], far_in.at[step, j], far_s.at[step, j], far_r.at[step, j], device_id=(dp, others[j]), device_id_type=MESH).wait_recv()
        for c in sends:
            c.wait_send()
        return chip.astype(F32) + jnp.concatenate([far_in[step, 0], far_in[step, 1]], axis=1).astype(F32)

    for c in small[:8]:
        c.wait()
    total = all_sum(0, dot(o[...], wo[...]))
    hid = (h[...].astype(F32) + total + bo[layer:layer + 1, :].astype(F32)).astype(BF)
    normed = layer_norm(hid.astype(F32), g[layer, 1:2, :], b[layer, 1:2, :])
    q = ((dot_nt(normed, wc[...]) + bc[layer:layer + 1, :].astype(F32)) * scale).astype(BF)
    r_pad, r_row = iota((audios * 8, rows), 0), iota((audios * 8, rows), 1)
    spread = ((r_pad // 8 == r_row // beams) & (r_pad % 8 == r_row % beams)).astype(F32).astype(BF)
    qpad[...] = dot(spread, q)

    @pl.loop(0, audios)
    def _(a):
        k_in(a).wait()
        v_in(a).wait()
        r = pl.ds(pl.multiple_of(a * 8, 8), 8)
        qa = qpad[r, :]
        qa = jnp.concatenate([qa] * (width // 64), axis=0)
        own = iota(qa.shape, 1) // 64 == iota(qa.shape, 0) // 8
        scores = dot(jnp.where(own, qa, 0.0).astype(BF), kbuf[a])
        e = jnp.exp(scores - jnp.max(scores, axis=-1, keepdims=True))
        probs = (e * (1.0 / jnp.sum(e, axis=-1, keepdims=True))).astype(BF)
        out = jnp.where(own, dot_nt(probs, vbuf[a]), 0.0)
        acc = out[0:8]
        for j in range(1, width // 64):
            acc = acc + out[j * 8:j * 8 + 8]
        opad[r, :] = acc

    for c in small[8:]:
        c.wait()
    c_pad, c_row = iota((rows, audios * 8), 1), iota((rows, audios * 8), 0)
    gather = ((c_pad // 8 == c_row // beams) & (c_pad % 8 == c_row % beams)).astype(F32).astype(BF)
    cross = dot(gather, opad[...].astype(BF)).astype(BF)
    total = all_sum(1, dot(cross, wco[...]))
    hid = (hid.astype(F32) + total + bco[layer:layer + 1, :].astype(F32)).astype(BF)
    normed = layer_norm(hid.astype(F32), g[layer, 2:3, :], b[layer, 2:3, :])
    inner = dot(normed, w1[...]) + b1[layer:layer + 1, :].astype(F32)
    inner = (0.5 * inner * (1.0 + lax.erf(inner * (2.0 ** -0.5)))).astype(BF)
    total = all_sum(2, dot(inner, w2[...]))
    out_ref[...] = (hid.astype(F32) + total + b2[layer:layer + 1, :].astype(F32)).astype(BF)


def rest_call(layer, beams, o, h, g, b, wo, bo, wc, bc, wco, bco, w1, b1, w2, b2, k, v):
    rows, dim = h.shape
    _, audios, width, frames = k.shape
    args = (o, h, g, b, wo, bo, wc, bc, wco, bco, w1, b1, w2, b2, k, v)
    return pl.pallas_call(
        functools.partial(rest_kernel, layer, beams),
        out_shape=jax.ShapeDtypeStruct(h.shape, BF),
        in_specs=[ANY] * len(args),
        out_specs=VM,
        scratch_shapes=[
            pltpu.VMEM(o.shape, BF), pltpu.VMEM(h.shape, BF), pltpu.VMEM(g.shape, BF), pltpu.VMEM(b.shape, BF),
            pltpu.VMEM(wo.shape[1:], BF), pltpu.VMEM(bo.shape, BF), pltpu.VMEM(wc.shape[1:], BF), pltpu.VMEM(bc.shape, BF),
            pltpu.VMEM(wco.shape[1:], BF), pltpu.VMEM(bco.shape, BF), pltpu.VMEM(w1.shape[1:], BF), pltpu.VMEM(b1.shape, BF),
            pltpu.VMEM(w2.shape[1:], BF), pltpu.VMEM(b2.shape, BF),
            pltpu.VMEM((audios, width, frames), BF), pltpu.VMEM((audios, width, frames), BF),
            pltpu.VMEM((audios * 8, width), F32), pltpu.VMEM((audios * 8, width), F32),
            pltpu.VMEM((3, rows, dim), BF), pltpu.VMEM((3, rows, dim), BF),
            pltpu.VMEM((3, 2, rows, dim // 2), BF), pltpu.VMEM((3, 2, rows, dim // 2), BF),
            pltpu.SemaphoreType.DMA((14,)), pltpu.SemaphoreType.DMA((audios,)), pltpu.SemaphoreType.DMA((audios,)),
            pltpu.SemaphoreType.DMA((3,)), pltpu.SemaphoreType.DMA((3,)), pltpu.SemaphoreType.DMA((3, 2)), pltpu.SemaphoreType.DMA((3, 2)),
        ],
        compiler_params=pltpu.CompilerParams(collective_id=layer, has_side_effects=True, vmem_limit_bytes=VMEM_LIMIT),
        name=f"rest_{layer}",
    )(*args)


def solution(mesh):
    cache_spec = P(None, 'dp', None, 'tp', None)
    col_spec = P(None, None, 'tp')
    row_spec = P(None, 'tp', None)
    vec_spec = P(None, 'tp')
    in_specs = (P('dp', None), P('dp'), cache_spec, cache_spec, cache_spec, cache_spec,
                P(), P(), col_spec, vec_spec, col_spec, col_spec, vec_spec, row_spec, P(), col_spec, vec_spec, row_spec, P(), col_spec, vec_spec, row_spec, P())

    def heads_first(cache):
        cache = jnp.transpose(cache, (0, 1, 3, 4, 2))
        return cache.reshape(cache.shape[:2] + (-1, cache.shape[-1]))

    def heads_last(cache, like):
        layers, batch, slots, heads, dim = like.shape
        return jnp.transpose(cache.reshape(layers, batch, heads, dim, slots), (0, 1, 4, 2, 3))

    def local_step(hidden, positions, self_keys, self_vals, cross_keys, cross_vals, g, b, wq, bq, wk, wv, bv, wo, bo, wc, bc, wco, bco, w1, b1, w2, b2):
        beams = hidden.shape[0] // cross_keys.shape[1]
        sk, sv, ck, cv = (heads_first(x) for x in (self_keys, self_vals, cross_keys, cross_vals))
        wq, wk, wv, wc = (jnp.swapaxes(w, 1, 2) for w in (wq, wk, wv, wc))
        outs = ()
        for layer in range(sk.shape[0]):
            o, *outs = self_call(layer, beams, hidden, positions, g, b, wq, wk, wv, bq, bv, sk, sv, tuple(outs))
            hidden = rest_call(layer, beams, o, hidden, g, b, wo, bo, wc, bc, wco, bco, w1, b1, w2, b2, ck, cv)
        return hidden, heads_last(outs[0], self_keys), heads_last(outs[1], self_vals)

    return jax.shard_map(local_step, mesh=mesh, in_specs=in_specs, out_specs=(P('dp', None), cache_spec, cache_spec), check_vma=False)
```

```python
import functools

import jax
import jax.numpy as jnp
from jax import lax
from jax.experimental import pallas as pl
from jax.experimental.pallas import tpu as pltpu
from jax.sharding import PartitionSpec as P

EPS = 1e-5
BF = jnp.bfloat16
F32 = jnp.float32
MESH = pl.DeviceIdType.MESH
ANY = pl.BlockSpec(memory_space=pl.ANY)
VM = pl.BlockSpec(memory_space=pltpu.VMEM)
SMEM = pl.BlockSpec(memory_space=pltpu.SMEM)
DMA = pltpu.SemaphoreType.DMA
NT = (((1,), (1,)), ((), ()))
VMEM_LIMIT = 60 * 1024 * 1024
REST_LIMIT = 38 * 1024 * 1024


def layer_norm(wide, gain_row, bias_row):
    center = wide - jnp.mean(wide, axis=-1, keepdims=True)
    var_est = jnp.mean(center * center, axis=-1, keepdims=True)
    return (center * lax.rsqrt(var_est + EPS) * gain_row.astype(F32) + bias_row.astype(F32)).astype(BF)


def dot(a, b):
    return jnp.dot(a, b, preferred_element_type=F32)


def dot_nt(a, b):
    return lax.dot_general(a, b, NT, preferred_element_type=F32)


def iota(shape, dim):
    return lax.broadcasted_iota(jnp.int32, shape, dim)


def column_insert(buf, lead, cols, row, pos, slots):
    width = cols.shape[0]
    last = (slots // 128) * 128
    tile = pos // 128

    def insert(start, size):
        hit = iota((width, size), 1) == pos - start
        col = jnp.take_along_axis(cols[...], jnp.full((width, 128), row, jnp.int32), axis=1)[:, :size]
        old = buf[lead + (slice(None), pl.ds(start, size))].astype(F32)
        buf[lead + (slice(None), pl.ds(start, size))] = jnp.where(hit, col, old).astype(BF)

    @pl.when(tile * 128 < last)
    def _():
        insert(pl.multiple_of(tile * 128, 128), 128)

    if slots > last:
        @pl.when(tile * 128 >= last)
        def _():
            insert(last, slots - last)


def as_columns(rows):
    pad = jnp.zeros((128 - rows.shape[0], rows.shape[1]), F32)
    return jnp.concatenate([rows, pad], axis=0).T


def copies(pairs, sem):
    return [pltpu.make_async_copy(s, d, sem.at[i]) for i, (s, d) in enumerate(pairs)]


def self_kernel(layer, beams, h_hbm, pos_ref, g_hbm, b_hbm, wq_hbm, wk_hbm, wv_hbm, bq_hbm, bv_hbm, k_hbm, v_hbm, o_ref, ko_hbm, vo_hbm,
                h, g, b, wq, wk, wv, bq, bv, kbuf, vbuf, qs, kt, vt, os, psem, ksem, vsem, kosem, vosem):
    rows = h.shape[0]
    audios = rows // beams
    slots = kbuf.shape[-1]
    scale = 64 ** -0.25

    small = copies([(h_hbm, h), (g_hbm, g), (b_hbm, b), (wq_hbm.at[layer], wq), (wk_hbm.at[layer], wk), (wv_hbm.at[layer], wv), (bq_hbm, bq), (bv_hbm, bv)], psem)
    for c in small:
        c.start()

    def block(a, src, dst, sem):
        return pltpu.make_async_copy(src, dst, sem.at[a])

    def at(a):
        return pl.ds(a * beams, beams)

    def k_in(a):
        return block(a, k_hbm.at[layer, at(a)], kbuf.at[at(a)], ksem)

    def v_in(a):
        return block(a, v_hbm.at[layer, at(a)], vbuf.at[at(a)], vsem)

    def k_out(a):
        return block(a, kbuf.at[at(a)], ko_hbm.at[layer, at(a)], kosem)

    def v_out(a):
        return block(a, vbuf.at[at(a)], vo_hbm.at[layer, at(a)], vosem)

    @pl.loop(0, audios)
    def _(a):
        k_in(a).start()
        v_in(a).start()

    for c in small:
        c.wait()
    normed = layer_norm(h[...].astype(F32), g[layer, 0:1, :], b[layer, 0:1, :])
    q = ((dot_nt(normed, wq[...]) + bq[layer:layer + 1, :].astype(F32)) * scale).astype(BF)
    kt[...] = as_columns((dot_nt(normed, wk[...]) * scale).astype(BF).astype(F32))
    vt[...] = as_columns((dot_nt(normed, wv[...]) + bv[layer:layer + 1, :].astype(F32)).astype(BF).astype(F32))
    spread = (iota((rows * 8, rows), 0) // 8 == iota((rows * 8, rows), 1)).astype(F32).astype(BF)
    q8 = dot(spread, q)
    qs[...] = jnp.where(iota(q8.shape, 1) // 64 == iota(q8.shape, 0) % 8, q8, 0.0)

    @pl.loop(0, audios // 2)
    def _(pair):
        group = (pair * 2, pair * 2 + 1)
        for a in group:
            k_in(a).wait()
            v_in(a).wait()
            for i in range(beams):
                r = a * beams + i
                column_insert(kbuf, (r,), kt, r, pos_ref[a * beams], slots)
                column_insert(vbuf, (r,), vt, r, pos_ref[a * beams], slots)
            k_out(a).start()
            v_out(a).start()
        probs = []
        for a in group:
            scores = []
            for i in range(beams):
                r = a * beams + i
                scores.append(dot(qs[pl.ds(pl.multiple_of(r * 8, 8), 8), :].astype(BF), kbuf[r]))
            scores = jnp.concatenate(scores, axis=0)
            scores = jnp.where(iota(scores.shape, 1) <= pos_ref[a * beams], scores, -1e30)
            e = jnp.exp(scores - jnp.max(scores, axis=-1, keepdims=True))
            probs.append(e * (1.0 / jnp.sum(e, axis=-1, keepdims=True)))
        for a, p in zip(group, probs):
            for i in range(beams):
                r = a * beams + i
                out = dot_nt(p[i * 8:i * 8 + 8].astype(BF), vbuf[r])
                mine = iota(out.shape, 1) // 64 == iota(out.shape, 0)
                os[pl.ds(r, 1), :] = jnp.sum(jnp.where(mine, out, 0.0), axis=0, keepdims=True)

    o_ref[...] = os[...].astype(BF)

    @pl.loop(0, audios)
    def _(a):
        k_out(a).wait()
        v_out(a).wait()


def self_call(layer, beams, h, pos, g, b, wq, wk, wv, bq, bv, k, v):
    rows = h.shape[0]
    audios = rows // beams
    _, _, width, slots = k.shape
    args = (h, pos, g, b, wq, wk, wv, bq, bv, k, v)
    return pl.pallas_call(
        functools.partial(self_kernel, layer, beams),
        out_shape=(jax.ShapeDtypeStruct((rows, width), BF), jax.ShapeDtypeStruct(k.shape, BF), jax.ShapeDtypeStruct(v.shape, BF)),
        in_specs=[ANY, SMEM] + [ANY] * 9,
        out_specs=(VM, ANY, ANY),
        scratch_shapes=[
            pltpu.VMEM(h.shape, BF), pltpu.VMEM(g.shape, BF), pltpu.VMEM(b.shape, BF),
            pltpu.VMEM(wq.shape[1:], BF), pltpu.VMEM(wk.shape[1:], BF), pltpu.VMEM(wv.shape[1:], BF),
            pltpu.VMEM(bq.shape, BF), pltpu.VMEM(bv.shape, BF),
            pltpu.VMEM((rows, width, slots), BF), pltpu.VMEM((rows, width, slots), BF),
            pltpu.VMEM((rows * 8, width), F32), pltpu.VMEM((width, 128), F32), pltpu.VMEM((width, 128), F32), pltpu.VMEM((rows, width), F32),
            DMA((8,)), DMA((audios,)), DMA((audios,)), DMA((audios,)), DMA((audios,)),
        ],
        compiler_params=pltpu.CompilerParams(vmem_limit_bytes=VMEM_LIMIT),
        name=f"self_{layer}",
    )(*args)


def rest_kernel(beams, parts, o_hbm, h_hbm, pos_ref, g_hbm, b_hbm, wq_hbm, bq_hbm, wk_hbm, wv_hbm, bv_hbm, wo_hbm, bo_hbm, wc_hbm, bc_hbm, wco_hbm, bco_hbm, w1_hbm, b1_hbm, w2_hbm, b2_hbm,
                sk_hbm, sv_hbm, ck_hbm, cv_hbm, out_ref, sk, sv, kn_ref, vn_ref,
                o, h, g, b, wq, bq, wk, wv, bv, wo, bo, wc, bc, wco, bco, w1, b1, w2, b2, ck, cv, hid, qc, oc, qs, vs, sn, os, snd, rcv,
                psem, wsem, skem, svem, ckem, cvem, ssem, rsem):
    rows = h.shape[0]
    audios = rows // beams
    group = audios // parts
    prow = rows // parts
    width = o.shape[1]
    heads = width // 64
    scale = 64 ** -0.25
    dp = lax.axis_index('dp')
    me = lax.axis_index('tp')
    mate = me + 1 - 2 * (me % 2)
    peers = ((me + 2) % 4, (mate + 2) % 4, mate)

    small = copies([(o_hbm, o), (h_hbm, h), (g_hbm, g), (b_hbm, b), (bq_hbm, bq), (bv_hbm, bv), (bo_hbm, bo), (bc_hbm, bc), (bco_hbm, bco), (b1_hbm, b1), (b2_hbm, b2)], psem)
    first = copies([(x.at[0], y.at[0]) for x, y in ((wo_hbm, wo), (wc_hbm, wc), (wco_hbm, wco), (w1_hbm, w1), (w2_hbm, w2))], wsem.at[0])
    second = copies([(x.at[1], y.at[1]) for x, y in ((wo_hbm, wo), (wc_hbm, wc), (wco_hbm, wco), (w1_hbm, w1), (w2_hbm, w2))]
                    + [(x.at[1], y) for x, y in ((wq_hbm, wq), (wk_hbm, wk), (wv_hbm, wv))], wsem.at[1])

    def cross_in(layer, a):
        return pltpu.make_async_copy(ck_hbm.at[layer, a], ck.at[a], ckem.at[a]), pltpu.make_async_copy(cv_hbm.at[layer, a], cv.at[a], cvem.at[a])

    def self_in(a):
        r = pl.ds(a * beams, beams)
        return pltpu.make_async_copy(sk_hbm.at[1, r], sk.at[r], skem.at[a]), pltpu.make_async_copy(sv_hbm.at[1, r], sv.at[r], svem.at[a])

    def start(pair):
        for c in pair:
            c.start()

    def wait(pair):
        for c in pair:
            c.wait()

    start(small)
    start(first[:2])

    @pl.loop(0, audios)
    def _(a):
        start(cross_in(0, a))

    start(first[2:])
    barrier = pltpu.get_barrier_semaphore()
    for peer in peers:
        pl.semaphore_signal(barrier, inc=1, device_id=(dp, peer), device_id_type=MESH)

    start(second)

    @pl.loop(0, audios)
    def _(a):
        start(self_in(a))

    pl.semaphore_wait(barrier, 3)

    def sends(step, m):
        return [pltpu.make_async_remote_copy(snd.at[step, m], rcv.at[step, m, j], ssem.at[step, m, j], rsem.at[step, m, j], device_id=(dp, peer), device_id_type=MESH) for j, peer in enumerate(peers)]

    def push(step, m, part):
        snd[step, m] = part.astype(BF)
        start(sends(step, m))

    def total(step, m):
        wait(sends(step, m))
        mine = snd[step, m].astype(F32) + rcv[step, m, 2].astype(F32)
        return mine + (rcv[step, m, 0].astype(F32) + rcv[step, m, 1].astype(F32))

    def settle(step, m, bias):
        new = (hid[m].astype(F32) + total(step, m) + bias.astype(F32)).astype(BF)
        hid[m] = new
        return new.astype(F32)

    def flags(shape, rule):
        return rule(iota(shape, 0), iota(shape, 1)).astype(F32).astype(BF)

    def pick(m):
        return flags((prow, rows), lambda r, c: c == r + m * prow)

    def cross_half(layer, m, wide):
        normed = layer_norm(wide, g[layer, 1:2, :], b[layer, 1:2, :])
        q = ((dot_nt(normed, wc[layer]) + bc[layer:layer + 1, :].astype(F32)) * scale).astype(BF)
        qc[m] = dot(flags((group * 8, prow), lambda r, c: (r // 8 == c // beams) & (r % 8 == c % beams)), q)

        @pl.loop(0, group // 2)
        def _(i):
            probs = []
            local = (i * 2, i * 2 + 1)
            for n in local:
                a = m * group + n
                wait(cross_in(layer, a))
                qa = qc[m, pl.ds(pl.multiple_of(n * 8, 8), 8), :]
                qa = jnp.concatenate([qa] * heads, axis=0)
                own = iota(qa.shape, 1) // 64 == iota(qa.shape, 0) // 8
                scores = dot(jnp.where(own, qa, 0.0).astype(BF), ck[a])
                e = jnp.exp(scores - jnp.max(scores, axis=-1, keepdims=True))
                probs.append((e * (1.0 / jnp.sum(e, axis=-1, keepdims=True))).astype(BF))
            for n, p in zip(local, probs):
                out = dot_nt(p, cv[m * group + n])
                own = iota(out.shape, 1) // 64 == iota(out.shape, 0) // 8
                out = jnp.where(own, out, 0.0)
                acc = out[0:8]
                for j in range(1, heads):
                    acc = acc + out[j * 8:j * 8 + 8]
                oc[m, pl.ds(pl.multiple_of(n * 8, 8), 8), :] = acc

        if layer == 0:
            @pl.loop(0, group)
            def _(n):
                start(cross_in(1, m * group + n))
        cross = dot(flags((prow, group * 8), lambda r, c: (c // 8 == r // beams) & (c % 8 == r % beams)), oc[m].astype(BF)).astype(BF)
        return dot(cross, wco[layer])

    def mlp_half(layer, m, wide):
        normed = layer_norm(wide, g[layer, 2:3, :], b[layer, 2:3, :])
        inner = dot(normed, w1[layer]) + b1[layer:layer + 1, :].astype(F32)
        inner = (0.5 * inner * (1.0 + lax.erf(inner * (2.0 ** -0.5)))).astype(BF)
        return dot(inner, w2[layer])

    def self_half(m, wide):
        normed = layer_norm(wide, g[1, 0:1, :], b[1, 0:1, :])
        q = ((dot_nt(normed, wq[...]) + bq[1:2, :].astype(F32)) * scale).astype(BF)
        k = (dot_nt(normed, wk[...]) * scale).astype(BF)
        v = (dot_nt(normed, wv[...]) + bv[1:2, :].astype(F32)).astype(BF)
        kn_ref[m] = k
        vn_ref[m] = v
        spread = flags((prow * 8, prow), lambda r, c: r // 8 == c)
        q8 = dot(spread, q)
        own = iota(q8.shape, 1) // 64 == iota(q8.shape, 0) % 8
        q8 = jnp.where(own, q8, 0.0)
        qs[m] = q8
        vs[m] = jnp.where(own, dot(spread, v), 0.0)
        sn[m] = jnp.broadcast_to(jnp.sum(q8 * dot(spread, k), axis=-1, keepdims=True), sn.shape[1:])

        @pl.loop(0, group // 2)
        def _(i):
            local = (i * 2, i * 2 + 1)
            probs, news = [], []
            for n in local:
                a = m * group + n
                wait(self_in(a))
                pos = pos_ref[a * beams]
                scores = []
                for j in range(beams):
                    row = pl.ds(pl.multiple_of((n * beams + j) * 8, 8), 8)
                    scores.append(dot(qs[m, row, :].astype(BF), sk[a * beams + j]))
                scores = jnp.concatenate(scores, axis=0)
                fresh = sn[m, pl.ds(pl.multiple_of(n * beams * 8, 8), beams * 8), 0:1]
                slot = iota(scores.shape, 1)
                scores = jnp.where(slot < pos, scores, -1e30)
                top = jnp.maximum(jnp.max(scores, axis=-1, keepdims=True), fresh)
                e = jnp.where(slot < pos, jnp.exp(scores - top), 0.0)
                e_new = jnp.exp(fresh - top)
                inv = 1.0 / (jnp.sum(e, axis=-1, keepdims=True) + e_new)
                probs.append(e * inv)
                news.append((e_new * inv).astype(BF).astype(F32))
            for n, p, p_new in zip(local, probs, news):
                a = m * group + n
                for j in range(beams):
                    row = pl.ds(pl.multiple_of((n * beams + j) * 8, 8), 8)
                    out = dot_nt(p[j * 8:j * 8 + 8].astype(BF), sv[a * beams + j])
                    mine = iota(out.shape, 1) // 64 == iota(out.shape, 0)
                    out = jnp.where(mine, out, 0.0) + p_new[j * 8:j * 8 + 8] * vs[m, row, :]
                    os[m, pl.ds(n * beams + j, 1), :] = jnp.sum(out, axis=0, keepdims=True)

        return dot(os[m].astype(BF), wo[1])

    wait(small)
    wait(first[:1])
    for m in range(parts):
        push(0, m, dot(dot(pick(m), o[...]).astype(BF), wo[0]))
        hid[m] = dot(pick(m), h[...]).astype(BF)
    wait(first[1:3])
    for m in range(parts):
        push(1, m, cross_half(0, m, settle(0, m, bo[0:1, :])))
        if m == 0:
            wait(first[3:])
    for m in range(parts):
        push(2, m, mlp_half(0, m, settle(1, m, bco[0:1, :])))
    wait(second)
    for m in range(parts):
        push(3, m, self_half(m, settle(2, m, b2[0:1, :])))
    for m in range(parts):
        push(4, m, cross_half(1, m, settle(3, m, bo[1:2, :])))
    for m in range(parts):
        push(5, m, mlp_half(1, m, settle(4, m, bco[1:2, :])))
    result = jnp.zeros((rows, h.shape[1]), F32)
    for m in range(parts):
        place = flags((rows, prow), lambda r, c: r == c + m * prow)
        result = result + dot(place, settle(5, m, b2[1:2, :]).astype(BF))
    out_ref[...] = result.astype(BF)


def rest_call(beams, parts, o, h, pos, g, b, wq, bq, wk, wv, bv, wo, bo, wc, bc, wco, bco, w1, b1, w2, b2, sk, sv, ck, cv):
    rows, dim = h.shape
    _, audios, width, frames = ck.shape
    slots = sk.shape[-1]
    prow = rows // parts
    prows8 = prow * 8
    args = (o, h, pos, g, b, wq, bq, wk, wv, bv, wo, bo, wc, bc, wco, bco, w1, b1, w2, b2, sk, sv, ck, cv)

    def whole(x):
        return pltpu.VMEM(x.shape, BF)

    def one(x):
        return pltpu.VMEM(x.shape[1:], BF)

    return pl.pallas_call(
        functools.partial(rest_kernel, beams, parts),
        out_shape=(pltpu.VMEM(h.shape, BF), pltpu.VMEM((rows, width, slots), BF), pltpu.VMEM((rows, width, slots), BF), pltpu.VMEM((parts, prow, width), BF), pltpu.VMEM((parts, prow, width), BF)),
        in_specs=[ANY, ANY, SMEM] + [ANY] * (len(args) - 3),
        out_specs=(VM,) * 5,
        scratch_shapes=[
            whole(o), whole(h), whole(g), whole(b), one(wq), whole(bq), one(wk), one(wv), whole(bv), whole(wo), whole(bo), whole(wc), whole(bc),
            whole(wco), whole(bco), whole(w1), whole(b1), whole(w2), whole(b2), one(ck), one(cv),
            pltpu.VMEM((parts, prow, dim), BF),
            pltpu.VMEM((parts, audios // parts * 8, width), F32), pltpu.VMEM((parts, audios // parts * 8, width), F32),
            pltpu.VMEM((parts, prows8, width), F32), pltpu.VMEM((parts, prows8, width), F32), pltpu.VMEM((parts, prows8, 128), F32), pltpu.VMEM((parts, prow, width), F32),
            pltpu.VMEM((6, parts, prow, dim), BF), pltpu.VMEM((6, parts, 3, prow, dim), BF),
            DMA((11,)), DMA((2, 8)), DMA((audios,)), DMA((audios,)), DMA((audios,)), DMA((audios,)), DMA((6, parts, 3)), DMA((6, parts, 3)),
        ],
        compiler_params=pltpu.CompilerParams(collective_id=0, has_side_effects=True, vmem_limit_bytes=REST_LIMIT),
        name="rest",
    )(*args)


def write_kernel(layer, beams, ring, hid, pos_ref, kn, vn, sk, sv, ki_hbm, vi_hbm, out_ref, ko_hbm, vo_hbm, kst, vst, kt, vt, kosem, vosem):
    parts, prow, width = kn.shape
    rows = parts * prow
    audios = rows // beams
    slots = sk.shape[-1]

    def k_out(a, s):
        return pltpu.make_async_copy(kst.at[s], ko_hbm.at[layer, pl.ds(a * beams, beams)], kosem.at[s])

    def v_out(a, s):
        return pltpu.make_async_copy(vst.at[s], vo_hbm.at[layer, pl.ds(a * beams, beams)], vosem.at[s])

    def columns(new):
        both = jnp.zeros((rows, width), F32)
        for m in range(parts):
            place = (iota((rows, prow), 0) == iota((rows, prow), 1) + m * prow).astype(F32).astype(BF)
            both = both + dot(place, new[m])
        return as_columns(both)

    kt[...] = columns(kn)
    vt[...] = columns(vn)
    out_ref[...] = hid[...]

    @pl.loop(0, audios)
    def _(a):
        s = lax.rem(a, ring)

        @pl.when(a >= ring)
        def _():
            k_out(a - ring, s).wait()
            v_out(a - ring, s).wait()

        for src, st, cols, out in ((sk, kst, kt, k_out), (sv, vst, vt, v_out)):
            for i in range(beams):
                r = a * beams + i
                st[s, i] = src[r]
                column_insert(st, (s, i), cols, r, pos_ref[a * beams], slots)
            out(a, s).start()

    @pl.loop(audios - ring, audios)
    def _(a):
        k_out(a, lax.rem(a, ring)).wait()
        v_out(a, lax.rem(a, ring)).wait()


def write_call(layer, beams, hid, pos, kn, vn, sk, sv, ko, vo):
    rows, width, slots = sk.shape
    ring = 4
    return pl.pallas_call(
        functools.partial(write_kernel, layer, beams, ring),
        out_shape=(jax.ShapeDtypeStruct(hid.shape, BF), jax.ShapeDtypeStruct(ko.shape, BF), jax.ShapeDtypeStruct(vo.shape, BF)),
        in_specs=[VM, SMEM, VM, VM, VM, VM, ANY, ANY],
        out_specs=(VM, ANY, ANY),
        input_output_aliases={6: 1, 7: 2},
        scratch_shapes=[
            pltpu.VMEM((ring, beams, width, slots), BF), pltpu.VMEM((ring, beams, width, slots), BF),
            pltpu.VMEM((width, 128), F32), pltpu.VMEM((width, 128), F32), DMA((ring,)), DMA((ring,)),
        ],
        compiler_params=pltpu.CompilerParams(vmem_limit_bytes=10 * 1024 * 1024),
        name="write",
    )(hid, pos, kn, vn, sk, sv, ko, vo)


def solution(mesh):
    cache_spec = P(None, 'dp', None, 'tp', None)
    col_spec = P(None, None, 'tp')
    row_spec = P(None, 'tp', None)
    vec_spec = P(None, 'tp')
    in_specs = (P('dp', None), P('dp'), cache_spec, cache_spec, cache_spec, cache_spec,
                P(), P(), col_spec, vec_spec, col_spec, col_spec, vec_spec, row_spec, P(), col_spec, vec_spec, row_spec, P(), col_spec, vec_spec, row_spec, P())

    def heads_first(cache):
        cache = jnp.transpose(cache, (0, 1, 3, 4, 2))
        return cache.reshape(cache.shape[:2] + (-1, cache.shape[-1]))

    def heads_last(cache, like):
        layers, batch, slots, heads, dim = like.shape
        return jnp.transpose(cache.reshape(layers, batch, heads, dim, slots), (0, 1, 4, 2, 3))

    def local_step(hidden, positions, self_keys, self_vals, cross_keys, cross_vals, g, b, wq, bq, wk, wv, bv, wo, bo, wc, bc, wco, bco, w1, b1, w2, b2):
        beams = hidden.shape[0] // cross_keys.shape[1]
        sk, sv, ck, cv = (heads_first(x) for x in (self_keys, self_vals, cross_keys, cross_vals))
        wq, wk, wv, wc = (jnp.swapaxes(w, 1, 2) for w in (wq, wk, wv, wc))
        o, ko, vo = self_call(0, beams, hidden, positions, g, b, wq, wk, wv, bq, bv, sk, sv)
        hidden, sk1, sv1, kn, vn = rest_call(beams, 2, o, hidden, positions, g, b, wq, bq, wk, wv, bv, wo, bo, wc, bc, wco, bco, w1, b1, w2, b2, sk, sv, ck, cv)
        hidden, ko, vo = write_call(1, beams, hidden, positions, kn, vn, sk1, sv1, ko, vo)
        return hidden, heads_last(ko, self_keys), heads_last(vo, self_vals)

    return jax.shard_map(local_step, mesh=mesh, in_specs=in_specs, out_specs=(P('dp', None), cache_spec, cache_spec), check_vma=False)
```

```python
import functools

import jax
import jax.numpy as jnp
from jax import lax
from jax.experimental import pallas as pl
from jax.experimental.pallas import tpu as pltpu
from jax.sharding import PartitionSpec as P

EPS = 1e-5
BF = jnp.bfloat16
F32 = jnp.float32
MESH = pl.DeviceIdType.MESH
ANY = pl.BlockSpec(memory_space=pl.ANY)
VM = pl.BlockSpec(memory_space=pltpu.VMEM)
SMEM = pl.BlockSpec(memory_space=pltpu.SMEM)
DMA = pltpu.SemaphoreType.DMA
NT = (((1,), (1,)), ((), ()))
VMEM_LIMIT = 60 * 1024 * 1024
REST_LIMIT = 38 * 1024 * 1024


def layer_norm(wide, gain_row, bias_row):
    center = wide - jnp.mean(wide, axis=-1, keepdims=True)
    var_est = jnp.mean(center * center, axis=-1, keepdims=True)
    return (center * lax.rsqrt(var_est + EPS) * gain_row.astype(F32) + bias_row.astype(F32)).astype(BF)


def dot(a, b):
    return jnp.dot(a, b, preferred_element_type=F32)


def dot_nt(a, b):
    return lax.dot_general(a, b, NT, preferred_element_type=F32)


def iota(shape, dim):
    return lax.broadcasted_iota(jnp.int32, shape, dim)


def insert_slot(places, row, beams, pos, slots):
    last = (slots // 128) * 128
    tile = pos // 128

    def insert(start, size):
        for buf, cols in places:
            width = cols.shape[0]
            hit = iota((width, size), 1) == pos - start
            for i in range(beams):
                col = jnp.take_along_axis(cols[...], jnp.full((width, 128), row + i, jnp.int32), axis=1)[:, :size]
                span = (row + i, slice(None), pl.ds(start, size))
                buf[span] = jnp.where(hit, col.astype(BF), buf[span])

    @pl.when(tile * 128 < last)
    def _():
        insert(pl.multiple_of(tile * 128, 128), 128)

    if slots > last:
        @pl.when(tile * 128 >= last)
        def _():
            insert(last, slots - last)


def as_columns(rows):
    pad = jnp.zeros((128 - rows.shape[0], rows.shape[1]), F32)
    return jnp.concatenate([rows, pad], axis=0).T


def copies(pairs, sem):
    return [pltpu.make_async_copy(s, d, sem.at[i]) for i, (s, d) in enumerate(pairs)]


def self_kernel(layer, beams, h_hbm, pos_ref, g_hbm, b_hbm, wq_hbm, wk_hbm, wv_hbm, bq_hbm, bv_hbm, k_hbm, v_hbm, o_ref, ko_hbm, vo_hbm,
                h, g, b, wq, wk, wv, bq, bv, kbuf, vbuf, qs, kt, vt, os, psem, ksem, vsem, kosem, vosem):
    rows = h.shape[0]
    audios = rows // beams
    slots = kbuf.shape[-1]
    scale = 64 ** -0.25

    small = copies([(h_hbm, h), (g_hbm, g), (b_hbm, b), (wq_hbm.at[layer], wq), (wk_hbm.at[layer], wk), (wv_hbm.at[layer], wv), (bq_hbm, bq), (bv_hbm, bv)], psem)
    for c in small:
        c.start()

    def block(a, src, dst, sem):
        return pltpu.make_async_copy(src, dst, sem.at[a])

    def at(a):
        return pl.ds(a * beams, beams)

    def k_in(a):
        return block(a, k_hbm.at[layer, at(a)], kbuf.at[at(a)], ksem)

    def v_in(a):
        return block(a, v_hbm.at[layer, at(a)], vbuf.at[at(a)], vsem)

    def k_out(a):
        return block(a, kbuf.at[at(a)], ko_hbm.at[layer, at(a)], kosem)

    def v_out(a):
        return block(a, vbuf.at[at(a)], vo_hbm.at[layer, at(a)], vosem)

    @pl.loop(0, audios)
    def _(a):
        k_in(a).start()
        v_in(a).start()

    for c in small:
        c.wait()
    normed = layer_norm(h[...].astype(F32), g[0, layer:layer + 1, :], b[0, layer:layer + 1, :])
    q = ((dot_nt(normed, wq[...]) + bq[layer:layer + 1, :].astype(F32)) * scale).astype(BF)
    kt[...] = as_columns((dot_nt(normed, wk[...]) * scale).astype(BF).astype(F32))
    vt[...] = as_columns((dot_nt(normed, wv[...]) + bv[layer:layer + 1, :].astype(F32)).astype(BF).astype(F32))
    spread = (iota((rows * 8, rows), 0) // 8 == iota((rows * 8, rows), 1)).astype(F32).astype(BF)
    q8 = dot(spread, q)
    qs[...] = jnp.where(iota(q8.shape, 1) // 64 == iota(q8.shape, 0) % 8, q8, 0.0)

    @pl.loop(0, audios // 2)
    def _(pair):
        group = (pair * 2, pair * 2 + 1)
        for a in group:
            k_in(a).wait()
            v_in(a).wait()
            insert_slot(((kbuf, kt), (vbuf, vt)), a * beams, beams, pos_ref[a * beams], slots)
            k_out(a).start()
            v_out(a).start()
        probs = []
        for a in group:
            scores = []
            for i in range(beams):
                r = a * beams + i
                scores.append(dot(qs[pl.ds(pl.multiple_of(r * 8, 8), 8), :].astype(BF), kbuf[r]))
            scores = jnp.concatenate(scores, axis=0)
            scores = jnp.where(iota(scores.shape, 1) <= pos_ref[a * beams], scores, -1e30)
            e = jnp.exp(scores - jnp.max(scores, axis=-1, keepdims=True))
            probs.append(e * (1.0 / jnp.sum(e, axis=-1, keepdims=True)))
        for a, p in zip(group, probs):
            for i in range(beams):
                r = a * beams + i
                out = dot_nt(p[i * 8:i * 8 + 8].astype(BF), vbuf[r])
                mine = iota(out.shape, 1) // 64 == iota(out.shape, 0)
                os[pl.ds(r, 1), :] = jnp.sum(jnp.where(mine, out, 0.0), axis=0, keepdims=True)

    o_ref[...] = os[...].astype(BF)

    @pl.loop(0, audios)
    def _(a):
        k_out(a).wait()
        v_out(a).wait()


def self_call(layer, beams, h, pos, g, b, wq, wk, wv, bq, bv, k, v):
    rows = h.shape[0]
    audios = rows // beams
    _, _, width, slots = k.shape
    args = (h, pos, g, b, wq, wk, wv, bq, bv, k, v)
    return pl.pallas_call(
        functools.partial(self_kernel, layer, beams),
        out_shape=(jax.ShapeDtypeStruct((rows, width), BF), jax.ShapeDtypeStruct(k.shape, BF), jax.ShapeDtypeStruct(v.shape, BF)),
        in_specs=[ANY, SMEM] + [ANY] * 9,
        out_specs=(VM, ANY, ANY),
        scratch_shapes=[
            pltpu.VMEM(h.shape, BF), pltpu.VMEM(g.shape, BF), pltpu.VMEM(b.shape, BF),
            pltpu.VMEM(wq.shape[1:], BF), pltpu.VMEM(wk.shape[1:], BF), pltpu.VMEM(wv.shape[1:], BF),
            pltpu.VMEM(bq.shape, BF), pltpu.VMEM(bv.shape, BF),
            pltpu.VMEM((rows, width, slots), BF), pltpu.VMEM((rows, width, slots), BF),
            pltpu.VMEM((rows * 8, width), F32), pltpu.VMEM((width, 128), F32), pltpu.VMEM((width, 128), F32), pltpu.VMEM((rows, width), F32),
            DMA((8,)), DMA((audios,)), DMA((audios,)), DMA((audios,)), DMA((audios,)),
        ],
        compiler_params=pltpu.CompilerParams(vmem_limit_bytes=VMEM_LIMIT),
        name=f"self_{layer}",
    )(*args)


def rest_kernel(beams, parts, o_hbm, h_hbm, pos_ref, g_hbm, b_hbm, wq_hbm, bq_hbm, wk_hbm, wv_hbm, bv_hbm, wo_hbm, bo_hbm, wc_hbm, bc_hbm, wco_hbm, bco_hbm, w1_hbm, b1_hbm, w2_hbm, b2_hbm,
                sk_hbm, sv_hbm, ck_hbm, cv_hbm, out_ref, sk, sv, kn_ref, vn_ref,
                o, h, g, b, wq, bq, wk, wv, bv, wo, bo, wc, bc, wco, bco, w1, b1, w2, b2, ck, cv, hid, qc, oc, qs, vs, sn, os, snd, rcv,
                psem, wsem, skem, svem, ckem, cvem, ssem, rsem):
    rows = h.shape[0]
    audios = rows // beams
    group = audios // parts
    prow = rows // parts
    width = o.shape[1]
    heads = width // 64
    scale = 64 ** -0.25
    dp = lax.axis_index('dp')
    me = lax.axis_index('tp')
    mate = me + 1 - 2 * (me % 2)
    peers = ((me + 2) % 4, (mate + 2) % 4, mate)

    small = copies([(o_hbm, o), (h_hbm, h), (g_hbm, g), (b_hbm, b), (bq_hbm, bq), (bv_hbm, bv), (bo_hbm, bo), (bc_hbm, bc), (bco_hbm, bco), (b1_hbm, b1), (b2_hbm, b2)], psem)
    first = copies([(x.at[0], y.at[0]) for x, y in ((wo_hbm, wo), (wc_hbm, wc), (wco_hbm, wco), (w1_hbm, w1), (w2_hbm, w2))], wsem.at[0])
    second = copies([(x.at[1], y.at[1]) for x, y in ((wo_hbm, wo), (wc_hbm, wc), (wco_hbm, wco), (w1_hbm, w1), (w2_hbm, w2))]
                    + [(x.at[1], y) for x, y in ((wq_hbm, wq), (wk_hbm, wk), (wv_hbm, wv))], wsem.at[1])

    def cross_in(layer, a):
        return pltpu.make_async_copy(ck_hbm.at[layer, a], ck.at[a], ckem.at[a]), pltpu.make_async_copy(cv_hbm.at[layer, a], cv.at[a], cvem.at[a])

    def self_in(a):
        r = pl.ds(a * beams, beams)
        return pltpu.make_async_copy(sk_hbm.at[1, r], sk.at[r], skem.at[a]), pltpu.make_async_copy(sv_hbm.at[1, r], sv.at[r], svem.at[a])

    def start(pair):
        for c in pair:
            c.start()

    def wait(pair):
        for c in pair:
            c.wait()

    start(small)
    start(first[:2])

    @pl.loop(0, audios)
    def _(a):
        start(cross_in(0, a))

    start(first[2:])
    barrier = pltpu.get_barrier_semaphore()
    for peer in peers:
        pl.semaphore_signal(barrier, inc=1, device_id=(dp, peer), device_id_type=MESH)

    start(second)

    @pl.loop(0, audios)
    def _(a):
        start(self_in(a))

    pl.semaphore_wait(barrier, 3)

    def sends(step, m):
        return [pltpu.make_async_remote_copy(snd.at[step, m], rcv.at[step, m, j], ssem.at[step, m, j], rsem.at[step, m, j], device_id=(dp, peer), device_id_type=MESH) for j, peer in enumerate(peers)]

    def push(step, m, part):
        snd[step, m] = part.astype(BF)
        start(sends(step, m))

    def total(step, m):
        wait(sends(step, m))
        mine = snd[step, m].astype(F32) + rcv[step, m, 2].astype(F32)
        return mine + (rcv[step, m, 0].astype(F32) + rcv[step, m, 1].astype(F32))

    def settle(step, m, bias):
        new = (hid[m].astype(F32) + total(step, m) + bias.astype(F32)).astype(BF)
        hid[m] = new
        return new.astype(F32)

    def flags(shape, rule):
        return rule(iota(shape, 0), iota(shape, 1)).astype(F32).astype(BF)

    def pick(m):
        return flags((prow, rows), lambda r, c: c == r + m * prow)

    def cross_half(layer, m, wide):
        normed = layer_norm(wide, g[1, layer:layer + 1, :], b[1, layer:layer + 1, :])
        q = ((dot_nt(normed, wc[layer]) + bc[layer:layer + 1, :].astype(F32)) * scale).astype(BF)
        qc[m] = dot(flags((group * 8, prow), lambda r, c: (r // 8 == c // beams) & (r % 8 == c % beams)), q)

        @pl.loop(0, group)
        def _(n):
            wait(cross_in(layer, m * group + n))

        own = iota((heads * 8, width), 1) // 64 == iota((heads * 8, width), 0) // 8

        def probs_of(n):
            qa = jnp.concatenate([qc[m, n * 8:n * 8 + 8, :]] * heads, axis=0)
            scores = dot(jnp.where(own, qa, 0.0).astype(BF), ck[m * group + n])
            e = jnp.exp(scores - jnp.max(scores, axis=-1, keepdims=True))
            return (e * (1.0 / jnp.sum(e, axis=-1, keepdims=True))).astype(BF)

        def mix(n, p):
            out = jnp.where(own, dot_nt(p, cv[m * group + n]), 0.0)
            acc = out[0:8]
            for j in range(1, heads):
                acc = acc + out[j * 8:j * 8 + 8]
            oc[m, n * 8:n * 8 + 8, :] = acc

        p = probs_of(0)
        for n in range(group):
            p_next = probs_of(n + 1) if n + 1 < group else None
            mix(n, p)
            p = p_next

        if layer == 0:
            @pl.loop(0, group)
            def _(n):
                start(cross_in(1, m * group + n))
        cross = dot(flags((prow, group * 8), lambda r, c: (c // 8 == r // beams) & (c % 8 == r % beams)), oc[m].astype(BF)).astype(BF)
        return dot(cross, wco[layer])

    def mlp_half(layer, m, wide):
        normed = layer_norm(wide, g[2, layer:layer + 1, :], b[2, layer:layer + 1, :])
        inner = dot(normed, w1[layer]) + b1[layer:layer + 1, :].astype(F32)
        inner = (0.5 * inner * (1.0 + lax.erf(inner * (2.0 ** -0.5)))).astype(BF)
        return dot(inner, w2[layer])

    def self_half(m, wide):
        normed = layer_norm(wide, g[0, 1:1 + 1, :], b[0, 1:1 + 1, :])
        q = ((dot_nt(normed, wq[...]) + bq[1:2, :].astype(F32)) * scale).astype(BF)
        k = (dot_nt(normed, wk[...]) * scale).astype(BF)
        v = (dot_nt(normed, wv[...]) + bv[1:2, :].astype(F32)).astype(BF)
        kn_ref[m] = k
        vn_ref[m] = v
        spread = flags((prow * 8, prow), lambda r, c: r // 8 == c)
        q8 = dot(spread, q)
        own = iota(q8.shape, 1) // 64 == iota(q8.shape, 0) % 8
        q8 = jnp.where(own, q8, 0.0)
        qs[m] = q8
        vs[m] = jnp.where(own, dot(spread, v), 0.0)
        sn[m] = jnp.broadcast_to(jnp.sum(q8 * dot(spread, k), axis=-1, keepdims=True), sn.shape[1:])

        @pl.loop(0, group // 2)
        def _(i):
            local = (i * 2, i * 2 + 1)
            probs, news = [], []
            for n in local:
                a = m * group + n
                wait(self_in(a))
                pos = pos_ref[a * beams]
                scores = []
                for j in range(beams):
                    row = pl.ds(pl.multiple_of((n * beams + j) * 8, 8), 8)
                    scores.append(dot(qs[m, row, :].astype(BF), sk[a * beams + j]))
                scores = jnp.concatenate(scores, axis=0)
                fresh = sn[m, pl.ds(pl.multiple_of(n * beams * 8, 8), beams * 8), 0:1]
                slot = iota(scores.shape, 1)
                scores = jnp.where(slot < pos, scores, -1e30)
                top = jnp.maximum(jnp.max(scores, axis=-1, keepdims=True), fresh)
                e = jnp.where(slot < pos, jnp.exp(scores - top), 0.0)
                e_new = jnp.exp(fresh - top)
                inv = 1.0 / (jnp.sum(e, axis=-1, keepdims=True) + e_new)
                probs.append(e * inv)
                news.append((e_new * inv).astype(BF).astype(F32))
            for n, p, p_new in zip(local, probs, news):
                a = m * group + n
                for j in range(beams):
                    row = pl.ds(pl.multiple_of((n * beams + j) * 8, 8), 8)
                    out = dot_nt(p[j * 8:j * 8 + 8].astype(BF), sv[a * beams + j])
                    mine = iota(out.shape, 1) // 64 == iota(out.shape, 0)
                    out = jnp.where(mine, out, 0.0) + p_new[j * 8:j * 8 + 8] * vs[m, row, :]
                    os[m, pl.ds(n * beams + j, 1), :] = jnp.sum(out, axis=0, keepdims=True)

        return dot(os[m].astype(BF), wo[1])

    wait(small)
    wait(first[:1])
    for m in range(parts):
        push(0, m, dot(dot(pick(m), o[...]).astype(BF), wo[0]))
        hid[m] = dot(pick(m), h[...]).astype(BF)
    wait(first[1:3])
    for m in range(parts):
        push(1, m, cross_half(0, m, settle(0, m, bo[0:1, :])))
        if m == 0:
            wait(first[3:])
    for m in range(parts):
        push(2, m, mlp_half(0, m, settle(1, m, bco[0:1, :])))
    wait(second)
    for m in range(parts):
        push(3, m, self_half(m, settle(2, m, b2[0:1, :])))
    for m in range(parts):
        push(4, m, cross_half(1, m, settle(3, m, bo[1:2, :])))
    for m in range(parts):
        push(5, m, mlp_half(1, m, settle(4, m, bco[1:2, :])))
    result = jnp.zeros((rows, h.shape[1]), F32)
    for m in range(parts):
        place = flags((rows, prow), lambda r, c: r == c + m * prow)
        result = result + dot(place, settle(5, m, b2[1:2, :]).astype(BF))
    out_ref[...] = result.astype(BF)


def rest_call(beams, parts, o, h, pos, g, b, wq, bq, wk, wv, bv, wo, bo, wc, bc, wco, bco, w1, b1, w2, b2, sk, sv, ck, cv):
    rows, dim = h.shape
    _, audios, width, frames = ck.shape
    slots = sk.shape[-1]
    prow = rows // parts
    prows8 = prow * 8
    args = (o, h, pos, g, b, wq, bq, wk, wv, bv, wo, bo, wc, bc, wco, bco, w1, b1, w2, b2, sk, sv, ck, cv)

    def whole(x):
        return pltpu.VMEM(x.shape, BF)

    def one(x):
        return pltpu.VMEM(x.shape[1:], BF)

    return pl.pallas_call(
        functools.partial(rest_kernel, beams, parts),
        out_shape=(pltpu.VMEM(h.shape, BF), pltpu.VMEM((rows, width, slots), BF), pltpu.VMEM((rows, width, slots), BF), pltpu.VMEM((parts, prow, width), BF), pltpu.VMEM((parts, prow, width), BF)),
        in_specs=[ANY, ANY, SMEM] + [ANY] * (len(args) - 3),
        out_specs=(VM,) * 5,
        scratch_shapes=[
            whole(o), whole(h), whole(g), whole(b), one(wq), whole(bq), one(wk), one(wv), whole(bv), whole(wo), whole(bo), whole(wc), whole(bc),
            whole(wco), whole(bco), whole(w1), whole(b1), whole(w2), whole(b2), one(ck), one(cv),
            pltpu.VMEM((parts, prow, dim), BF),
            pltpu.VMEM((parts, audios // parts * 8, width), F32), pltpu.VMEM((parts, audios // parts * 8, width), F32),
            pltpu.VMEM((parts, prows8, width), F32), pltpu.VMEM((parts, prows8, width), F32), pltpu.VMEM((parts, prows8, 128), F32), pltpu.VMEM((parts, prow, width), F32),
            pltpu.VMEM((6, parts, prow, dim), BF), pltpu.VMEM((6, parts, 3, prow, dim), BF),
            DMA((11,)), DMA((2, 8)), DMA((audios,)), DMA((audios,)), DMA((audios,)), DMA((audios,)), DMA((6, parts, 3)), DMA((6, parts, 3)),
        ],
        compiler_params=pltpu.CompilerParams(collective_id=0, has_side_effects=True, vmem_limit_bytes=REST_LIMIT),
        name="rest",
    )(*args)


def write_kernel(layer, beams, hid, pos_ref, kn, vn, sk_in, sv_in, ki_hbm, vi_hbm, out_ref, ko_hbm, vo_hbm, sk, sv, kt, vt, kosem, vosem):
    parts, prow, width = kn.shape
    rows = parts * prow
    audios = rows // beams
    slots = sk.shape[-1]

    def k_out(a):
        r = pl.ds(a * beams, beams)
        return pltpu.make_async_copy(sk.at[r], ko_hbm.at[layer, r], kosem.at[a])

    def v_out(a):
        r = pl.ds(a * beams, beams)
        return pltpu.make_async_copy(sv.at[r], vo_hbm.at[layer, r], vosem.at[a])

    def columns(new):
        both = jnp.zeros((rows, width), F32)
        for m in range(parts):
            place = (iota((rows, prow), 0) == iota((rows, prow), 1) + m * prow).astype(F32).astype(BF)
            both = both + dot(place, new[m])
        return as_columns(both)

    kt[...] = columns(kn)
    vt[...] = columns(vn)
    out_ref[...] = hid[...]

    @pl.loop(0, audios)
    def _(a):
        insert_slot(((sk, kt), (sv, vt)), a * beams, beams, pos_ref[a * beams], slots)
        k_out(a).start()
        v_out(a).start()

    @pl.loop(0, audios)
    def _(a):
        k_out(a).wait()
        v_out(a).wait()


def write_call(layer, beams, hid, pos, kn, vn, sk, sv, ko, vo):
    rows, width, slots = sk.shape
    audios = rows // beams
    return pl.pallas_call(
        functools.partial(write_kernel, layer, beams),
        out_shape=(jax.ShapeDtypeStruct(hid.shape, BF), jax.ShapeDtypeStruct(ko.shape, BF), jax.ShapeDtypeStruct(vo.shape, BF), pltpu.VMEM(sk.shape, BF), pltpu.VMEM(sv.shape, BF)),
        in_specs=[VM, SMEM, VM, VM, VM, VM, ANY, ANY],
        out_specs=(VM, ANY, ANY, VM, VM),
        input_output_aliases={4: 3, 5: 4, 6: 1, 7: 2},
        scratch_shapes=[pltpu.VMEM((width, 128), F32), pltpu.VMEM((width, 128), F32), DMA((audios,)), DMA((audios,))],
        compiler_params=pltpu.CompilerParams(vmem_limit_bytes=4 * 1024 * 1024),
        name="write",
    )(hid, pos, kn, vn, sk, sv, ko, vo)[:3]


def solution(mesh):
    cache_spec = P(None, 'dp', None, 'tp', None)
    col_spec = P(None, None, 'tp')
    row_spec = P(None, 'tp', None)
    vec_spec = P(None, 'tp')
    in_specs = (P('dp', None), P('dp'), cache_spec, cache_spec, cache_spec, cache_spec,
                P(), P(), col_spec, vec_spec, col_spec, col_spec, vec_spec, row_spec, P(), col_spec, vec_spec, row_spec, P(), col_spec, vec_spec, row_spec, P())

    def heads_first(cache):
        cache = jnp.transpose(cache, (0, 1, 3, 4, 2))
        return cache.reshape(cache.shape[:2] + (-1, cache.shape[-1]))

    def heads_last(cache, like):
        layers, batch, slots, heads, dim = like.shape
        return jnp.transpose(cache.reshape(layers, batch, heads, dim, slots), (0, 1, 4, 2, 3))

    def local_step(hidden, positions, self_keys, self_vals, cross_keys, cross_vals, g, b, wq, bq, wk, wv, bv, wo, bo, wc, bc, wco, bco, w1, b1, w2, b2):
        beams = hidden.shape[0] // cross_keys.shape[1]
        sk, sv, ck, cv = (heads_first(x) for x in (self_keys, self_vals, cross_keys, cross_vals))
        wq, wk, wv, wc = (jnp.swapaxes(w, 1, 2) for w in (wq, wk, wv, wc))
        g, b = (jnp.swapaxes(x, 0, 1) for x in (g, b))
        o, ko, vo = self_call(0, beams, hidden, positions, g, b, wq, wk, wv, bq, bv, sk, sv)
        hidden, sk1, sv1, kn, vn = rest_call(beams, 2, o, hidden, positions, g, b, wq, bq, wk, wv, bv, wo, bo, wc, bc, wco, bco, w1, b1, w2, b2, sk, sv, ck, cv)
        hidden, ko, vo = write_call(1, beams, hidden, positions, kn, vn, sk1, sv1, ko, vo)
        return hidden, heads_last(ko, self_keys), heads_last(vo, self_vals)

    return jax.shard_map(local_step, mesh=mesh, in_specs=in_specs, out_specs=(P('dp', None), cache_spec, cache_spec), check_vma=False)
```

```python
import functools

import jax
import jax.numpy as jnp
from jax import lax
from jax.experimental import pallas as pl
from jax.experimental.pallas import tpu as pltpu
from jax.sharding import PartitionSpec as P

EPS = 1e-5
BF = jnp.bfloat16
F32 = jnp.float32
MESH = pl.DeviceIdType.MESH
ANY = pl.BlockSpec(memory_space=pl.ANY)
VM = pl.BlockSpec(memory_space=pltpu.VMEM)
SMEM = pl.BlockSpec(memory_space=pltpu.SMEM)
DMA = pltpu.SemaphoreType.DMA
NT = (((1,), (1,)), ((), ()))
VMEM_LIMIT = 60 * 1024 * 1024
REST_LIMIT = 38 * 1024 * 1024


def layer_norm(wide, gain_row, bias_row):
    center = wide - jnp.mean(wide, axis=-1, keepdims=True)
    var_est = jnp.mean(center * center, axis=-1, keepdims=True)
    return (center * lax.rsqrt(var_est + EPS) * gain_row.astype(F32) + bias_row.astype(F32)).astype(BF)


def dot(a, b):
    return jnp.dot(a, b, preferred_element_type=F32)


def dot_nt(a, b):
    return lax.dot_general(a, b, NT, preferred_element_type=F32)


def iota(shape, dim):
    return lax.broadcasted_iota(jnp.int32, shape, dim)


def insert_slot(places, row, beams, pos, slots):
    last = (slots // 128) * 128
    tile = pos // 128

    def insert(start, size):
        for buf, cols in places:
            width = cols.shape[0]
            hit = iota((width, size), 1) == pos - start
            for i in range(beams):
                col = jnp.take_along_axis(cols[...], jnp.full((width, 128), row + i, jnp.int32), axis=1)[:, :size]
                span = (row + i, slice(None), pl.ds(start, size))
                buf[span] = jnp.where(hit, col.astype(BF), buf[span])

    @pl.when(tile * 128 < last)
    def _():
        insert(pl.multiple_of(tile * 128, 128), 128)

    if slots > last:
        @pl.when(tile * 128 >= last)
        def _():
            insert(last, slots - last)


def as_columns(rows):
    pad = jnp.zeros((128 - rows.shape[0], rows.shape[1]), F32)
    return jnp.concatenate([rows, pad], axis=0).T


def copies(pairs, sem):
    return [pltpu.make_async_copy(s, d, sem.at[i]) for i, (s, d) in enumerate(pairs)]


def self_kernel(layer, beams, h_hbm, pos_ref, g_hbm, b_hbm, wq_hbm, wk_hbm, wv_hbm, bq_hbm, bv_hbm, k_hbm, v_hbm, o_ref, ko_hbm, vo_hbm,
                h, g, b, wq, wk, wv, bq, bv, kbuf, vbuf, qs, kt, vt, os, psem, ksem, vsem, kosem, vosem):
    rows = h.shape[0]
    audios = rows // beams
    slots = kbuf.shape[-1]
    scale = 64 ** -0.25

    small = copies([(h_hbm, h), (g_hbm, g), (b_hbm, b), (wq_hbm.at[layer], wq), (wk_hbm.at[layer], wk), (wv_hbm.at[layer], wv), (bq_hbm, bq), (bv_hbm, bv)], psem)
    for c in small:
        c.start()

    def block(a, src, dst, sem):
        return pltpu.make_async_copy(src, dst, sem.at[a])

    def at(a):
        return pl.ds(a * beams, beams)

    def k_in(a):
        return block(a, k_hbm.at[layer, at(a)], kbuf.at[at(a)], ksem)

    def v_in(a):
        return block(a, v_hbm.at[layer, at(a)], vbuf.at[at(a)], vsem)

    def k_out(a):
        return block(a, kbuf.at[at(a)], ko_hbm.at[layer, at(a)], kosem)

    def v_out(a):
        return block(a, vbuf.at[at(a)], vo_hbm.at[layer, at(a)], vosem)

    @pl.loop(0, audios)
    def _(a):
        k_in(a).start()
        v_in(a).start()

    for c in small:
        c.wait()
    normed = layer_norm(h[...].astype(F32), g[0, layer:layer + 1, :], b[0, layer:layer + 1, :])
    q = ((dot_nt(normed, wq[...]) + bq[layer:layer + 1, :].astype(F32)) * scale).astype(BF)
    kt[...] = as_columns((dot_nt(normed, wk[...]) * scale).astype(BF).astype(F32))
    vt[...] = as_columns((dot_nt(normed, wv[...]) + bv[layer:layer + 1, :].astype(F32)).astype(BF).astype(F32))
    spread = (iota((rows * 8, rows), 0) // 8 == iota((rows * 8, rows), 1)).astype(F32).astype(BF)
    q8 = dot(spread, q)
    qs[...] = jnp.where(iota(q8.shape, 1) // 64 == iota(q8.shape, 0) % 8, q8, 0.0)

    @pl.loop(0, audios // 2)
    def _(pair):
        group = (pair * 2, pair * 2 + 1)
        for a in group:
            k_in(a).wait()
            v_in(a).wait()
            insert_slot(((kbuf, kt), (vbuf, vt)), a * beams, beams, pos_ref[a * beams], slots)
            k_out(a).start()
            v_out(a).start()
        probs = []
        for a in group:
            scores = []
            for i in range(beams):
                r = a * beams + i
                scores.append(dot(qs[pl.ds(pl.multiple_of(r * 8, 8), 8), :].astype(BF), kbuf[r]))
            scores = jnp.concatenate(scores, axis=0)
            scores = jnp.where(iota(scores.shape, 1) <= pos_ref[a * beams], scores, -1e30)
            e = jnp.exp(scores - jnp.max(scores, axis=-1, keepdims=True))
            probs.append(e * (1.0 / jnp.sum(e, axis=-1, keepdims=True)))
        for a, p in zip(group, probs):
            for i in range(beams):
                r = a * beams + i
                out = dot_nt(p[i * 8:i * 8 + 8].astype(BF), vbuf[r])
                mine = iota(out.shape, 1) // 64 == iota(out.shape, 0)
                os[pl.ds(r, 1), :] = jnp.sum(jnp.where(mine, out, 0.0), axis=0, keepdims=True)

    o_ref[...] = os[...].astype(BF)

    @pl.loop(0, audios)
    def _(a):
        k_out(a).wait()
        v_out(a).wait()


def self_call(layer, beams, h, pos, g, b, wq, wk, wv, bq, bv, k, v):
    rows = h.shape[0]
    audios = rows // beams
    _, _, width, slots = k.shape
    args = (h, pos, g, b, wq, wk, wv, bq, bv, k, v)
    return pl.pallas_call(
        functools.partial(self_kernel, layer, beams),
        out_shape=(jax.ShapeDtypeStruct((rows, width), BF), jax.ShapeDtypeStruct(k.shape, BF), jax.ShapeDtypeStruct(v.shape, BF)),
        in_specs=[ANY, SMEM] + [ANY] * 9,
        out_specs=(VM, ANY, ANY),
        scratch_shapes=[
            pltpu.VMEM(h.shape, BF), pltpu.VMEM(g.shape, BF), pltpu.VMEM(b.shape, BF),
            pltpu.VMEM(wq.shape[1:], BF), pltpu.VMEM(wk.shape[1:], BF), pltpu.VMEM(wv.shape[1:], BF),
            pltpu.VMEM(bq.shape, BF), pltpu.VMEM(bv.shape, BF),
            pltpu.VMEM((rows, width, slots), BF), pltpu.VMEM((rows, width, slots), BF),
            pltpu.VMEM((rows * 8, width), F32), pltpu.VMEM((width, 128), F32), pltpu.VMEM((width, 128), F32), pltpu.VMEM((rows, width), F32),
            DMA((8,)), DMA((audios,)), DMA((audios,)), DMA((audios,)), DMA((audios,)),
        ],
        cost_estimate=pl.CostEstimate(flops=0, bytes_accessed=4 * k.size, transcendentals=0),
        compiler_params=pltpu.CompilerParams(vmem_limit_bytes=VMEM_LIMIT),
        name=f"self_{layer}",
    )(*args)


def rest_kernel(beams, parts, o_hbm, h_hbm, pos_ref, g_hbm, b_hbm, wq_hbm, bq_hbm, wk_hbm, wv_hbm, bv_hbm, wo_hbm, bo_hbm, wc_hbm, bc_hbm, wco_hbm, bco_hbm, w1_hbm, b1_hbm, w2_hbm, b2_hbm,
                wo_far, wco_far, sk_hbm, sv_hbm, ck_hbm, cv_hbm, part_ref, out_ref, sk, sv, kn_ref, vn_ref,
                o, h, g, b, wq, bq, wk, wv, bv, wo, bo, wc, bc, wco, wco1, bco, w1, b1, w2, b2, ck, cv, hid, qc, oc, qs, vs, sn, os, got, snd, rcv,
                psem, wsem, gsem, gssem, grsem, skem, svem, ckem, cvem, ssem, rsem):
    rows = h.shape[0]
    audios = rows // beams
    group = audios // parts
    prow = rows // parts
    width = o.shape[1]
    heads = width // 64
    scale = 64 ** -0.25
    dp = lax.axis_index('dp')
    me = lax.axis_index('tp')
    mate = me + 1 - 2 * (me % 2)
    peers = ((me + 2) % 4, (mate + 2) % 4, mate)

    small = copies([(o_hbm, o), (h_hbm, h), (g_hbm, g), (b_hbm, b), (bq_hbm, bq), (bv_hbm, bv), (bo_hbm, bo), (bc_hbm, bc), (bco_hbm, bco), (b1_hbm, b1), (b2_hbm, b2)], psem)
    matrices = ((wo_hbm.at[0], wo_far.at[0], wo.at[0]), (wco_hbm.at[0], wco_far, wco.at[0]), (wo_hbm.at[1], wo_far.at[1], wo.at[1]))
    gathered = [copies([(own, rows_of.at[0])], gsem.at[i]) for i, (own, _, rows_of) in enumerate(matrices)]

    def shared(i):
        own, far, rows_of = matrices[i]
        return [pltpu.make_async_remote_copy(src, rows_of.at[1 + j], gssem.at[i, j], grsem.at[i, j], device_id=(dp, mate), device_id_type=MESH) for j, src in enumerate((own, far))]

    first = copies([(x.at[0], y.at[0]) for x, y in ((wc_hbm, wc), (w1_hbm, w1), (w2_hbm, w2))], wsem.at[0])
    second = copies([(x.at[1], y.at[1]) for x, y in ((wc_hbm, wc), (w1_hbm, w1), (w2_hbm, w2))]
                    + [(wco_hbm.at[1], wco1)] + [(x.at[1], y) for x, y in ((wq_hbm, wq), (wk_hbm, wk), (wv_hbm, wv))], wsem.at[1])

    def cross_in(layer, a):
        return pltpu.make_async_copy(ck_hbm.at[layer, a], ck.at[a], ckem.at[a]), pltpu.make_async_copy(cv_hbm.at[layer, a], cv.at[a], cvem.at[a])

    def self_in(a):
        r = pl.ds(a * beams, beams)
        return pltpu.make_async_copy(sk_hbm.at[1, r], sk.at[r], skem.at[a]), pltpu.make_async_copy(sv_hbm.at[1, r], sv.at[r], svem.at[a])

    def start(pair):
        for c in pair:
            c.start()

    def wait(pair):
        for c in pair:
            c.wait()

    start(small)
    start(gathered[0])
    start(first[:1])

    @pl.loop(0, audios)
    def _(a):
        start(cross_in(0, a))

    start(gathered[1])
    start(first[1:])
    barrier = pltpu.get_barrier_semaphore()
    for peer in peers:
        pl.semaphore_signal(barrier, inc=1, device_id=(dp, peer), device_id_type=MESH)

    start(gathered[2])
    start(second)

    @pl.loop(0, audios)
    def _(a):
        start(self_in(a))

    pl.semaphore_wait(barrier, 3)
    start(shared(0))

    def sends(step, m):
        return [pltpu.make_async_remote_copy(snd.at[step, m], rcv.at[step, m, j], ssem.at[step, m, j], rsem.at[step, m, j], device_id=(dp, peer), device_id_type=MESH) for j, peer in enumerate(peers)]

    def push(step, m, part):
        snd[step, m] = part.astype(BF)
        start(sends(step, m))

    def total(step, m):
        wait(sends(step, m))
        mine = snd[step, m].astype(F32) + rcv[step, m, 2].astype(F32)
        return mine + (rcv[step, m, 0].astype(F32) + rcv[step, m, 1].astype(F32))

    def heads_sends(step, m):
        return [pltpu.make_async_remote_copy(got.at[step, m, 3], got.at[step, m, j], ssem.at[step, m, j], rsem.at[step, m, j], device_id=(dp, peer), device_id_type=MESH) for j, peer in enumerate(peers)]

    def push_heads(step, m, out):
        got[step, m, 3] = out
        start(heads_sends(step, m))

    def project(step, m, i):
        wait(heads_sends(step, m))
        _, far, rows_of = matrices[i]
        here = dot(got[step, m, 3], rows_of[0]) + dot(got[step, m, 2], rows_of[1])
        return here + (dot(got[step, m, 0], far[...]) + dot(got[step, m, 1], rows_of[2]))

    def settle(m, update, bias):
        new = (hid[m].astype(F32) + update + bias.astype(F32)).astype(BF)
        hid[m] = new
        return new.astype(F32)

    def flags(shape, rule):
        return rule(iota(shape, 0), iota(shape, 1)).astype(F32).astype(BF)

    def pick(m):
        return flags((prow, rows), lambda r, c: c == r + m * prow)

    def cross_half(layer, m, wide):
        normed = layer_norm(wide, g[1, layer:layer + 1, :], b[1, layer:layer + 1, :])
        q = ((dot_nt(normed, wc[layer]) + bc[layer:layer + 1, :].astype(F32)) * scale).astype(BF)
        qc[m] = dot(flags((group * 8, prow), lambda r, c: (r // 8 == c // beams) & (r % 8 == c % beams)), q)

        @pl.loop(0, group)
        def _(n):
            wait(cross_in(layer, m * group + n))

        own = iota((heads * 8, width), 1) // 64 == iota((heads * 8, width), 0) // 8

        def probs_of(n):
            qa = jnp.concatenate([qc[m, n * 8:n * 8 + 8, :]] * heads, axis=0)
            scores = dot(jnp.where(own, qa, 0.0).astype(BF), ck[m * group + n])
            e = jnp.exp(scores - jnp.max(scores, axis=-1, keepdims=True))
            return (e * (1.0 / jnp.sum(e, axis=-1, keepdims=True))).astype(BF)

        def mix(n, p):
            out = jnp.where(own, dot_nt(p, cv[m * group + n]), 0.0)
            acc = out[0:8]
            for j in range(1, heads):
                acc = acc + out[j * 8:j * 8 + 8]
            oc[m, n * 8:n * 8 + 8, :] = acc

        p = probs_of(0)
        for n in range(group):
            p_next = probs_of(n + 1) if n + 1 < group else None
            mix(n, p)
            p = p_next

        if layer == 0:
            @pl.loop(0, group)
            def _(n):
                start(cross_in(1, m * group + n))
        cross = dot(flags((prow, group * 8), lambda r, c: (c // 8 == r // beams) & (c % 8 == r % beams)), oc[m].astype(BF)).astype(BF)
        return cross

    def mlp_half(layer, m, wide):
        normed = layer_norm(wide, g[2, layer:layer + 1, :], b[2, layer:layer + 1, :])
        inner = dot(normed, w1[layer]) + b1[layer:layer + 1, :].astype(F32)
        inner = (0.5 * inner * (1.0 + lax.erf(inner * (2.0 ** -0.5)))).astype(BF)
        return dot(inner, w2[layer])

    def self_half(m, wide):
        normed = layer_norm(wide, g[0, 1:1 + 1, :], b[0, 1:1 + 1, :])
        q = ((dot_nt(normed, wq[...]) + bq[1:2, :].astype(F32)) * scale).astype(BF)
        k = (dot_nt(normed, wk[...]) * scale).astype(BF)
        v = (dot_nt(normed, wv[...]) + bv[1:2, :].astype(F32)).astype(BF)
        kn_ref[m] = k
        vn_ref[m] = v
        spread = flags((prow * 8, prow), lambda r, c: r // 8 == c)
        q8 = dot(spread, q)
        own = iota(q8.shape, 1) // 64 == iota(q8.shape, 0) % 8
        q8 = jnp.where(own, q8, 0.0)
        qs[m] = q8
        vs[m] = jnp.where(own, dot(spread, v), 0.0)
        sn[m] = jnp.broadcast_to(jnp.sum(q8 * dot(spread, k), axis=-1, keepdims=True), sn.shape[1:])

        @pl.loop(0, group // 2)
        def _(i):
            local = (i * 2, i * 2 + 1)
            probs, news = [], []
            for n in local:
                a = m * group + n
                wait(self_in(a))
                pos = pos_ref[a * beams]
                scores = []
                for j in range(beams):
                    row = pl.ds(pl.multiple_of((n * beams + j) * 8, 8), 8)
                    scores.append(dot(qs[m, row, :].astype(BF), sk[a * beams + j]))
                scores = jnp.concatenate(scores, axis=0)
                fresh = sn[m, pl.ds(pl.multiple_of(n * beams * 8, 8), beams * 8), 0:1]
                slot = iota(scores.shape, 1)
                scores = jnp.where(slot < pos, scores, -1e30)
                top = jnp.maximum(jnp.max(scores, axis=-1, keepdims=True), fresh)
                e = jnp.where(slot < pos, jnp.exp(scores - top), 0.0)
                e_new = jnp.exp(fresh - top)
                inv = 1.0 / (jnp.sum(e, axis=-1, keepdims=True) + e_new)
                probs.append(e * inv)
                news.append((e_new * inv).astype(BF).astype(F32))
            for n, p, p_new in zip(local, probs, news):
                a = m * group + n
                for j in range(beams):
                    row = pl.ds(pl.multiple_of((n * beams + j) * 8, 8), 8)
                    out = dot_nt(p[j * 8:j * 8 + 8].astype(BF), sv[a * beams + j])
                    mine = iota(out.shape, 1) // 64 == iota(out.shape, 0)
                    out = jnp.where(mine, out, 0.0) + p_new[j * 8:j * 8 + 8] * vs[m, row, :]
                    os[m, pl.ds(n * beams + j, 1), :] = jnp.sum(out, axis=0, keepdims=True)

        return os[m].astype(BF)

    wait(small)
    for m in range(parts):
        push_heads(0, m, dot(pick(m), o[...]).astype(BF))
    start(shared(1))
    start(shared(2))
    for m in range(parts):
        hid[m] = dot(pick(m), h[...]).astype(BF)
    wait(gathered[0])
    wait(shared(0))
    wait(first[:1])
    for m in range(parts):
        push_heads(1, m, cross_half(0, m, settle(m, project(0, m, 0), bo[0:1, :])))
    wait(gathered[1])
    wait(shared(1))
    wait(first[1:])
    for m in range(parts):
        push(2, m, mlp_half(0, m, settle(m, project(1, m, 1), bco[0:1, :])))
    wait(gathered[2])
    wait(shared(2))
    wait(second)
    for m in range(parts):
        push_heads(3, m, self_half(m, settle(m, total(2, m), b2[0:1, :])))
    for m in range(parts):
        push(4, m, dot(cross_half(1, m, settle(m, project(3, m, 2), bo[1:2, :])), wco1[...]))
    final = jnp.zeros((rows, h.shape[1]), F32)
    resid = jnp.zeros((rows, h.shape[1]), F32)
    for m in range(parts):
        place = flags((rows, prow), lambda r, c: r == c + m * prow)
        wide = settle(m, total(4, m), bco[1:2, :])
        final = final + dot(place, mlp_half(1, m, wide).astype(BF))
        resid = resid + dot(place, hid[m])
    part_ref[...] = final.astype(BF)
    out_ref[...] = resid.astype(BF)


def rest_call(beams, parts, o, h, pos, g, b, wq, bq, wk, wv, bv, wo, bo, wc, bc, wco, bco, w1, b1, w2, b2, more, sk, sv, ck, cv):
    rows, dim = h.shape
    _, audios, width, frames = ck.shape
    slots = sk.shape[-1]
    prow = rows // parts
    prows8 = prow * 8
    args = (o, h, pos, g, b, wq, bq, wk, wv, bv, wo, bo, wc, bc, wco, bco, w1, b1, w2, b2) + more + (sk, sv, ck, cv)

    def whole(x):
        return pltpu.VMEM(x.shape, BF)

    def one(x):
        return pltpu.VMEM(x.shape[1:], BF)

    return pl.pallas_call(
        functools.partial(rest_kernel, beams, parts),
        out_shape=(pltpu.VMEM(h.shape, BF), pltpu.VMEM(h.shape, BF), pltpu.VMEM((rows, width, slots), BF), pltpu.VMEM((rows, width, slots), BF), pltpu.VMEM((parts, prow, width), BF), pltpu.VMEM((parts, prow, width), BF)),
        in_specs=[ANY, ANY, SMEM] + [ANY] * (len(args) - 9) + [VM, VM] + [ANY] * 4,
        out_specs=(VM,) * 6,
        scratch_shapes=[
            whole(o), whole(h), whole(g), whole(b), one(wq), whole(bq), one(wk), one(wv), whole(bv), pltpu.VMEM((2, 3, width, dim), BF), whole(bo), whole(wc), whole(bc),
            pltpu.VMEM((1, 3, width, dim), BF), one(wco), whole(bco), whole(w1), whole(b1), whole(w2), whole(b2), one(ck), one(cv),
            pltpu.VMEM((parts, prow, dim), BF),
            pltpu.VMEM((parts, audios // parts * 8, width), F32), pltpu.VMEM((parts, audios // parts * 8, width), F32),
            pltpu.VMEM((parts, prows8, width), F32), pltpu.VMEM((parts, prows8, width), F32), pltpu.VMEM((parts, prows8, 128), F32), pltpu.VMEM((parts, prow, width), F32),
            pltpu.VMEM((6, parts, 4, prow, width), BF), pltpu.VMEM((6, parts, prow, dim), BF), pltpu.VMEM((6, parts, 3, prow, dim), BF),
            DMA((11,)), DMA((2, 8)), DMA((3, 1)), DMA((3, 2)), DMA((3, 2)), DMA((audios,)), DMA((audios,)), DMA((audios,)), DMA((audios,)), DMA((6, parts, 3)), DMA((6, parts, 3)),
        ],
        compiler_params=pltpu.CompilerParams(collective_id=0, has_side_effects=True, vmem_limit_bytes=REST_LIMIT),
        name="rest",
    )(*args)


def write_kernel(layer, beams, pos_ref, kn, vn, sk_in, sv_in, ki_hbm, vi_hbm, ko_hbm, vo_hbm, sk, sv, kt, vt, kosem, vosem):
    parts, prow, width = kn.shape
    rows = parts * prow
    audios = rows // beams
    slots = sk.shape[-1]

    def k_out(a):
        r = pl.ds(a * beams, beams)
        return pltpu.make_async_copy(sk.at[r], ko_hbm.at[layer, r], kosem.at[a])

    def v_out(a):
        r = pl.ds(a * beams, beams)
        return pltpu.make_async_copy(sv.at[r], vo_hbm.at[layer, r], vosem.at[a])

    def columns(new):
        both = jnp.zeros((rows, width), F32)
        for m in range(parts):
            place = (iota((rows, prow), 0) == iota((rows, prow), 1) + m * prow).astype(F32).astype(BF)
            both = both + dot(place, new[m])
        return as_columns(both)

    kt[...] = columns(kn)
    vt[...] = columns(vn)

    @pl.loop(0, audios)
    def _(a):
        insert_slot(((sk, kt), (sv, vt)), a * beams, beams, pos_ref[a * beams], slots)
        k_out(a).start()
        v_out(a).start()

    @pl.loop(0, audios)
    def _(a):
        k_out(a).wait()
        v_out(a).wait()


def write_call(layer, beams, pos, kn, vn, sk, sv, ko, vo):
    rows, width, slots = sk.shape
    audios = rows // beams
    return pl.pallas_call(
        functools.partial(write_kernel, layer, beams),
        out_shape=(jax.ShapeDtypeStruct(ko.shape, BF), jax.ShapeDtypeStruct(vo.shape, BF), pltpu.VMEM(sk.shape, BF), pltpu.VMEM(sv.shape, BF)),
        in_specs=[SMEM, VM, VM, VM, VM, ANY, ANY],
        out_specs=(ANY, ANY, VM, VM),
        input_output_aliases={3: 2, 4: 3, 5: 0, 6: 1},
        cost_estimate=pl.CostEstimate(flops=0, bytes_accessed=4 * sk.size, transcendentals=0),
        scratch_shapes=[pltpu.VMEM((width, 128), F32), pltpu.VMEM((width, 128), F32), DMA((audios,)), DMA((audios,))],
        compiler_params=pltpu.CompilerParams(vmem_limit_bytes=4 * 1024 * 1024),
        name="write",
    )(pos, kn, vn, sk, sv, ko, vo)[:2]


def solution(mesh):
    cache_spec = P(None, 'dp', None, 'tp', None)
    col_spec = P(None, None, 'tp')
    row_spec = P(None, 'tp', None)
    vec_spec = P(None, 'tp')
    in_specs = (P('dp', None), P('dp'), cache_spec, cache_spec, cache_spec, cache_spec,
                P(), P(), col_spec, vec_spec, col_spec, col_spec, vec_spec, row_spec, P(), col_spec, vec_spec, row_spec, P(), col_spec, vec_spec, row_spec, P())

    def heads_first(cache):
        cache = jnp.transpose(cache, (0, 1, 3, 4, 2))
        return cache.reshape(cache.shape[:2] + (-1, cache.shape[-1]))

    def heads_last(cache, like):
        layers, batch, slots, heads, dim = like.shape
        return jnp.transpose(cache.reshape(layers, batch, heads, dim, slots), (0, 1, 4, 2, 3))

    def local_step(hidden, positions, self_keys, self_vals, cross_keys, cross_vals, g, b, wq, bq, wk, wv, bv, wo, bo, wc, bc, wco, bco, w1, b1, w2, b2):
        beams = hidden.shape[0] // cross_keys.shape[1]
        sk, sv, ck, cv = (heads_first(x) for x in (self_keys, self_vals, cross_keys, cross_vals))
        wq, wk, wv, wc = (jnp.swapaxes(w, 1, 2) for w in (wq, wk, wv, wc))
        g, b = (jnp.swapaxes(x, 0, 1) for x in (g, b))
        def hop(x, flip):
            return lax.ppermute(x, 'tp', [(i, i ^ flip) for i in range(4)])

        more = (hop(wo, 2), hop(wco[0], 2))
        o, ko, vo = self_call(0, beams, hidden, positions, g, b, wq, wk, wv, bq, bv, sk, sv)
        part, hidden, sk1, sv1, kn, vn = rest_call(beams, 2, o, hidden, positions, g, b, wq, bq, wk, wv, bv, wo, bo, wc, bc, wco, bco, w1, b1, w2, b2, more, sk, sv, ck, cv)
        ko, vo = write_call(1, beams, positions, kn, vn, sk1, sv1, ko, vo)
        here, mate, far, diag = (x.astype(F32) for x in (part, hop(part, 1), hop(part, 2), hop(part, 3)))
        hidden = (hidden.astype(F32) + ((here + mate) + (far + diag)) + b2[1].astype(F32)).astype(BF)
        return hidden, heads_last(ko, self_keys), heads_last(vo, self_vals)

    return jax.shard_map(local_step, mesh=mesh, in_specs=in_specs, out_specs=(P('dp', None), cache_spec, cache_spec), check_vma=False)
```

```python
import functools

import jax
import jax.numpy as jnp
from jax import lax
from jax.experimental import pallas as pl
from jax.experimental.pallas import tpu as pltpu
from jax.sharding import PartitionSpec as P

EPS = 1e-5
BF = jnp.bfloat16
F32 = jnp.float32
MESH = pl.DeviceIdType.MESH
ANY = pl.BlockSpec(memory_space=pl.ANY)
VM = pl.BlockSpec(memory_space=pltpu.VMEM)
SMEM = pl.BlockSpec(memory_space=pltpu.SMEM)
DMA = pltpu.SemaphoreType.DMA
NT = (((1,), (1,)), ((), ()))
VMEM_LIMIT = 60 * 1024 * 1024
REST_LIMIT = 38 * 1024 * 1024


def layer_norm(wide, gain_row, bias_row):
    center = wide - jnp.mean(wide, axis=-1, keepdims=True)
    var_est = jnp.mean(center * center, axis=-1, keepdims=True)
    return (center * lax.rsqrt(var_est + EPS) * gain_row.astype(F32) + bias_row.astype(F32)).astype(BF)


def dot(a, b):
    return jnp.dot(a, b, preferred_element_type=F32)


def dot_nt(a, b):
    return lax.dot_general(a, b, NT, preferred_element_type=F32)


def iota(shape, dim):
    return lax.broadcasted_iota(jnp.int32, shape, dim)


def insert_slot(places, row, beams, pos, slots):
    last = (slots // 128) * 128
    tile = pos // 128

    def insert(start, size):
        for buf, cols in places:
            width = cols.shape[0]
            hit = iota((width, size), 1) == pos - start
            for i in range(beams):
                col = jnp.take_along_axis(cols[...], jnp.full((width, 128), row + i, jnp.int32), axis=1)[:, :size]
                span = (row + i, slice(None), pl.ds(start, size))
                buf[span] = jnp.where(hit, col.astype(BF), buf[span])

    @pl.when(tile * 128 < last)
    def _():
        insert(pl.multiple_of(tile * 128, 128), 128)

    if slots > last:
        @pl.when(tile * 128 >= last)
        def _():
            insert(last, slots - last)


def as_columns(rows):
    pad = jnp.zeros((128 - rows.shape[0], rows.shape[1]), F32)
    return jnp.concatenate([rows, pad], axis=0).T


def copies(pairs, sem):
    return [pltpu.make_async_copy(s, d, sem.at[i]) for i, (s, d) in enumerate(pairs)]


def self_kernel(layer, beams, h_hbm, pos_ref, g_hbm, b_hbm, wq_hbm, wk_hbm, wv_hbm, bq_hbm, bv_hbm, k_hbm, v_hbm, o_ref, ko_hbm, vo_hbm,
                h, g, b, wq, wk, wv, bq, bv, kbuf, vbuf, qs, kt, vt, os, psem, ksem, vsem, kosem, vosem):
    rows = h.shape[0]
    audios = rows // beams
    slots = kbuf.shape[-1]
    scale = 64 ** -0.25

    small = copies([(h_hbm, h), (g_hbm, g), (b_hbm, b), (wq_hbm.at[layer], wq), (wk_hbm.at[layer], wk), (wv_hbm.at[layer], wv), (bq_hbm, bq), (bv_hbm, bv)], psem)
    for c in small:
        c.start()

    def block(a, src, dst, sem):
        return pltpu.make_async_copy(src, dst, sem.at[a])

    def at(a):
        return pl.ds(a * beams, beams)

    def k_in(a):
        return block(a, k_hbm.at[layer, at(a)], kbuf.at[at(a)], ksem)

    def v_in(a):
        return block(a, v_hbm.at[layer, at(a)], vbuf.at[at(a)], vsem)

    def k_out(a):
        return block(a, kbuf.at[at(a)], ko_hbm.at[layer, at(a)], kosem)

    def v_out(a):
        return block(a, vbuf.at[at(a)], vo_hbm.at[layer, at(a)], vosem)

    @pl.loop(0, audios)
    def _(a):
        k_in(a).start()
        v_in(a).start()

    for c in small:
        c.wait()
    normed = layer_norm(h[...].astype(F32), g[0, layer:layer + 1, :], b[0, layer:layer + 1, :])
    qs[...] = ((dot_nt(normed, wq[...]) + bq[layer:layer + 1, :].astype(F32)) * scale).astype(BF).astype(F32)
    kt[...] = as_columns((dot_nt(normed, wk[...]) * scale).astype(BF).astype(F32))
    vt[...] = as_columns((dot_nt(normed, wv[...]) + bv[layer:layer + 1, :].astype(F32)).astype(BF).astype(F32))
    own = iota((8, qs.shape[1]), 1) // 64 == iota((8, qs.shape[1]), 0)
    pairs = audios // 2
    hold = pairs // 2

    def release(pair):
        for a in (pair * 2, pair * 2 + 1):
            k_out(a).start()
            v_out(a).start()

    @pl.loop(0, pairs)
    def _(pair):
        group = (pair * 2, pair * 2 + 1)
        for a in group:
            k_in(a).wait()
            v_in(a).wait()
        for a in group:
            insert_slot(((kbuf, kt), (vbuf, vt)), a * beams, beams, pos_ref[a * beams], slots)

        @pl.when(pair >= hold)
        def _():
            release(pair - hold)

        probs = []
        for a in group:
            scores = []
            for i in range(beams):
                q = jnp.broadcast_to(qs[pl.ds(a * beams + i, 1), :], own.shape)
                scores.append(dot(jnp.where(own, q, 0.0).astype(BF), kbuf[a * beams + i]))
            scores = jnp.concatenate(scores, axis=0)
            scores = jnp.where(iota(scores.shape, 1) <= pos_ref[a * beams], scores, -1e30)
            e = jnp.exp(scores - jnp.max(scores, axis=-1, keepdims=True))
            probs.append(e * (1.0 / jnp.sum(e, axis=-1, keepdims=True)))
        for a, p in zip(group, probs):
            for i in range(beams):
                r = a * beams + i
                out = dot_nt(p[i * 8:i * 8 + 8].astype(BF), vbuf[r])
                os[pl.ds(r, 1), :] = jnp.sum(jnp.where(own, out, 0.0), axis=0, keepdims=True)

    @pl.loop(pairs - hold, pairs)
    def _(pair):
        release(pair)

    o_ref[...] = os[...].astype(BF)

    @pl.loop(0, audios)
    def _(a):
        k_out(a).wait()
        v_out(a).wait()


def self_call(layer, beams, h, pos, g, b, wq, wk, wv, bq, bv, k, v):
    rows = h.shape[0]
    audios = rows // beams
    _, _, width, slots = k.shape
    args = (h, pos, g, b, wq, wk, wv, bq, bv, k, v)
    return pl.pallas_call(
        functools.partial(self_kernel, layer, beams),
        out_shape=(jax.ShapeDtypeStruct((rows, width), BF), jax.ShapeDtypeStruct(k.shape, BF), jax.ShapeDtypeStruct(v.shape, BF)),
        in_specs=[ANY, SMEM] + [ANY] * 9,
        out_specs=(VM, ANY, ANY),
        scratch_shapes=[
            pltpu.VMEM(h.shape, BF), pltpu.VMEM(g.shape, BF), pltpu.VMEM(b.shape, BF),
            pltpu.VMEM(wq.shape[1:], BF), pltpu.VMEM(wk.shape[1:], BF), pltpu.VMEM(wv.shape[1:], BF),
            pltpu.VMEM(bq.shape, BF), pltpu.VMEM(bv.shape, BF),
            pltpu.VMEM((rows, width, slots), BF), pltpu.VMEM((rows, width, slots), BF),
            pltpu.VMEM((rows, width), F32), pltpu.VMEM((width, 128), F32), pltpu.VMEM((width, 128), F32), pltpu.VMEM((rows, width), F32),
            DMA((8,)), DMA((audios,)), DMA((audios,)), DMA((audios,)), DMA((audios,)),
        ],
        cost_estimate=pl.CostEstimate(flops=0, bytes_accessed=4 * k.size, transcendentals=0),
        compiler_params=pltpu.CompilerParams(vmem_limit_bytes=VMEM_LIMIT),
        name=f"self_{layer}",
    )(*args)


def rest_kernel(beams, parts, o_hbm, h_hbm, pos_ref, g_hbm, b_hbm, wq_hbm, bq_hbm, wk_hbm, wv_hbm, bv_hbm, wo_hbm, bo_hbm, wc_hbm, bc_hbm, wco_hbm, bco_hbm, w1_hbm, b1_hbm, w2_hbm, b2_hbm,
                sk_hbm, sv_hbm, ck_hbm, cv_hbm, part_ref, out_ref, sk, sv, kn_ref, vn_ref,
                o, h, g, b, wq, bq, wk, wv, bv, wo, bo, wc, bc, wco, bco, w1, b1, w2, b2, ck, cv, hid, qr, kr, vr, os, snd, rcv,
                psem, wsem, skem, svem, ckem, cvem, ssem, rsem):
    rows = h.shape[0]
    audios = rows // beams
    group = audios // parts
    prow = rows // parts
    width = o.shape[1]
    heads = width // 64
    scale = 64 ** -0.25
    dp = lax.axis_index('dp')
    me = lax.axis_index('tp')
    mate = me + 1 - 2 * (me % 2)
    peers = ((me + 2) % 4, (mate + 2) % 4, mate)

    small = copies([(o_hbm, o), (h_hbm, h), (g_hbm, g), (b_hbm, b), (bq_hbm, bq), (bv_hbm, bv), (bo_hbm, bo), (bc_hbm, bc), (bco_hbm, bco), (b1_hbm, b1), (b2_hbm, b2)], psem)
    def layer_copies(layer, arrays, sem):
        return copies([(x.at[layer], y.at[layer]) for x, y in arrays], sem)

    early = layer_copies(0, ((wo_hbm, wo),), wsem.at[0])
    first = layer_copies(0, ((wc_hbm, wc), (wco_hbm, wco), (w1_hbm, w1), (w2_hbm, w2)), wsem.at[1])
    second = layer_copies(1, ((wo_hbm, wo), (wc_hbm, wc), (wco_hbm, wco), (w1_hbm, w1), (w2_hbm, w2)), wsem.at[2])
    extra = copies([(x.at[1], y) for x, y in ((wq_hbm, wq), (wk_hbm, wk), (wv_hbm, wv))], wsem.at[3])

    def cross_in(layer, a):
        return pltpu.make_async_copy(ck_hbm.at[layer, a], ck.at[a], ckem.at[a]), pltpu.make_async_copy(cv_hbm.at[layer, a], cv.at[a], cvem.at[a])

    def self_in(a):
        r = pl.ds(a * beams, beams)
        return pltpu.make_async_copy(sk_hbm.at[1, r], sk.at[r], skem.at[a]), pltpu.make_async_copy(sv_hbm.at[1, r], sv.at[r], svem.at[a])

    def start(pair):
        for c in pair:
            c.start()

    def wait(pair):
        for c in pair:
            c.wait()

    start(early)
    start(small)
    start(first[:1])

    @pl.loop(0, audios)
    def _(a):
        start(cross_in(0, a))

    start(first[1:])
    barrier = pltpu.get_barrier_semaphore()
    for peer in peers:
        pl.semaphore_signal(barrier, inc=1, device_id=(dp, peer), device_id_type=MESH)

    start(extra)
    start(second)

    @pl.loop(0, audios)
    def _(a):
        start(self_in(a))

    pl.semaphore_wait(barrier, 3)

    def sends(step, m):
        return [pltpu.make_async_remote_copy(snd.at[step, m], rcv.at[step, m, j], ssem.at[step, m, j], rsem.at[step, m, j], device_id=(dp, peer), device_id_type=MESH) for j, peer in enumerate(peers)]

    def push(step, m, part):
        snd[step, m] = part.astype(BF)
        start(sends(step, m))

    def total(step, m):
        wait(sends(step, m))
        mine = snd[step, m].astype(F32) + rcv[step, m, 2].astype(F32)
        return mine + (rcv[step, m, 0].astype(F32) + rcv[step, m, 1].astype(F32))

    def settle(m, update, bias):
        new = (hid[m].astype(F32) + update + bias.astype(F32)).astype(BF)
        hid[m] = new
        return new.astype(F32)

    def flags(shape, rule):
        return rule(iota(shape, 0), iota(shape, 1)).astype(F32).astype(BF)

    def pick(m):
        return flags((prow, rows), lambda r, c: c == r + m * prow)

    def cross_half(layer, m, wide):
        normed = layer_norm(wide, g[1, layer:layer + 1, :], b[1, layer:layer + 1, :])
        q = ((dot_nt(normed, wc[layer]) + bc[layer:layer + 1, :].astype(F32)) * scale).astype(BF)
        qr[m, 0:prow, :] = q.astype(F32)

        @pl.loop(0, group)
        def _(n):
            wait(cross_in(layer, m * group + n))

        own = iota((heads * 8, width), 1) // 64 == iota((heads * 8, width), 0) // 8

        def probs_of(n):
            qa = jnp.concatenate([qr[m, n * beams:n * beams + 8, :]] * heads, axis=0)
            scores = dot(jnp.where(own, qa, 0.0).astype(BF), ck[m * group + n])
            e = jnp.exp(scores - jnp.max(scores, axis=-1, keepdims=True))
            return (e * (1.0 / jnp.sum(e, axis=-1, keepdims=True))).astype(BF)

        def mix(n, p):
            out = jnp.where(own, dot_nt(p, cv[m * group + n]), 0.0)
            acc = out[0:8]
            for j in range(1, heads):
                acc = acc + out[j * 8:j * 8 + 8]
            os[m, n * beams:(n + 1) * beams, :] = acc[0:beams]

        p = probs_of(0)
        for n in range(group):
            p_next = probs_of(n + 1) if n + 1 < group else None
            mix(n, p)
            p = p_next

        if layer == 0:
            @pl.loop(0, group)
            def _(n):
                start(cross_in(1, m * group + n))
        return dot(os[m].astype(BF), wco[layer])

    def mlp_half(layer, m, wide):
        normed = layer_norm(wide, g[2, layer:layer + 1, :], b[2, layer:layer + 1, :])
        inner = dot(normed, w1[layer]) + b1[layer:layer + 1, :].astype(F32)
        inner = (0.5 * inner * (1.0 + lax.erf(inner * (2.0 ** -0.5)))).astype(BF)
        return dot(inner, w2[layer])

    def self_half(m, wide):
        normed = layer_norm(wide, g[0, 1:1 + 1, :], b[0, 1:1 + 1, :])
        q = ((dot_nt(normed, wq[...]) + bq[1:2, :].astype(F32)) * scale).astype(BF)
        k = (dot_nt(normed, wk[...]) * scale).astype(BF)
        v = (dot_nt(normed, wv[...]) + bv[1:2, :].astype(F32)).astype(BF)
        kn_ref[m] = k
        vn_ref[m] = v
        qr[m, 0:prow, :] = q.astype(F32)
        kr[m] = k.astype(F32)
        vr[m] = v.astype(F32)
        own = iota((8, width), 1) // 64 == iota((8, width), 0)

        @pl.loop(0, group)
        def _(n):
            wait(self_in(m * group + n))

        def row(ref, r):
            return jnp.where(own, jnp.broadcast_to(ref[m, r:r + 1, :], own.shape), 0.0)

        def probs_of(n):
            pos = pos_ref[(m * group + n) * beams]
            scores, fresh = [], []
            for j in range(beams):
                r = n * beams + j
                q8 = row(qr, r)
                scores.append(dot(q8.astype(BF), sk[m * prow + r]))
                fresh.append(jnp.sum(q8 * row(kr, r), axis=-1, keepdims=True))
            scores = jnp.concatenate(scores, axis=0)
            fresh = jnp.concatenate(fresh, axis=0)
            old = iota(scores.shape, 1) < pos
            scores = jnp.where(old, scores, -1e30)
            top = jnp.maximum(jnp.max(scores, axis=-1, keepdims=True), fresh)
            e = jnp.where(old, jnp.exp(scores - top), 0.0)
            e_new = jnp.exp(fresh - top)
            inv = 1.0 / (jnp.sum(e, axis=-1, keepdims=True) + e_new)
            return (e * inv), (e_new * inv).astype(BF).astype(F32)

        def mix(n, p, p_new):
            for j in range(beams):
                r = n * beams + j
                out = dot_nt(p[j * 8:j * 8 + 8].astype(BF), sv[m * prow + r])
                out = jnp.where(own, out, 0.0) + p_new[j * 8:j * 8 + 8] * row(vr, r)
                os[m, r:r + 1, :] = jnp.sum(out, axis=0, keepdims=True)

        p = probs_of(0)
        for n in range(group):
            p_next = probs_of(n + 1) if n + 1 < group else None
            mix(n, *p)
            p = p_next

        return dot(os[m].astype(BF), wo[1])

    wait(early)
    wait(small)
    for m in range(parts):
        push(0, m, dot(dot(pick(m), o[...]).astype(BF), wo[0]))
    for m in range(parts):
        hid[m] = dot(pick(m), h[...]).astype(BF)
        qr[m, prow:, :] = jnp.zeros((qr.shape[1] - prow, width), F32)
    wait(first)
    for m in range(parts):
        push(1, m, cross_half(0, m, settle(m, total(0, m), bo[0:1, :])))
    for m in range(parts):
        push(2, m, mlp_half(0, m, settle(m, total(1, m), bco[0:1, :])))
    wait(second)
    wait(extra)
    for m in range(parts):
        push(3, m, self_half(m, settle(m, total(2, m), b2[0:1, :])))
    for m in range(parts):
        push(4, m, cross_half(1, m, settle(m, total(3, m), bo[1:2, :])))
    final = jnp.zeros((rows, h.shape[1]), F32)
    resid = jnp.zeros((rows, h.shape[1]), F32)
    for m in range(parts):
        place = flags((rows, prow), lambda r, c: r == c + m * prow)
        wide = settle(m, total(4, m), bco[1:2, :])
        final = final + dot(place, mlp_half(1, m, wide).astype(BF))
        resid = resid + dot(place, hid[m])
    part_ref[...] = final.astype(BF)
    out_ref[...] = resid.astype(BF)


def rest_call(beams, parts, o, h, pos, g, b, wq, bq, wk, wv, bv, wo, bo, wc, bc, wco, bco, w1, b1, w2, b2, sk, sv, ck, cv):
    rows, dim = h.shape
    _, audios, width, frames = ck.shape
    slots = sk.shape[-1]
    prow = rows // parts
    args = (o, h, pos, g, b, wq, bq, wk, wv, bv, wo, bo, wc, bc, wco, bco, w1, b1, w2, b2, sk, sv, ck, cv)

    def whole(x):
        return pltpu.VMEM(x.shape, BF)

    def one(x):
        return pltpu.VMEM(x.shape[1:], BF)

    return pl.pallas_call(
        functools.partial(rest_kernel, beams, parts),
        out_shape=(pltpu.VMEM(h.shape, BF), pltpu.VMEM(h.shape, BF), pltpu.VMEM((rows, width, slots), BF), pltpu.VMEM((rows, width, slots), BF), pltpu.VMEM((parts, prow, width), BF), pltpu.VMEM((parts, prow, width), BF)),
        in_specs=[ANY, ANY, SMEM] + [ANY] * (len(args) - 3),
        out_specs=(VM,) * 6,
        scratch_shapes=[
            whole(o), whole(h), whole(g), whole(b), one(wq), whole(bq), one(wk), one(wv), whole(bv), whole(wo), whole(bo), whole(wc), whole(bc), whole(wco), whole(bco), whole(w1), whole(b1), whole(w2), whole(b2), one(ck), one(cv),
            pltpu.VMEM((parts, prow, dim), BF),
            pltpu.VMEM((parts, prow + 8, width), F32), pltpu.VMEM((parts, prow, width), F32), pltpu.VMEM((parts, prow, width), F32), pltpu.VMEM((parts, prow, width), F32),
            pltpu.VMEM((5, parts, prow, dim), BF), pltpu.VMEM((5, parts, 3, prow, dim), BF),
            DMA((11,)), DMA((4, 8)), DMA((audios,)), DMA((audios,)), DMA((audios,)), DMA((audios,)), DMA((5, parts, 3)), DMA((5, parts, 3)),
        ],
        compiler_params=pltpu.CompilerParams(collective_id=0, has_side_effects=True, vmem_limit_bytes=REST_LIMIT),
        name="rest",
    )(*args)


def write_kernel(layer, beams, pos_ref, kn, vn, sk_in, sv_in, ki_hbm, vi_hbm, ko_hbm, vo_hbm, sk, sv, kt, vt, kosem, vosem):
    parts, prow, width = kn.shape
    rows = parts * prow
    audios = rows // beams
    slots = sk.shape[-1]

    def k_out(a):
        r = pl.ds(a * beams, beams)
        return pltpu.make_async_copy(sk.at[r], ko_hbm.at[layer, r], kosem.at[a])

    def v_out(a):
        r = pl.ds(a * beams, beams)
        return pltpu.make_async_copy(sv.at[r], vo_hbm.at[layer, r], vosem.at[a])

    def columns(new):
        both = jnp.zeros((rows, width), F32)
        for m in range(parts):
            place = (iota((rows, prow), 0) == iota((rows, prow), 1) + m * prow).astype(F32).astype(BF)
            both = both + dot(place, new[m])
        return as_columns(both)

    kt[...] = columns(kn)
    vt[...] = columns(vn)

    @pl.loop(0, audios)
    def _(a):
        insert_slot(((sk, kt), (sv, vt)), a * beams, beams, pos_ref[a * beams], slots)
        k_out(a).start()
        v_out(a).start()

    @pl.loop(0, audios)
    def _(a):
        k_out(a).wait()
        v_out(a).wait()


def write_call(layer, beams, pos, kn, vn, sk, sv, ko, vo):
    rows, width, slots = sk.shape
    audios = rows // beams
    return pl.pallas_call(
        functools.partial(write_kernel, layer, beams),
        out_shape=(jax.ShapeDtypeStruct(ko.shape, BF), jax.ShapeDtypeStruct(vo.shape, BF), pltpu.VMEM(sk.shape, BF), pltpu.VMEM(sv.shape, BF)),
        in_specs=[SMEM, VM, VM, VM, VM, ANY, ANY],
        out_specs=(ANY, ANY, VM, VM),
        input_output_aliases={3: 2, 4: 3, 5: 0, 6: 1},
        cost_estimate=pl.CostEstimate(flops=0, bytes_accessed=4 * sk.size, transcendentals=0),
        scratch_shapes=[pltpu.VMEM((width, 128), F32), pltpu.VMEM((width, 128), F32), DMA((audios,)), DMA((audios,))],
        compiler_params=pltpu.CompilerParams(vmem_limit_bytes=4 * 1024 * 1024),
        name="write",
    )(pos, kn, vn, sk, sv, ko, vo)[:2]


def solution(mesh):
    cache_spec = P(None, 'dp', None, 'tp', None)
    col_spec = P(None, None, 'tp')
    row_spec = P(None, 'tp', None)
    vec_spec = P(None, 'tp')
    in_specs = (P('dp', None), P('dp'), cache_spec, cache_spec, cache_spec, cache_spec,
                P(), P(), col_spec, vec_spec, col_spec, col_spec, vec_spec, row_spec, P(), col_spec, vec_spec, row_spec, P(), col_spec, vec_spec, row_spec, P())

    def heads_first(cache):
        cache = jnp.transpose(cache, (0, 1, 3, 4, 2))
        return cache.reshape(cache.shape[:2] + (-1, cache.shape[-1]))

    def heads_last(cache, like):
        layers, batch, slots, heads, dim = like.shape
        return jnp.transpose(cache.reshape(layers, batch, heads, dim, slots), (0, 1, 4, 2, 3))

    def local_step(hidden, positions, self_keys, self_vals, cross_keys, cross_vals, g, b, wq, bq, wk, wv, bv, wo, bo, wc, bc, wco, bco, w1, b1, w2, b2):
        beams = hidden.shape[0] // cross_keys.shape[1]
        sk, sv, ck, cv = (heads_first(x) for x in (self_keys, self_vals, cross_keys, cross_vals))
        wq, wk, wv, wc = (jnp.swapaxes(w, 1, 2) for w in (wq, wk, wv, wc))
        g, b = (jnp.swapaxes(x, 0, 1) for x in (g, b))
        def hop(x, flip):
            return lax.ppermute(x, 'tp', [(i, i ^ flip) for i in range(4)])

        o, ko, vo = self_call(0, beams, hidden, positions, g, b, wq, wk, wv, bq, bv, sk, sv)
        part, hidden, sk1, sv1, kn, vn = rest_call(beams, 2, o, hidden, positions, g, b, wq, bq, wk, wv, bv, wo, bo, wc, bc, wco, bco, w1, b1, w2, b2, sk, sv, ck, cv)
        ko, vo = write_call(1, beams, positions, kn, vn, sk1, sv1, ko, vo)
        here, mate, far, diag = (x.astype(F32) for x in (part, hop(part, 1), hop(part, 2), hop(part, 3)))
        hidden = (hidden.astype(F32) + ((here + mate) + (far + diag)) + b2[1].astype(F32)).astype(BF)
        return hidden, heads_last(ko, self_keys), heads_last(vo, self_vals)

    return jax.shard_map(local_step, mesh=mesh, in_specs=in_specs, out_specs=(P('dp', None), cache_spec, cache_spec), check_vma=False)
```

```python
import functools

import jax
import jax.numpy as jnp
from jax import lax
from jax.experimental import pallas as pl
from jax.experimental.pallas import tpu as pltpu
from jax.sharding import PartitionSpec as P

EPS = 1e-5
BF = jnp.bfloat16
F32 = jnp.float32
MESH = pl.DeviceIdType.MESH
ANY = pl.BlockSpec(memory_space=pl.ANY)
VM = pl.BlockSpec(memory_space=pltpu.VMEM)
SMEM = pl.BlockSpec(memory_space=pltpu.SMEM)
DMA = pltpu.SemaphoreType.DMA
NT = (((1,), (1,)), ((), ()))
VMEM_LIMIT = 60 * 1024 * 1024
REST_LIMIT = 38 * 1024 * 1024


def layer_norm(wide, gain_row, bias_row):
    center = wide - jnp.mean(wide, axis=-1, keepdims=True)
    var_est = jnp.mean(center * center, axis=-1, keepdims=True)
    return (center * lax.rsqrt(var_est + EPS) * gain_row.astype(F32) + bias_row.astype(F32)).astype(BF)


def dot(a, b):
    return jnp.dot(a, b, preferred_element_type=F32)


def dot_nt(a, b):
    return lax.dot_general(a, b, NT, preferred_element_type=F32)


def iota(shape, dim):
    return lax.broadcasted_iota(jnp.int32, shape, dim)


def insert_slot(places, row, beams, pos, slots):
    last = (slots // 128) * 128
    tile = pos // 128

    def insert(start, size):
        for buf, cols in places:
            width = cols.shape[0]
            hit = iota((width, size), 1) == pos - start
            for i in range(beams):
                col = jnp.take_along_axis(cols[...], jnp.full((width, 128), row + i, jnp.int32), axis=1)[:, :size]
                span = (row + i, slice(None), pl.ds(start, size))
                buf[span] = jnp.where(hit, col.astype(BF), buf[span])

    @pl.when(tile * 128 < last)
    def _():
        insert(pl.multiple_of(tile * 128, 128), 128)

    if slots > last:
        @pl.when(tile * 128 >= last)
        def _():
            insert(last, slots - last)


def as_columns(rows):
    pad = jnp.zeros((128 - rows.shape[0], rows.shape[1]), F32)
    return jnp.concatenate([rows, pad], axis=0).T


def copies(pairs, sem):
    return [pltpu.make_async_copy(s, d, sem.at[i]) for i, (s, d) in enumerate(pairs)]


def self_kernel(layer, beams, h_hbm, pos_hbm, g_hbm, b_hbm, wq_hbm, wk_hbm, wv_hbm, bq_hbm, bv_hbm, k_hbm, v_hbm, o_hbm, ko_hbm, vo_hbm,
                h, pos_ref, g, b, wq, wk, wv, bq, bv, kbuf, vbuf, qs, kt, vt, os, o, psem, ksem, vsem, kosem, vosem):
    rows = h.shape[0]
    audios = rows // beams
    slots = kbuf.shape[-1]
    scale = 64 ** -0.25

    small = copies([(h_hbm, h), (g_hbm, g), (b_hbm, b), (wq_hbm.at[layer], wq), (wk_hbm.at[layer], wk), (wv_hbm.at[layer], wv), (bq_hbm, bq), (bv_hbm, bv), (pos_hbm, pos_ref)], psem)
    for c in small:
        c.start()

    def block(a, src, dst, sem):
        return pltpu.make_async_copy(src, dst, sem.at[a])

    def at(a):
        return pl.ds(a * beams, beams)

    def k_in(a):
        return block(a, k_hbm.at[layer, at(a)], kbuf.at[at(a)], ksem)

    def v_in(a):
        return block(a, v_hbm.at[layer, at(a)], vbuf.at[at(a)], vsem)

    def k_out(a):
        return block(a, kbuf.at[at(a)], ko_hbm.at[layer, at(a)], kosem)

    def v_out(a):
        return block(a, vbuf.at[at(a)], vo_hbm.at[layer, at(a)], vosem)

    @pl.loop(0, audios)
    def _(a):
        k_in(a).start()
        v_in(a).start()

    for c in small:
        c.wait()
    normed = layer_norm(h[...].astype(F32), g[0, layer:layer + 1, :], b[0, layer:layer + 1, :])
    qs[...] = ((dot_nt(normed, wq[...]) + bq[layer:layer + 1, :].astype(F32)) * scale).astype(BF).astype(F32)
    kt[...] = as_columns((dot_nt(normed, wk[...]) * scale).astype(BF).astype(F32))
    vt[...] = as_columns((dot_nt(normed, wv[...]) + bv[layer:layer + 1, :].astype(F32)).astype(BF).astype(F32))
    own = iota((8, qs.shape[1]), 1) // 64 == iota((8, qs.shape[1]), 0)
    pairs = audios // 2
    hold = pairs // 2

    def release(pair):
        for a in (pair * 2, pair * 2 + 1):
            k_out(a).start()
            v_out(a).start()

    @pl.loop(0, pairs)
    def _(pair):
        group = (pair * 2, pair * 2 + 1)
        for a in group:
            k_in(a).wait()
            v_in(a).wait()
        for a in group:
            insert_slot(((kbuf, kt), (vbuf, vt)), a * beams, beams, pos_ref[a * beams], slots)

        @pl.when(pair >= hold)
        def _():
            release(pair - hold)

        probs = []
        for a in group:
            scores = []
            for i in range(beams):
                q = jnp.broadcast_to(qs[pl.ds(a * beams + i, 1), :], own.shape)
                scores.append(dot(jnp.where(own, q, 0.0).astype(BF), kbuf[a * beams + i]))
            scores = jnp.concatenate(scores, axis=0)
            scores = jnp.where(iota(scores.shape, 1) <= pos_ref[a * beams], scores, -1e30)
            e = jnp.exp(scores - jnp.max(scores, axis=-1, keepdims=True))
            probs.append(e * (1.0 / jnp.sum(e, axis=-1, keepdims=True)))
        for a, p in zip(group, probs):
            for i in range(beams):
                r = a * beams + i
                out = dot_nt(p[i * 8:i * 8 + 8].astype(BF), vbuf[r])
                os[pl.ds(r, 1), :] = jnp.sum(jnp.where(own, out, 0.0), axis=0, keepdims=True)

    @pl.loop(pairs - hold, pairs)
    def _(pair):
        release(pair)

    o[...] = os[...].astype(BF)
    last = pltpu.make_async_copy(o, o_hbm, psem.at[0])
    last.start()

    @pl.loop(0, audios)
    def _(a):
        k_out(a).wait()
        v_out(a).wait()

    last.wait()


def self_call(layer, beams, h, pos, g, b, wq, wk, wv, bq, bv, k, v):
    rows = h.shape[0]
    audios = rows // beams
    _, _, width, slots = k.shape
    args = (h, pos, g, b, wq, wk, wv, bq, bv, k, v)
    return pl.pallas_call(
        functools.partial(self_kernel, layer, beams),
        out_shape=(jax.ShapeDtypeStruct((rows, width), BF), jax.ShapeDtypeStruct(k.shape, BF), jax.ShapeDtypeStruct(v.shape, BF)),
        in_specs=[ANY] * 11,
        out_specs=(ANY, ANY, ANY),
        scratch_shapes=[
            pltpu.VMEM(h.shape, BF), pltpu.SMEM(pos.shape, jnp.int32), pltpu.VMEM(g.shape, BF), pltpu.VMEM(b.shape, BF),
            pltpu.VMEM(wq.shape[1:], BF), pltpu.VMEM(wk.shape[1:], BF), pltpu.VMEM(wv.shape[1:], BF),
            pltpu.VMEM(bq.shape, BF), pltpu.VMEM(bv.shape, BF),
            pltpu.VMEM((rows, width, slots), BF), pltpu.VMEM((rows, width, slots), BF),
            pltpu.VMEM((rows, width), F32), pltpu.VMEM((width, 128), F32), pltpu.VMEM((width, 128), F32), pltpu.VMEM((rows, width), F32), pltpu.VMEM((rows, width), BF),
            DMA((9,)), DMA((audios,)), DMA((audios,)), DMA((audios,)), DMA((audios,)),
        ],
        cost_estimate=pl.CostEstimate(flops=0, bytes_accessed=4 * k.size, transcendentals=0),
        compiler_params=pltpu.CompilerParams(vmem_limit_bytes=VMEM_LIMIT),
        name=f"self_{layer}",
    )(*args)


def rest_kernel(beams, parts, o_hbm, h_hbm, pos_hbm, g_hbm, b_hbm, wq_hbm, bq_hbm, wk_hbm, wv_hbm, bv_hbm, wo_hbm, bo_hbm, wc_hbm, bc_hbm, wco_hbm, bco_hbm, w1_hbm, b1_hbm, w2_hbm, b2_hbm,
                sk_hbm, sv_hbm, ck_hbm, cv_hbm, part_ref, out_ref, sk, sv, kt, vt, spot,
                o, h, pos_ref, g, b, wq, bq, wk, wv, bv, wo, bo, wc, bc, wco, bco, w1, b1, w2, b2, ck, cv, hid, qr, kr, vr, kall, vall, os, snd, rcv,
                psem, wsem, skem, svem, ckem, cvem, ssem, rsem):
    rows = h.shape[0]
    audios = rows // beams
    group = audios // parts
    prow = rows // parts
    width = o.shape[1]
    heads = width // 64
    scale = 64 ** -0.25
    dp = lax.axis_index('dp')
    me = lax.axis_index('tp')
    mate = me + 1 - 2 * (me % 2)
    peers = ((me + 2) % 4, (mate + 2) % 4, mate)

    small = copies([(o_hbm, o), (h_hbm, h), (g_hbm, g), (b_hbm, b), (bq_hbm, bq), (bv_hbm, bv), (bo_hbm, bo), (bc_hbm, bc), (bco_hbm, bco), (b1_hbm, b1), (b2_hbm, b2), (pos_hbm, pos_ref)], psem)
    def layer_copies(layer, arrays, sem):
        return copies([(x.at[layer], y.at[layer]) for x, y in arrays], sem)

    early = layer_copies(0, ((wo_hbm, wo),), wsem.at[0])
    first = layer_copies(0, ((wc_hbm, wc), (wco_hbm, wco), (w1_hbm, w1), (w2_hbm, w2)), wsem.at[1])
    second = layer_copies(1, ((wo_hbm, wo), (wc_hbm, wc), (wco_hbm, wco), (w1_hbm, w1), (w2_hbm, w2)), wsem.at[2])
    extra = copies([(x.at[1], y) for x, y in ((wq_hbm, wq), (wk_hbm, wk), (wv_hbm, wv))], wsem.at[3])

    def cross_in(layer, a):
        return pltpu.make_async_copy(ck_hbm.at[layer, a], ck.at[a], ckem.at[a]), pltpu.make_async_copy(cv_hbm.at[layer, a], cv.at[a], cvem.at[a])

    def self_in(a):
        r = pl.ds(a * beams, beams)
        return pltpu.make_async_copy(sk_hbm.at[1, r], sk.at[r], skem.at[a]), pltpu.make_async_copy(sv_hbm.at[1, r], sv.at[r], svem.at[a])

    def start(pair):
        for c in pair:
            c.start()

    def wait(pair):
        for c in pair:
            c.wait()

    start(early)
    start(small)
    start(first[:1])

    @pl.loop(0, audios)
    def _(a):
        start(cross_in(0, a))

    start(first[1:])
    barrier = pltpu.get_barrier_semaphore()
    for peer in peers:
        pl.semaphore_signal(barrier, inc=1, device_id=(dp, peer), device_id_type=MESH)

    start(extra)
    start(second)

    @pl.loop(0, audios)
    def _(a):
        start(self_in(a))

    pl.semaphore_wait(barrier, 3)

    def sends(step, m):
        return [pltpu.make_async_remote_copy(snd.at[step, m], rcv.at[step, m, j], ssem.at[step, m, j], rsem.at[step, m, j], device_id=(dp, peer), device_id_type=MESH) for j, peer in enumerate(peers)]

    def push(step, m, part):
        snd[step, m] = part.astype(BF)
        start(sends(step, m))

    def total(step, m):
        wait(sends(step, m))
        mine = snd[step, m].astype(F32) + rcv[step, m, 2].astype(F32)
        return mine + (rcv[step, m, 0].astype(F32) + rcv[step, m, 1].astype(F32))

    def settle(m, update, bias):
        new = (hid[m].astype(F32) + update + bias.astype(F32)).astype(BF)
        hid[m] = new
        return new.astype(F32)

    def flags(shape, rule):
        return rule(iota(shape, 0), iota(shape, 1)).astype(F32).astype(BF)

    def pick(m):
        return flags((prow, rows), lambda r, c: c == r + m * prow)

    def cross_half(layer, m, wide):
        normed = layer_norm(wide, g[1, layer:layer + 1, :], b[1, layer:layer + 1, :])
        q = ((dot_nt(normed, wc[layer]) + bc[layer:layer + 1, :].astype(F32)) * scale).astype(BF)
        qr[m, 0:prow, :] = q.astype(F32)

        @pl.loop(0, group)
        def _(n):
            wait(cross_in(layer, m * group + n))

        own = iota((heads * 8, width), 1) // 64 == iota((heads * 8, width), 0) // 8

        def probs_of(n):
            qa = jnp.concatenate([qr[m, n * beams:n * beams + 8, :]] * heads, axis=0)
            scores = dot(jnp.where(own, qa, 0.0).astype(BF), ck[m * group + n])
            e = jnp.exp(scores - jnp.max(scores, axis=-1, keepdims=True))
            return (e * (1.0 / jnp.sum(e, axis=-1, keepdims=True))).astype(BF)

        def mix(n, p):
            out = jnp.where(own, dot_nt(p, cv[m * group + n]), 0.0)
            acc = out[0:8]
            for j in range(1, heads):
                acc = acc + out[j * 8:j * 8 + 8]
            os[m, n * beams:(n + 1) * beams, :] = acc[0:beams]

        p = probs_of(0)
        for n in range(group):
            p_next = probs_of(n + 1) if n + 1 < group else None
            mix(n, p)
            p = p_next

        if layer == 0:
            @pl.loop(0, group)
            def _(n):
                start(cross_in(1, m * group + n))
        return dot(os[m].astype(BF), wco[layer])

    def mlp_half(layer, m, wide):
        normed = layer_norm(wide, g[2, layer:layer + 1, :], b[2, layer:layer + 1, :])
        inner = dot(normed, w1[layer]) + b1[layer:layer + 1, :].astype(F32)
        inner = (0.5 * inner * (1.0 + lax.erf(inner * (2.0 ** -0.5)))).astype(BF)
        return dot(inner, w2[layer])

    def self_half(m, wide):
        normed = layer_norm(wide, g[0, 1:1 + 1, :], b[0, 1:1 + 1, :])
        q = ((dot_nt(normed, wq[...]) + bq[1:2, :].astype(F32)) * scale).astype(BF)
        k = (dot_nt(normed, wk[...]) * scale).astype(BF)
        v = (dot_nt(normed, wv[...]) + bv[1:2, :].astype(F32)).astype(BF)
        kall[m * prow:(m + 1) * prow, :] = k.astype(F32)
        vall[m * prow:(m + 1) * prow, :] = v.astype(F32)
        qr[m, 0:prow, :] = q.astype(F32)
        kr[m] = k.astype(F32)
        vr[m] = v.astype(F32)
        own = iota((8, width), 1) // 64 == iota((8, width), 0)

        @pl.loop(0, group)
        def _(n):
            wait(self_in(m * group + n))

        def row(ref, r):
            return jnp.where(own, jnp.broadcast_to(ref[m, r:r + 1, :], own.shape), 0.0)

        def probs_of(n):
            pos = pos_ref[(m * group + n) * beams]
            scores, fresh = [], []
            for j in range(beams):
                r = n * beams + j
                q8 = row(qr, r)
                scores.append(dot(q8.astype(BF), sk[m * prow + r]))
                fresh.append(jnp.sum(q8 * row(kr, r), axis=-1, keepdims=True))
            scores = jnp.concatenate(scores, axis=0)
            fresh = jnp.concatenate(fresh, axis=0)
            old = iota(scores.shape, 1) < pos
            scores = jnp.where(old, scores, -1e30)
            top = jnp.maximum(jnp.max(scores, axis=-1, keepdims=True), fresh)
            e = jnp.where(old, jnp.exp(scores - top), 0.0)
            e_new = jnp.exp(fresh - top)
            inv = 1.0 / (jnp.sum(e, axis=-1, keepdims=True) + e_new)
            return (e * inv), (e_new * inv).astype(BF).astype(F32)

        def mix(n, p, p_new):
            for j in range(beams):
                r = n * beams + j
                out = dot_nt(p[j * 8:j * 8 + 8].astype(BF), sv[m * prow + r])
                out = jnp.where(own, out, 0.0) + p_new[j * 8:j * 8 + 8] * row(vr, r)
                os[m, r:r + 1, :] = jnp.sum(out, axis=0, keepdims=True)

        p = probs_of(0)
        for n in range(group):
            p_next = probs_of(n + 1) if n + 1 < group else None
            mix(n, *p)
            p = p_next

        return dot(os[m].astype(BF), wo[1])

    wait(early)
    wait(small)
    for m in range(parts):
        push(0, m, dot(dot(pick(m), o[...]).astype(BF), wo[0]))
    for m in range(parts):
        hid[m] = dot(pick(m), h[...]).astype(BF)
        qr[m, prow:, :] = jnp.zeros((qr.shape[1] - prow, width), F32)
    kall[rows:, :] = jnp.zeros((128 - rows, width), F32)
    vall[rows:, :] = jnp.zeros((128 - rows, width), F32)
    wait(first)
    for m in range(parts):
        push(1, m, cross_half(0, m, settle(m, total(0, m), bo[0:1, :])))
    for m in range(parts):
        push(2, m, mlp_half(0, m, settle(m, total(1, m), bco[0:1, :])))
    wait(second)
    wait(extra)
    for m in range(parts):
        push(3, m, self_half(m, settle(m, total(2, m), b2[0:1, :])))
    kt[...] = kall[...].T
    vt[...] = vall[...].T
    for a in range(audios):
        spot[a] = jnp.full(spot.shape[1:], pos_ref[a * beams], jnp.int32)
    for m in range(parts):
        push(4, m, cross_half(1, m, settle(m, total(3, m), bo[1:2, :])))
    final = jnp.zeros((rows, h.shape[1]), F32)
    resid = jnp.zeros((rows, h.shape[1]), F32)
    for m in range(parts):
        place = flags((rows, prow), lambda r, c: r == c + m * prow)
        wide = settle(m, total(4, m), bco[1:2, :])
        final = final + dot(place, mlp_half(1, m, wide).astype(BF))
        resid = resid + dot(place, hid[m])
    part_ref[...] = final.astype(BF)
    out_ref[...] = resid.astype(BF)


def rest_call(beams, parts, o, h, pos, g, b, wq, bq, wk, wv, bv, wo, bo, wc, bc, wco, bco, w1, b1, w2, b2, sk, sv, ck, cv):
    rows, dim = h.shape
    _, audios, width, frames = ck.shape
    slots = sk.shape[-1]
    prow = rows // parts
    args = (o, h, pos, g, b, wq, bq, wk, wv, bv, wo, bo, wc, bc, wco, bco, w1, b1, w2, b2, sk, sv, ck, cv)

    def whole(x):
        return pltpu.VMEM(x.shape, BF)

    def one(x):
        return pltpu.VMEM(x.shape[1:], BF)

    return pl.pallas_call(
        functools.partial(rest_kernel, beams, parts),
        out_shape=(pltpu.VMEM(h.shape, BF), pltpu.VMEM(h.shape, BF), pltpu.VMEM((rows, width, slots), BF), pltpu.VMEM((rows, width, slots), BF), pltpu.VMEM((width, 128), F32), pltpu.VMEM((width, 128), F32), pltpu.VMEM((audios, 8, 128), jnp.int32)),
        in_specs=[ANY] * len(args),
        out_specs=(VM,) * 7,
        scratch_shapes=[
            whole(o), whole(h), pltpu.SMEM(pos.shape, jnp.int32), whole(g), whole(b), one(wq), whole(bq), one(wk), one(wv), whole(bv), whole(wo), whole(bo), whole(wc), whole(bc), whole(wco), whole(bco), whole(w1), whole(b1), whole(w2), whole(b2), one(ck), one(cv),
            pltpu.VMEM((parts, prow, dim), BF),
            pltpu.VMEM((parts, prow + 8, width), F32), pltpu.VMEM((parts, prow, width), F32), pltpu.VMEM((parts, prow, width), F32),
            pltpu.VMEM((128, width), F32), pltpu.VMEM((128, width), F32), pltpu.VMEM((parts, prow, width), F32),
            pltpu.VMEM((5, parts, prow, dim), BF), pltpu.VMEM((5, parts, 3, prow, dim), BF),
            DMA((12,)), DMA((4, 8)), DMA((audios,)), DMA((audios,)), DMA((audios,)), DMA((audios,)), DMA((5, parts, 3)), DMA((5, parts, 3)),
        ],
        compiler_params=pltpu.CompilerParams(collective_id=0, has_side_effects=True, vmem_limit_bytes=REST_LIMIT),
        name="rest",
    )(*args)


def write_kernel(layer, beams, spot, kt, vt, sk_in, sv_in, ki_hbm, vi_hbm, ko_hbm, vo_hbm, sk, sv, kosem, vosem):
    rows, width, slots = sk.shape
    audios = rows // beams

    def k_out(a):
        r = pl.ds(a * beams, beams)
        return pltpu.make_async_copy(sk.at[r], ko_hbm.at[layer, r], kosem.at[a])

    def v_out(a):
        r = pl.ds(a * beams, beams)
        return pltpu.make_async_copy(sv.at[r], vo_hbm.at[layer, r], vosem.at[a])

    @pl.loop(0, audios)
    def _(a):
        hits = [iota((width, min(128, slots - t)), 1) + t == spot[a, 0:1, :min(128, slots - t)] for t in range(0, slots, 128)]
        for buf, cols, out in ((sk, kt, k_out), (sv, vt, v_out)):
            for i in range(beams):
                r = a * beams + i
                col = jnp.take_along_axis(cols[...], jnp.full((width, 128), r, jnp.int32), axis=1).astype(BF)
                for n, hit in enumerate(hits):
                    size = hit.shape[1]
                    span = (r, slice(None), slice(n * 128, n * 128 + size))
                    buf[span] = jnp.where(hit, col[:, :size], buf[span])
            out(a).start()

    @pl.loop(0, audios)
    def _(a):
        k_out(a).wait()
        v_out(a).wait()


def write_call(layer, beams, spot, kt, vt, sk, sv, ko, vo):
    audios = sk.shape[0] // beams
    return pl.pallas_call(
        functools.partial(write_kernel, layer, beams),
        out_shape=(jax.ShapeDtypeStruct(ko.shape, BF), jax.ShapeDtypeStruct(vo.shape, BF), pltpu.VMEM(sk.shape, BF), pltpu.VMEM(sv.shape, BF)),
        in_specs=[VM, VM, VM, VM, VM, ANY, ANY],
        out_specs=(ANY, ANY, VM, VM),
        input_output_aliases={3: 2, 4: 3, 5: 0, 6: 1},
        cost_estimate=pl.CostEstimate(flops=0, bytes_accessed=4 * sk.size, transcendentals=0),
        scratch_shapes=[DMA((audios,)), DMA((audios,))],
        compiler_params=pltpu.CompilerParams(vmem_limit_bytes=4 * 1024 * 1024),
        name="write",
    )(spot, kt, vt, sk, sv, ko, vo)[:2]


def solution(mesh):
    cache_spec = P(None, 'dp', None, 'tp', None)
    col_spec = P(None, None, 'tp')
    row_spec = P(None, 'tp', None)
    vec_spec = P(None, 'tp')
    in_specs = (P('dp', None), P('dp'), cache_spec, cache_spec, cache_spec, cache_spec,
                P(), P(), col_spec, vec_spec, col_spec, col_spec, vec_spec, row_spec, P(), col_spec, vec_spec, row_spec, P(), col_spec, vec_spec, row_spec, P())

    def heads_first(cache):
        cache = jnp.transpose(cache, (0, 1, 3, 4, 2))
        return cache.reshape(cache.shape[:2] + (-1, cache.shape[-1]))

    def heads_last(cache, like):
        layers, batch, slots, heads, dim = like.shape
        return jnp.transpose(cache.reshape(layers, batch, heads, dim, slots), (0, 1, 4, 2, 3))

    def local_step(hidden, positions, self_keys, self_vals, cross_keys, cross_vals, g, b, wq, bq, wk, wv, bv, wo, bo, wc, bc, wco, bco, w1, b1, w2, b2):
        beams = hidden.shape[0] // cross_keys.shape[1]
        sk, sv, ck, cv = (heads_first(x) for x in (self_keys, self_vals, cross_keys, cross_vals))
        wq, wk, wv, wc = (jnp.swapaxes(w, 1, 2) for w in (wq, wk, wv, wc))
        g, b = (jnp.swapaxes(x, 0, 1) for x in (g, b))
        def hop(x, flip):
            return lax.ppermute(x, 'tp', [(i, i ^ flip) for i in range(4)])

        o, ko, vo = self_call(0, beams, hidden, positions, g, b, wq, wk, wv, bq, bv, sk, sv)
        part, hidden, sk1, sv1, kt, vt, spot = rest_call(beams, 3, o, hidden, positions, g, b, wq, bq, wk, wv, bv, wo, bo, wc, bc, wco, bco, w1, b1, w2, b2, sk, sv, ck, cv)
        ko, vo = write_call(1, beams, spot, kt, vt, sk1, sv1, ko, vo)
        here, mate, far, diag = (x.astype(F32) for x in (part, hop(part, 1), hop(part, 2), hop(part, 3)))
        hidden = (hidden.astype(F32) + ((here + mate) + (far + diag)) + b2[1].astype(F32)).astype(BF)
        return hidden, heads_last(ko, self_keys), heads_last(vo, self_vals)

    return jax.shard_map(local_step, mesh=mesh, in_specs=in_specs, out_specs=(P('dp', None), cache_spec, cache_spec), check_vma=False)
```

```python
import functools

import jax
import jax.numpy as jnp
from jax import lax
from jax.experimental import pallas as pl
from jax.experimental.pallas import tpu as pltpu
from jax.sharding import PartitionSpec as P

EPS = 1e-5
BF = jnp.bfloat16
F32 = jnp.float32
MESH = pl.DeviceIdType.MESH
ANY = pl.BlockSpec(memory_space=pl.ANY)
VM = pl.BlockSpec(memory_space=pltpu.VMEM)
SMEM = pl.BlockSpec(memory_space=pltpu.SMEM)
DMA = pltpu.SemaphoreType.DMA
NT = (((1,), (1,)), ((), ()))
VMEM_LIMIT = 60 * 1024 * 1024
REST_LIMIT = 38 * 1024 * 1024


def layer_norm(wide, gain_row, bias_row):
    center = wide - jnp.mean(wide, axis=-1, keepdims=True)
    var_est = jnp.mean(center * center, axis=-1, keepdims=True)
    return (center * lax.rsqrt(var_est + EPS) * gain_row.astype(F32) + bias_row.astype(F32)).astype(BF)


def dot(a, b):
    return jnp.dot(a, b, preferred_element_type=F32)


def dot_nt(a, b):
    return lax.dot_general(a, b, NT, preferred_element_type=F32)


def iota(shape, dim):
    return lax.broadcasted_iota(jnp.int32, shape, dim)


def insert_slot(places, row, beams, pos, slots):
    last = (slots // 128) * 128
    tile = pos // 128

    def insert(start, size):
        for buf, cols in places:
            width = cols.shape[0]
            hit = iota((width, size), 1) == pos - start
            for i in range(beams):
                col = jnp.take_along_axis(cols[...], jnp.full((width, 128), row + i, jnp.int32), axis=1)[:, :size]
                span = (row + i, slice(None), pl.ds(start, size))
                buf[span] = jnp.where(hit, col.astype(BF), buf[span])

    @pl.when(tile * 128 < last)
    def _():
        insert(pl.multiple_of(tile * 128, 128), 128)

    if slots > last:
        @pl.when(tile * 128 >= last)
        def _():
            insert(last, slots - last)


def as_columns(rows):
    pad = jnp.zeros((128 - rows.shape[0], rows.shape[1]), F32)
    return jnp.concatenate([rows, pad], axis=0).T


def copies(pairs, sem):
    return [pltpu.make_async_copy(s, d, sem.at[i]) for i, (s, d) in enumerate(pairs)]


def self_kernel(layer, beams, parts, h_hbm, pos_hbm, g_hbm, b_hbm, wq_hbm, wk_hbm, wv_hbm, bq_hbm, bv_hbm, k_hbm, v_hbm, o_hbm, ko_hbm, vo_hbm,
                h, pos_ref, g, b, wq, wk, wv, bq, bv, kbuf, vbuf, qs, kt, vt, os, o, psem, ksem, vsem, kosem, vosem):
    rows = h.shape[0]
    audios = rows // beams
    slots = kbuf.shape[-1]
    scale = 64 ** -0.25

    small = copies([(h_hbm, h), (g_hbm, g), (b_hbm, b), (wq_hbm.at[layer], wq), (wk_hbm.at[layer], wk), (wv_hbm.at[layer], wv), (bq_hbm, bq), (bv_hbm, bv), (pos_hbm, pos_ref)], psem)
    for c in small:
        c.start()

    def block(a, src, dst, sem):
        return pltpu.make_async_copy(src, dst, sem.at[a])

    def at(a):
        return pl.ds(a * beams, beams)

    def k_in(a):
        return block(a, k_hbm.at[layer, at(a)], kbuf.at[at(a)], ksem)

    def v_in(a):
        return block(a, v_hbm.at[layer, at(a)], vbuf.at[at(a)], vsem)

    def k_out(a):
        return block(a, kbuf.at[at(a)], ko_hbm.at[layer, at(a)], kosem)

    def v_out(a):
        return block(a, vbuf.at[at(a)], vo_hbm.at[layer, at(a)], vosem)

    @pl.loop(0, audios)
    def _(a):
        k_in(a).start()
        v_in(a).start()

    for c in small:
        c.wait()
    normed = layer_norm(h[...].astype(F32), g[0, layer:layer + 1, :], b[0, layer:layer + 1, :])
    qs[...] = ((dot_nt(normed, wq[...]) + bq[layer:layer + 1, :].astype(F32)) * scale).astype(BF).astype(F32)
    kt[...] = as_columns((dot_nt(normed, wk[...]) * scale).astype(BF).astype(F32))
    vt[...] = as_columns((dot_nt(normed, wv[...]) + bv[layer:layer + 1, :].astype(F32)).astype(BF).astype(F32))
    own = iota((8, qs.shape[1]), 1) // 64 == iota((8, qs.shape[1]), 0)
    pairs = audios // 2
    hold = pairs // 2

    def release(pair):
        for a in (pair * 2, pair * 2 + 1):
            k_out(a).start()
            v_out(a).start()

    @pl.loop(0, pairs)
    def _(pair):
        group = (pair * 2, pair * 2 + 1)
        for a in group:
            k_in(a).wait()
            v_in(a).wait()
        for a in group:
            insert_slot(((kbuf, kt), (vbuf, vt)), a * beams, beams, pos_ref[a * beams], slots)

        @pl.when(pair >= hold)
        def _():
            release(pair - hold)

        probs = []
        for a in group:
            scores = []
            for i in range(beams):
                q = jnp.broadcast_to(qs[pl.ds(a * beams + i, 1), :], own.shape)
                scores.append(dot(jnp.where(own, q, 0.0).astype(BF), kbuf[a * beams + i]))
            scores = jnp.concatenate(scores, axis=0)
            scores = jnp.where(iota(scores.shape, 1) <= pos_ref[a * beams], scores, -1e30)
            e = jnp.exp(scores - jnp.max(scores, axis=-1, keepdims=True))
            probs.append(e * (1.0 / jnp.sum(e, axis=-1, keepdims=True)))
        for a, p in zip(group, probs):
            for i in range(beams):
                r = a * beams + i
                out = dot_nt(p[i * 8:i * 8 + 8].astype(BF), vbuf[r])
                os[pl.ds(r, 1), :] = jnp.sum(jnp.where(own, out, 0.0), axis=0, keepdims=True)

    @pl.loop(pairs - hold, pairs)
    def _(pair):
        release(pair)

    for m in range(parts):
        o[m] = os[m * rows // parts:(m + 1) * rows // parts, :].astype(BF)
    last = pltpu.make_async_copy(o, o_hbm, psem.at[0])
    last.start()

    @pl.loop(0, audios)
    def _(a):
        k_out(a).wait()
        v_out(a).wait()

    last.wait()


def self_call(layer, beams, parts, h, pos, g, b, wq, wk, wv, bq, bv, k, v):
    rows = h.shape[0]
    audios = rows // beams
    _, _, width, slots = k.shape
    args = (h, pos, g, b, wq, wk, wv, bq, bv, k, v)
    return pl.pallas_call(
        functools.partial(self_kernel, layer, beams, parts),
        out_shape=(jax.ShapeDtypeStruct((parts, rows // parts, width), BF), jax.ShapeDtypeStruct(k.shape, BF), jax.ShapeDtypeStruct(v.shape, BF)),
        in_specs=[ANY] * 11,
        out_specs=(ANY, ANY, ANY),
        scratch_shapes=[
            pltpu.VMEM(h.shape, BF), pltpu.SMEM(pos.shape, jnp.int32), pltpu.VMEM(g.shape, BF), pltpu.VMEM(b.shape, BF),
            pltpu.VMEM(wq.shape[1:], BF), pltpu.VMEM(wk.shape[1:], BF), pltpu.VMEM(wv.shape[1:], BF),
            pltpu.VMEM(bq.shape, BF), pltpu.VMEM(bv.shape, BF),
            pltpu.VMEM((rows, width, slots), BF), pltpu.VMEM((rows, width, slots), BF),
            pltpu.VMEM((rows, width), F32), pltpu.VMEM((width, 128), F32), pltpu.VMEM((width, 128), F32), pltpu.VMEM((rows, width), F32), pltpu.VMEM((parts, rows // parts, width), BF),
            DMA((9,)), DMA((audios,)), DMA((audios,)), DMA((audios,)), DMA((audios,)),
        ],
        cost_estimate=pl.CostEstimate(flops=0, bytes_accessed=4 * k.size, transcendentals=0),
        compiler_params=pltpu.CompilerParams(vmem_limit_bytes=VMEM_LIMIT),
        name=f"self_{layer}",
    )(*args)


def rest_kernel(beams, parts, o_hbm, h_hbm, pos_hbm, g_hbm, b_hbm, wq_hbm, bq_hbm, wk_hbm, wv_hbm, bv_hbm, wo_hbm, bo_hbm, wc_hbm, bc_hbm, wco_hbm, bco_hbm, w1_hbm, b1_hbm, w2_hbm, b2_hbm,
                sk_hbm, sv_hbm, ck_hbm, cv_hbm, part_ref, out_ref, sk, sv, kt, vt, spot,
                o, h, pos_ref, g, b, wq, bq, wk, wv, bv, wo, bo, wc, bc, wco, bco, w1, b1, w2, b2, ck, cv, hid, qr, kr, vr, kall, vall, os, snd, rcv,
                psem, wsem, skem, svem, ckem, cvem, ssem, rsem):
    rows = h.shape[0]
    audios = rows // beams
    group = audios // parts
    prow = rows // parts
    width = o.shape[-1]
    heads = width // 64
    scale = 64 ** -0.25
    dp = lax.axis_index('dp')
    me = lax.axis_index('tp')
    mate = me + 1 - 2 * (me % 2)
    peers = ((me + 2) % 4, (mate + 2) % 4, mate)

    small = copies([(o_hbm, o), (h_hbm, h), (g_hbm, g), (b_hbm, b), (bq_hbm, bq), (bv_hbm, bv), (bo_hbm, bo), (bc_hbm, bc), (bco_hbm, bco), (b1_hbm, b1), (b2_hbm, b2), (pos_hbm, pos_ref)], psem)
    def layer_copies(layer, arrays, sem):
        return copies([(x.at[layer], y.at[layer]) for x, y in arrays], sem)

    early = layer_copies(0, ((wo_hbm, wo),), wsem.at[0])
    first = layer_copies(0, ((wc_hbm, wc), (wco_hbm, wco), (w1_hbm, w1), (w2_hbm, w2)), wsem.at[1])
    second = layer_copies(1, ((wo_hbm, wo), (wc_hbm, wc), (wco_hbm, wco), (w1_hbm, w1), (w2_hbm, w2)), wsem.at[2])
    extra = copies([(x.at[1], y) for x, y in ((wq_hbm, wq), (wk_hbm, wk), (wv_hbm, wv))], wsem.at[3])

    def cross_in(layer, a):
        return pltpu.make_async_copy(ck_hbm.at[layer, a], ck.at[a], ckem.at[a]), pltpu.make_async_copy(cv_hbm.at[layer, a], cv.at[a], cvem.at[a])

    def self_in(a):
        r = pl.ds(a * beams, beams)
        return pltpu.make_async_copy(sk_hbm.at[1, r], sk.at[r], skem.at[a]), pltpu.make_async_copy(sv_hbm.at[1, r], sv.at[r], svem.at[a])

    def start(pair):
        for c in pair:
            c.start()

    def wait(pair):
        for c in pair:
            c.wait()

    start(early)
    start(small)
    barrier = pltpu.get_barrier_semaphore()
    for peer in peers:
        pl.semaphore_signal(barrier, inc=1, device_id=(dp, peer), device_id_type=MESH)

    def sends(step, m):
        return [pltpu.make_async_remote_copy(snd.at[step, m], rcv.at[step, m, j], ssem.at[step, m, j], rsem.at[step, m, j], device_id=(dp, peer), device_id_type=MESH) for j, peer in enumerate(peers)]

    def push(step, m, part):
        snd[step, m] = part.astype(BF)
        start(sends(step, m))

    def total(step, m):
        wait(sends(step, m))
        mine = snd[step, m].astype(F32) + rcv[step, m, 2].astype(F32)
        return mine + (rcv[step, m, 0].astype(F32) + rcv[step, m, 1].astype(F32))

    def settle(m, update, bias):
        new = (hid[m].astype(F32) + update + bias.astype(F32)).astype(BF)
        hid[m] = new
        return new.astype(F32)

    def flags(shape, rule):
        return rule(iota(shape, 0), iota(shape, 1)).astype(F32).astype(BF)

    def pick(m):
        return flags((prow, rows), lambda r, c: c == r + m * prow)

    def cross_half(layer, m, wide):
        normed = layer_norm(wide, g[1, layer:layer + 1, :], b[1, layer:layer + 1, :])
        q = ((dot_nt(normed, wc[layer]) + bc[layer:layer + 1, :].astype(F32)) * scale).astype(BF)
        qr[m, 0:prow, :] = q.astype(F32)

        @pl.loop(0, group)
        def _(n):
            wait(cross_in(layer, m * group + n))

        own = iota((heads * 8, width), 1) // 64 == iota((heads * 8, width), 0) // 8

        def probs_of(n):
            qa = jnp.concatenate([qr[m, n * beams:n * beams + 8, :]] * heads, axis=0)
            scores = dot(jnp.where(own, qa, 0.0).astype(BF), ck[m * group + n])
            e = jnp.exp(scores - jnp.max(scores, axis=-1, keepdims=True))
            return (e * (1.0 / jnp.sum(e, axis=-1, keepdims=True))).astype(BF)

        def mix(n, p):
            out = jnp.where(own, dot_nt(p, cv[m * group + n]), 0.0)
            acc = out[0:8]
            for j in range(1, heads):
                acc = acc + out[j * 8:j * 8 + 8]
            os[m, n * beams:(n + 1) * beams, :] = acc[0:beams]

        probs = [probs_of(n) for n in range(group)]
        for n in range(group):
            mix(n, probs[n])

        if layer == 0:
            @pl.loop(0, group)
            def _(n):
                start(cross_in(1, m * group + n))
        return dot(os[m].astype(BF), wco[layer])

    def mlp_half(layer, m, wide):
        normed = layer_norm(wide, g[2, layer:layer + 1, :], b[2, layer:layer + 1, :])
        inner = dot(normed, w1[layer]) + b1[layer:layer + 1, :].astype(F32)
        inner = (0.5 * inner * (1.0 + lax.erf(inner * (2.0 ** -0.5)))).astype(BF)
        return dot(inner, w2[layer])

    def self_half(m, wide):
        normed = layer_norm(wide, g[0, 1:1 + 1, :], b[0, 1:1 + 1, :])
        q = ((dot_nt(normed, wq[...]) + bq[1:2, :].astype(F32)) * scale).astype(BF)
        k = (dot_nt(normed, wk[...]) * scale).astype(BF)
        v = (dot_nt(normed, wv[...]) + bv[1:2, :].astype(F32)).astype(BF)
        kall[m * prow:(m + 1) * prow, :] = k.astype(F32)
        vall[m * prow:(m + 1) * prow, :] = v.astype(F32)
        qr[m, 0:prow, :] = q.astype(F32)
        kr[m] = k.astype(F32)
        vr[m] = v.astype(F32)
        own = iota((8, width), 1) // 64 == iota((8, width), 0)

        @pl.loop(0, group)
        def _(n):
            wait(self_in(m * group + n))

        def row(ref, r):
            return jnp.where(own, jnp.broadcast_to(ref[m, r:r + 1, :], own.shape), 0.0)

        def probs_of(n):
            pos = pos_ref[(m * group + n) * beams]
            scores, fresh = [], []
            for j in range(beams):
                r = n * beams + j
                q8 = row(qr, r)
                scores.append(dot(q8.astype(BF), sk[m * prow + r]))
                fresh.append(jnp.sum(q8 * row(kr, r), axis=-1, keepdims=True))
            scores = jnp.concatenate(scores, axis=0)
            fresh = jnp.concatenate(fresh, axis=0)
            old = iota(scores.shape, 1) < pos
            scores = jnp.where(old, scores, -1e30)
            top = jnp.maximum(jnp.max(scores, axis=-1, keepdims=True), fresh)
            e = jnp.where(old, jnp.exp(scores - top), 0.0)
            e_new = jnp.exp(fresh - top)
            inv = 1.0 / (jnp.sum(e, axis=-1, keepdims=True) + e_new)
            return (e * inv), (e_new * inv).astype(BF).astype(F32)

        def mix(n, p, p_new):
            for j in range(beams):
                r = n * beams + j
                out = dot_nt(p[j * 8:j * 8 + 8].astype(BF), sv[m * prow + r])
                out = jnp.where(own, out, 0.0) + p_new[j * 8:j * 8 + 8] * row(vr, r)
                os[m, r:r + 1, :] = jnp.sum(out, axis=0, keepdims=True)

        probs = [probs_of(n) for n in range(group)]
        for n in range(group):
            mix(n, *probs[n])

        return dot(os[m].astype(BF), wo[1])

    wait(early)
    wait(small)
    shares = [dot(o[m], wo[0]) for m in range(parts)]
    pl.semaphore_wait(barrier, 3)
    for m in range(parts):
        push(0, m, shares[m])
    start(first[:1])

    @pl.loop(0, audios)
    def _(a):
        start(cross_in(0, a))

    start(first[1:])
    start(extra)
    start(second)

    @pl.loop(0, audios)
    def _(a):
        start(self_in(a))

    for m in range(parts):
        hid[m] = dot(pick(m), h[...]).astype(BF)
        qr[m, prow:, :] = jnp.zeros((qr.shape[1] - prow, width), F32)
    kall[rows:, :] = jnp.zeros((128 - rows, width), F32)
    vall[rows:, :] = jnp.zeros((128 - rows, width), F32)
    wait(first)
    for m in range(parts):
        push(1, m, cross_half(0, m, settle(m, total(0, m), bo[0:1, :])))
    for m in range(parts):
        push(2, m, mlp_half(0, m, settle(m, total(1, m), bco[0:1, :])))
    wait(second)
    wait(extra)
    for m in range(parts):
        push(3, m, self_half(m, settle(m, total(2, m), b2[0:1, :])))
    kt[...] = kall[...].T
    vt[...] = vall[...].T
    for a in range(audios):
        spot[a] = jnp.full(spot.shape[1:], pos_ref[a * beams], jnp.int32)
    for m in range(parts):
        push(4, m, cross_half(1, m, settle(m, total(3, m), bo[1:2, :])))
    final = jnp.zeros((rows, h.shape[1]), F32)
    resid = jnp.zeros((rows, h.shape[1]), F32)
    for m in range(parts):
        place = flags((rows, prow), lambda r, c: r == c + m * prow)
        wide = settle(m, total(4, m), bco[1:2, :])
        final = final + dot(place, mlp_half(1, m, wide).astype(BF))
        resid = resid + dot(place, hid[m])
    part_ref[...] = final.astype(BF)
    out_ref[...] = resid.astype(BF)


def rest_call(beams, parts, o, h, pos, g, b, wq, bq, wk, wv, bv, wo, bo, wc, bc, wco, bco, w1, b1, w2, b2, sk, sv, ck, cv):
    rows, dim = h.shape
    _, audios, width, frames = ck.shape
    slots = sk.shape[-1]
    prow = rows // parts
    args = (o, h, pos, g, b, wq, bq, wk, wv, bv, wo, bo, wc, bc, wco, bco, w1, b1, w2, b2, sk, sv, ck, cv)

    def whole(x):
        return pltpu.VMEM(x.shape, BF)

    def one(x):
        return pltpu.VMEM(x.shape[1:], BF)

    return pl.pallas_call(
        functools.partial(rest_kernel, beams, parts),
        out_shape=(pltpu.VMEM(h.shape, BF), pltpu.VMEM(h.shape, BF), pltpu.VMEM((rows, width, slots), BF), pltpu.VMEM((rows, width, slots), BF), pltpu.VMEM((width, 128), F32), pltpu.VMEM((width, 128), F32), pltpu.VMEM((audios, 8, 128), jnp.int32)),
        in_specs=[ANY] * len(args),
        out_specs=(VM,) * 7,
        scratch_shapes=[
            whole(o), whole(h), pltpu.SMEM(pos.shape, jnp.int32), whole(g), whole(b), one(wq), whole(bq), one(wk), one(wv), whole(bv), whole(wo), whole(bo), whole(wc), whole(bc), whole(wco), whole(bco), whole(w1), whole(b1), whole(w2), whole(b2), one(ck), one(cv),
            pltpu.VMEM((parts, prow, dim), BF),
            pltpu.VMEM((parts, prow + 8, width), F32), pltpu.VMEM((parts, prow, width), F32), pltpu.VMEM((parts, prow, width), F32),
            pltpu.VMEM((128, width), F32), pltpu.VMEM((128, width), F32), pltpu.VMEM((parts, prow, width), F32),
            pltpu.VMEM((5, parts, prow, dim), BF), pltpu.VMEM((5, parts, 3, prow, dim), BF),
            DMA((12,)), DMA((4, 8)), DMA((audios,)), DMA((audios,)), DMA((audios,)), DMA((audios,)), DMA((5, parts, 3)), DMA((5, parts, 3)),
        ],
        compiler_params=pltpu.CompilerParams(collective_id=0, has_side_effects=True, vmem_limit_bytes=REST_LIMIT),
        name="rest",
    )(*args)


def write_kernel(layer, beams, spot, kt, vt, sk_in, sv_in, ki_hbm, vi_hbm, ko_hbm, vo_hbm, sk, sv, kosem, vosem):
    rows, width, slots = sk.shape
    audios = rows // beams

    def k_out(a):
        r = pl.ds(a * beams, beams)
        return pltpu.make_async_copy(sk.at[r], ko_hbm.at[layer, r], kosem.at[a])

    def v_out(a):
        r = pl.ds(a * beams, beams)
        return pltpu.make_async_copy(sv.at[r], vo_hbm.at[layer, r], vosem.at[a])

    @pl.loop(0, audios)
    def _(a):
        hits = [iota((width, min(128, slots - t)), 1) + t == spot[a, 0:1, :min(128, slots - t)] for t in range(0, slots, 128)]
        for buf, cols, out in ((sk, kt, k_out), (sv, vt, v_out)):
            for i in range(beams):
                r = a * beams + i
                col = jnp.take_along_axis(cols[...], jnp.full((width, 128), r, jnp.int32), axis=1).astype(BF)
                for n, hit in enumerate(hits):
                    size = hit.shape[1]
                    span = (r, slice(None), slice(n * 128, n * 128 + size))
                    buf[span] = jnp.where(hit, col[:, :size], buf[span])
            out(a).start()

    @pl.loop(0, audios)
    def _(a):
        k_out(a).wait()
        v_out(a).wait()


def write_call(layer, beams, spot, kt, vt, sk, sv, ko, vo):
    audios = sk.shape[0] // beams
    return pl.pallas_call(
        functools.partial(write_kernel, layer, beams),
        out_shape=(jax.ShapeDtypeStruct(ko.shape, BF), jax.ShapeDtypeStruct(vo.shape, BF), pltpu.VMEM(sk.shape, BF), pltpu.VMEM(sv.shape, BF)),
        in_specs=[VM, VM, VM, VM, VM, ANY, ANY],
        out_specs=(ANY, ANY, VM, VM),
        input_output_aliases={3: 2, 4: 3, 5: 0, 6: 1},
        cost_estimate=pl.CostEstimate(flops=0, bytes_accessed=4 * sk.size, transcendentals=0),
        scratch_shapes=[DMA((audios,)), DMA((audios,))],
        compiler_params=pltpu.CompilerParams(vmem_limit_bytes=4 * 1024 * 1024),
        name="write",
    )(spot, kt, vt, sk, sv, ko, vo)[:2]


def solution(mesh):
    cache_spec = P(None, 'dp', None, 'tp', None)
    col_spec = P(None, None, 'tp')
    row_spec = P(None, 'tp', None)
    vec_spec = P(None, 'tp')
    in_specs = (P('dp', None), P('dp'), cache_spec, cache_spec, cache_spec, cache_spec,
                P(), P(), col_spec, vec_spec, col_spec, col_spec, vec_spec, row_spec, P(), col_spec, vec_spec, row_spec, P(), col_spec, vec_spec, row_spec, P())

    def heads_first(cache):
        cache = jnp.transpose(cache, (0, 1, 3, 4, 2))
        return cache.reshape(cache.shape[:2] + (-1, cache.shape[-1]))

    def heads_last(cache, like):
        layers, batch, slots, heads, dim = like.shape
        return jnp.transpose(cache.reshape(layers, batch, heads, dim, slots), (0, 1, 4, 2, 3))

    def local_step(hidden, positions, self_keys, self_vals, cross_keys, cross_vals, g, b, wq, bq, wk, wv, bv, wo, bo, wc, bc, wco, bco, w1, b1, w2, b2):
        beams = hidden.shape[0] // cross_keys.shape[1]
        sk, sv, ck, cv = (heads_first(x) for x in (self_keys, self_vals, cross_keys, cross_vals))
        wq, wk, wv, wc = (jnp.swapaxes(w, 1, 2) for w in (wq, wk, wv, wc))
        g, b = (jnp.swapaxes(x, 0, 1) for x in (g, b))
        def hop(x, flip):
            return lax.ppermute(x, 'tp', [(i, i ^ flip) for i in range(4)])

        parts = 2
        o, ko, vo = self_call(0, beams, parts, hidden, positions, g, b, wq, wk, wv, bq, bv, sk, sv)
        part, hidden, sk1, sv1, kt, vt, spot = rest_call(beams, parts, o, hidden, positions, g, b, wq, bq, wk, wv, bv, wo, bo, wc, bc, wco, bco, w1, b1, w2, b2, sk, sv, ck, cv)
        ko, vo = write_call(1, beams, spot, kt, vt, sk1, sv1, ko, vo)
        here, mate, far, diag = (x.astype(F32) for x in (part, hop(part, 1), hop(part, 2), hop(part, 3)))
        hidden = (hidden.astype(F32) + ((here + mate) + (far + diag)) + b2[1].astype(F32)).astype(BF)
        return hidden, heads_last(ko, self_keys), heads_last(vo, self_vals)

    return jax.shard_map(local_step, mesh=mesh, in_specs=in_specs, out_specs=(P('dp', None), cache_spec, cache_spec), check_vma=False)
```

```python
import functools

import jax
import jax.numpy as jnp
from jax import lax
from jax.experimental import pallas as pl
from jax.experimental.pallas import tpu as pltpu
from jax.sharding import PartitionSpec as P

EPS = 1e-5
BF = jnp.bfloat16
F32 = jnp.float32
MESH = pl.DeviceIdType.MESH
ANY = pl.BlockSpec(memory_space=pl.ANY)
VM = pl.BlockSpec(memory_space=pltpu.VMEM)
SMEM = pl.BlockSpec(memory_space=pltpu.SMEM)
DMA = pltpu.SemaphoreType.DMA
NT = (((1,), (1,)), ((), ()))
VMEM_LIMIT = 60 * 1024 * 1024
REST_LIMIT = 38 * 1024 * 1024


def layer_norm(wide, gain_row, bias_row):
    center = wide - jnp.mean(wide, axis=-1, keepdims=True)
    var_est = jnp.mean(center * center, axis=-1, keepdims=True)
    return (center * lax.rsqrt(var_est + EPS) * gain_row.astype(F32) + bias_row.astype(F32)).astype(BF)


def dot(a, b):
    return jnp.dot(a, b, preferred_element_type=F32)


def dot_nt(a, b):
    return lax.dot_general(a, b, NT, preferred_element_type=F32)


def iota(shape, dim):
    return lax.broadcasted_iota(jnp.int32, shape, dim)


def insert_slot(places, row, beams, pos, slots):
    last = (slots // 128) * 128
    tile = pos // 128

    def insert(start, size):
        for buf, cols in places:
            width = cols.shape[0]
            hit = iota((width, size), 1) == pos - start
            for i in range(beams):
                col = jnp.take_along_axis(cols[...], jnp.full((width, 128), row + i, jnp.int32), axis=1)[:, :size]
                span = (row + i, slice(None), pl.ds(start, size))
                buf[span] = jnp.where(hit, col.astype(BF), buf[span])

    @pl.when(tile * 128 < last)
    def _():
        insert(pl.multiple_of(tile * 128, 128), 128)

    if slots > last:
        @pl.when(tile * 128 >= last)
        def _():
            insert(last, slots - last)


def as_columns(rows):
    pad = jnp.zeros((128 - rows.shape[0], rows.shape[1]), F32)
    return jnp.concatenate([rows, pad], axis=0).T


def copies(pairs, sem):
    return [pltpu.make_async_copy(s, d, sem.at[i]) for i, (s, d) in enumerate(pairs)]


def self_kernel(layer, beams, parts, h_hbm, pos_hbm, g_hbm, b_hbm, wq_hbm, wk_hbm, wv_hbm, bq_hbm, bv_hbm, k_hbm, v_hbm, o_hbm, ko_hbm, vo_hbm,
                h, pos_ref, g, b, wq, wk, wv, bq, bv, kbuf, vbuf, qs, kt, vt, os, o, psem, ksem, vsem, kosem, vosem):
    rows = h.shape[0]
    audios = rows // beams
    slots = kbuf.shape[-1]
    scale = 64 ** -0.25

    small = copies([(h_hbm, h), (g_hbm, g), (b_hbm, b), (wq_hbm.at[layer], wq), (wk_hbm.at[layer], wk), (wv_hbm.at[layer], wv), (bq_hbm, bq), (bv_hbm, bv), (pos_hbm, pos_ref)], psem)
    for c in small:
        c.start()

    def block(a, src, dst, sem):
        return pltpu.make_async_copy(src, dst, sem.at[a])

    def at(a):
        return pl.ds(a * beams, beams)

    def k_in(a):
        return block(a, k_hbm.at[layer, at(a)], kbuf.at[at(a)], ksem)

    def v_in(a):
        return block(a, v_hbm.at[layer, at(a)], vbuf.at[at(a)], vsem)

    def k_out(a):
        return block(a, kbuf.at[at(a)], ko_hbm.at[layer, at(a)], kosem)

    def v_out(a):
        return block(a, vbuf.at[at(a)], vo_hbm.at[layer, at(a)], vosem)

    @pl.loop(0, audios)
    def _(a):
        k_in(a).start()
        v_in(a).start()

    for c in small:
        c.wait()
    normed = layer_norm(h[...].astype(F32), g[0, layer:layer + 1, :], b[0, layer:layer + 1, :])
    qs[...] = ((dot_nt(normed, wq[...]) + bq[layer:layer + 1, :].astype(F32)) * scale).astype(BF).astype(F32)
    kt[...] = as_columns((dot_nt(normed, wk[...]) * scale).astype(BF).astype(F32))
    vt[...] = as_columns((dot_nt(normed, wv[...]) + bv[layer:layer + 1, :].astype(F32)).astype(BF).astype(F32))
    own = iota((8, qs.shape[1]), 1) // 64 == iota((8, qs.shape[1]), 0)
    pairs = audios // 2
    hold = pairs // 2

    def release(pair):
        for a in (pair * 2, pair * 2 + 1):
            k_out(a).start()
            v_out(a).start()

    @pl.loop(0, pairs)
    def _(pair):
        group = (pair * 2, pair * 2 + 1)
        for a in group:
            k_in(a).wait()
            v_in(a).wait()
        for a in group:
            insert_slot(((kbuf, kt), (vbuf, vt)), a * beams, beams, pos_ref[a * beams], slots)

        @pl.when(pair >= hold)
        def _():
            release(pair - hold)

        probs = []
        for a in group:
            scores = []
            for i in range(beams):
                q = jnp.broadcast_to(qs[pl.ds(a * beams + i, 1), :], own.shape)
                scores.append(dot(jnp.where(own, q, 0.0).astype(BF), kbuf[a * beams + i]))
            scores = jnp.concatenate(scores, axis=0)
            scores = jnp.where(iota(scores.shape, 1) <= pos_ref[a * beams], scores, -1e30)
            e = jnp.exp(scores - jnp.max(scores, axis=-1, keepdims=True))
            probs.append(e * (1.0 / jnp.sum(e, axis=-1, keepdims=True)))
        for a, p in zip(group, probs):
            for i in range(beams):
                r = a * beams + i
                out = dot_nt(p[i * 8:i * 8 + 8].astype(BF), vbuf[r])
                os[pl.ds(r, 1), :] = jnp.sum(jnp.where(own, out, 0.0), axis=0, keepdims=True)

    @pl.loop(pairs - hold, pairs)
    def _(pair):
        release(pair)

    for m in range(parts):
        o[m] = os[m * rows // parts:(m + 1) * rows // parts, :].astype(BF)
    last = pltpu.make_async_copy(o, o_hbm, psem.at[0])
    last.start()

    @pl.loop(0, audios)
    def _(a):
        k_out(a).wait()
        v_out(a).wait()

    last.wait()


def self_call(layer, beams, parts, h, pos, g, b, wq, wk, wv, bq, bv, k, v):
    rows = h.shape[0]
    audios = rows // beams
    _, _, width, slots = k.shape
    args = (h, pos, g, b, wq, wk, wv, bq, bv, k, v)
    return pl.pallas_call(
        functools.partial(self_kernel, layer, beams, parts),
        out_shape=(jax.ShapeDtypeStruct((parts, rows // parts, width), BF), jax.ShapeDtypeStruct(k.shape, BF), jax.ShapeDtypeStruct(v.shape, BF)),
        in_specs=[ANY] * 11,
        out_specs=(ANY, ANY, ANY),
        scratch_shapes=[
            pltpu.VMEM(h.shape, BF), pltpu.SMEM(pos.shape, jnp.int32), pltpu.VMEM(g.shape, BF), pltpu.VMEM(b.shape, BF),
            pltpu.VMEM(wq.shape[1:], BF), pltpu.VMEM(wk.shape[1:], BF), pltpu.VMEM(wv.shape[1:], BF),
            pltpu.VMEM(bq.shape, BF), pltpu.VMEM(bv.shape, BF),
            pltpu.VMEM((rows, width, slots), BF), pltpu.VMEM((rows, width, slots), BF),
            pltpu.VMEM((rows, width), F32), pltpu.VMEM((width, 128), F32), pltpu.VMEM((width, 128), F32), pltpu.VMEM((rows, width), F32), pltpu.VMEM((parts, rows // parts, width), BF),
            DMA((9,)), DMA((audios,)), DMA((audios,)), DMA((audios,)), DMA((audios,)),
        ],
        cost_estimate=pl.CostEstimate(flops=0, bytes_accessed=4 * k.size, transcendentals=0),
        compiler_params=pltpu.CompilerParams(vmem_limit_bytes=VMEM_LIMIT),
        name=f"self_{layer}",
    )(*args)


def rest_kernel(beams, parts, o_hbm, h_hbm, pos_hbm, g_hbm, b_hbm, wq_hbm, bq_hbm, wk_hbm, wv_hbm, bv_hbm, wo_hbm, bo_hbm, wc_hbm, bc_hbm, wco_hbm, bco_hbm, w1_hbm, b1_hbm, w2_hbm, b2_hbm,
                wo_far, sk_hbm, sv_hbm, ck_hbm, cv_hbm, part_ref, out_ref, sk, sv, kt, vt, spot,
                o, h, pos_ref, g, b, wq, bq, wk, wv, bv, wo, bo, wc, bc, wco, bco, w1, b1, w2, b2, ck, cv, hid, qr, kr, vr, kall, vall, os, got, snd, rcv,
                psem, wsem, msem, mrsem, skem, svem, ckem, cvem, ssem, rsem):
    rows = h.shape[0]
    audios = rows // beams
    group = audios // parts
    prow = rows // parts
    width = o.shape[-1]
    heads = width // 64
    scale = 64 ** -0.25
    dp = lax.axis_index('dp')
    me = lax.axis_index('tp')
    mate = me + 1 - 2 * (me % 2)
    peers = ((me + 2) % 4, (mate + 2) % 4, mate)

    small = copies([(o_hbm, o), (h_hbm, h), (g_hbm, g), (b_hbm, b), (bq_hbm, bq), (bv_hbm, bv), (bo_hbm, bo), (bc_hbm, bc), (bco_hbm, bco), (b1_hbm, b1), (b2_hbm, b2), (pos_hbm, pos_ref)], psem)
    def layer_copies(layer, arrays, sem):
        return copies([(x.at[layer], y.at[layer]) for x, y in arrays], sem)

    first = layer_copies(0, ((wc_hbm, wc), (wco_hbm, wco), (w1_hbm, w1), (w2_hbm, w2)), wsem.at[1])
    second = layer_copies(1, ((wc_hbm, wc), (wco_hbm, wco), (w1_hbm, w1), (w2_hbm, w2)), wsem.at[2])
    early = copies([(wo_hbm.at[i], wo.at[i, 0]) for i in range(2)], wsem.at[0])

    def shared(layer):
        return [pltpu.make_async_remote_copy(src.at[layer], wo.at[layer, 1 + j], msem.at[layer, j], mrsem.at[layer, j], device_id=(dp, mate), device_id_type=MESH) for j, src in enumerate((wo_hbm, wo_far))]

    extra = copies([(x.at[1], y) for x, y in ((wq_hbm, wq), (wk_hbm, wk), (wv_hbm, wv))], wsem.at[3])

    def cross_in(layer, a):
        return pltpu.make_async_copy(ck_hbm.at[layer, a], ck.at[a], ckem.at[a]), pltpu.make_async_copy(cv_hbm.at[layer, a], cv.at[a], cvem.at[a])

    def self_in(a):
        r = pl.ds(a * beams, beams)
        return pltpu.make_async_copy(sk_hbm.at[1, r], sk.at[r], skem.at[a]), pltpu.make_async_copy(sv_hbm.at[1, r], sv.at[r], svem.at[a])

    def start(pair):
        for c in pair:
            c.start()

    def wait(pair):
        for c in pair:
            c.wait()

    start(small)
    start(early)
    barrier = pltpu.get_barrier_semaphore()
    for peer in peers:
        pl.semaphore_signal(barrier, inc=1, device_id=(dp, peer), device_id_type=MESH)

    def sends(step, m):
        return [pltpu.make_async_remote_copy(snd.at[step, m], rcv.at[step, m, j], ssem.at[step, m, j], rsem.at[step, m, j], device_id=(dp, peer), device_id_type=MESH) for j, peer in enumerate(peers)]

    def push(step, m, part):
        snd[step, m] = part.astype(BF)
        start(sends(step, m))

    def total(step, m):
        wait(sends(step, m))
        mine = snd[step, m].astype(F32) + rcv[step, m, 2].astype(F32)
        return mine + (rcv[step, m, 0].astype(F32) + rcv[step, m, 1].astype(F32))

    def heads_sends(step, m):
        return [pltpu.make_async_remote_copy(got.at[step, m, 3], got.at[step, m, j], ssem.at[step, m, j], rsem.at[step, m, j], device_id=(dp, peer), device_id_type=MESH) for j, peer in enumerate(peers)]

    def push_heads(step, m, out):
        got[step, m, 3] = out
        start(heads_sends(step, m))

    def project(step, m, layer):
        wait(heads_sends(step, m))
        here = dot(got[step, m, 3], wo[layer, 0]) + dot(got[step, m, 2], wo[layer, 1])
        return here + (dot(got[step, m, 0], wo_far[layer]) + dot(got[step, m, 1], wo[layer, 2]))

    def settle(m, update, bias):
        new = (hid[m].astype(F32) + update + bias.astype(F32)).astype(BF)
        hid[m] = new
        return new.astype(F32)

    def flags(shape, rule):
        return rule(iota(shape, 0), iota(shape, 1)).astype(F32).astype(BF)

    def pick(m):
        return flags((prow, rows), lambda r, c: c == r + m * prow)

    def cross_half(layer, m, wide):
        normed = layer_norm(wide, g[1, layer:layer + 1, :], b[1, layer:layer + 1, :])
        q = ((dot_nt(normed, wc[layer]) + bc[layer:layer + 1, :].astype(F32)) * scale).astype(BF)
        qr[m, 0:prow, :] = q.astype(F32)

        @pl.loop(0, group)
        def _(n):
            wait(cross_in(layer, m * group + n))

        own = iota((heads * 8, width), 1) // 64 == iota((heads * 8, width), 0) // 8

        def probs_of(n):
            qa = jnp.concatenate([qr[m, n * beams:n * beams + 8, :]] * heads, axis=0)
            scores = dot(jnp.where(own, qa, 0.0).astype(BF), ck[m * group + n])
            e = jnp.exp(scores - jnp.max(scores, axis=-1, keepdims=True))
            return (e * (1.0 / jnp.sum(e, axis=-1, keepdims=True))).astype(BF)

        def mix(n, p):
            out = jnp.where(own, dot_nt(p, cv[m * group + n]), 0.0)
            acc = out[0:8]
            for j in range(1, heads):
                acc = acc + out[j * 8:j * 8 + 8]
            os[m, n * beams:(n + 1) * beams, :] = acc[0:beams]

        probs = [probs_of(n) for n in range(group)]
        for n in range(group):
            mix(n, probs[n])

        if layer == 0:
            @pl.loop(0, group)
            def _(n):
                start(cross_in(1, m * group + n))
        return dot(os[m].astype(BF), wco[layer])

    def mlp_half(layer, m, wide):
        normed = layer_norm(wide, g[2, layer:layer + 1, :], b[2, layer:layer + 1, :])
        inner = dot(normed, w1[layer]) + b1[layer:layer + 1, :].astype(F32)
        inner = (0.5 * inner * (1.0 + lax.erf(inner * (2.0 ** -0.5)))).astype(BF)
        return dot(inner, w2[layer])

    def self_half(m, wide):
        normed = layer_norm(wide, g[0, 1:1 + 1, :], b[0, 1:1 + 1, :])
        q = ((dot_nt(normed, wq[...]) + bq[1:2, :].astype(F32)) * scale).astype(BF)
        k = (dot_nt(normed, wk[...]) * scale).astype(BF)
        v = (dot_nt(normed, wv[...]) + bv[1:2, :].astype(F32)).astype(BF)
        kall[m * prow:(m + 1) * prow, :] = k.astype(F32)
        vall[m * prow:(m + 1) * prow, :] = v.astype(F32)
        qr[m, 0:prow, :] = q.astype(F32)
        kr[m] = k.astype(F32)
        vr[m] = v.astype(F32)
        own = iota((8, width), 1) // 64 == iota((8, width), 0)

        @pl.loop(0, group)
        def _(n):
            wait(self_in(m * group + n))

        def row(ref, r):
            return jnp.where(own, jnp.broadcast_to(ref[m, r:r + 1, :], own.shape), 0.0)

        def probs_of(n):
            pos = pos_ref[(m * group + n) * beams]
            scores, fresh = [], []
            for j in range(beams):
                r = n * beams + j
                q8 = row(qr, r)
                scores.append(dot(q8.astype(BF), sk[m * prow + r]))
                fresh.append(jnp.sum(q8 * row(kr, r), axis=-1, keepdims=True))
            scores = jnp.concatenate(scores, axis=0)
            fresh = jnp.concatenate(fresh, axis=0)
            old = iota(scores.shape, 1) < pos
            scores = jnp.where(old, scores, -1e30)
            top = jnp.maximum(jnp.max(scores, axis=-1, keepdims=True), fresh)
            e = jnp.where(old, jnp.exp(scores - top), 0.0)
            e_new = jnp.exp(fresh - top)
            inv = 1.0 / (jnp.sum(e, axis=-1, keepdims=True) + e_new)
            return (e * inv), (e_new * inv).astype(BF).astype(F32)

        def mix(n, p, p_new):
            for j in range(beams):
                r = n * beams + j
                out = dot_nt(p[j * 8:j * 8 + 8].astype(BF), sv[m * prow + r])
                out = jnp.where(own, out, 0.0) + p_new[j * 8:j * 8 + 8] * row(vr, r)
                os[m, r:r + 1, :] = jnp.sum(out, axis=0, keepdims=True)

        probs = [probs_of(n) for n in range(group)]
        for n in range(group):
            mix(n, *probs[n])

        return os[m].astype(BF)

    wait(small)
    pl.semaphore_wait(barrier, 3)
    for m in range(parts):
        push_heads(0, m, o[m])
    start(shared(0))
    start(first[:1])

    @pl.loop(0, audios)
    def _(a):
        start(cross_in(0, a))

    start(first[1:])
    start(extra)
    start(shared(1))
    start(second)

    @pl.loop(0, audios)
    def _(a):
        start(self_in(a))

    for m in range(parts):
        hid[m] = dot(pick(m), h[...]).astype(BF)
        qr[m, prow:, :] = jnp.zeros((qr.shape[1] - prow, width), F32)
    kall[rows:, :] = jnp.zeros((128 - rows, width), F32)
    vall[rows:, :] = jnp.zeros((128 - rows, width), F32)
    wait(early)
    wait(shared(0))
    wait(first)
    for m in range(parts):
        push(1, m, cross_half(0, m, settle(m, project(0, m, 0), bo[0:1, :])))
    for m in range(parts):
        push(2, m, mlp_half(0, m, settle(m, total(1, m), bco[0:1, :])))
    wait(second)
    wait(extra)
    for m in range(parts):
        push_heads(3, m, self_half(m, settle(m, total(2, m), b2[0:1, :])))
    kt[...] = kall[...].T
    vt[...] = vall[...].T
    for a in range(audios):
        spot[a] = jnp.full(spot.shape[1:], pos_ref[a * beams], jnp.int32)
    wait(shared(1))
    for m in range(parts):
        push(4, m, cross_half(1, m, settle(m, project(3, m, 1), bo[1:2, :])))
    final = jnp.zeros((rows, h.shape[1]), F32)
    resid = jnp.zeros((rows, h.shape[1]), F32)
    for m in range(parts):
        place = flags((rows, prow), lambda r, c: r == c + m * prow)
        wide = settle(m, total(4, m), bco[1:2, :])
        final = final + dot(place, mlp_half(1, m, wide).astype(BF))
        resid = resid + dot(place, hid[m])
    part_ref[...] = final.astype(BF)
    out_ref[...] = resid.astype(BF)


def rest_call(beams, parts, o, h, pos, g, b, wq, bq, wk, wv, bv, wo, bo, wc, bc, wco, bco, w1, b1, w2, b2, wo_far, sk, sv, ck, cv):
    rows, dim = h.shape
    _, audios, width, frames = ck.shape
    slots = sk.shape[-1]
    prow = rows // parts
    args = (o, h, pos, g, b, wq, bq, wk, wv, bv, wo, bo, wc, bc, wco, bco, w1, b1, w2, b2, wo_far, sk, sv, ck, cv)

    def whole(x):
        return pltpu.VMEM(x.shape, BF)

    def one(x):
        return pltpu.VMEM(x.shape[1:], BF)

    return pl.pallas_call(
        functools.partial(rest_kernel, beams, parts),
        out_shape=(pltpu.VMEM(h.shape, BF), pltpu.VMEM(h.shape, BF), pltpu.VMEM((rows, width, slots), BF), pltpu.VMEM((rows, width, slots), BF), pltpu.VMEM((width, 128), F32), pltpu.VMEM((width, 128), F32), pltpu.VMEM((audios, 8, 128), jnp.int32)),
        in_specs=[ANY] * (len(args) - 5) + [VM] + [ANY] * 4,
        out_specs=(VM,) * 7,
        scratch_shapes=[
            whole(o), whole(h), pltpu.SMEM(pos.shape, jnp.int32), whole(g), whole(b), one(wq), whole(bq), one(wk), one(wv), whole(bv), pltpu.VMEM((2, 3, width, dim), BF), whole(bo), whole(wc), whole(bc), whole(wco), whole(bco), whole(w1), whole(b1), whole(w2), whole(b2), one(ck), one(cv),
            pltpu.VMEM((parts, prow, dim), BF),
            pltpu.VMEM((parts, prow + 8, width), F32), pltpu.VMEM((parts, prow, width), F32), pltpu.VMEM((parts, prow, width), F32),
            pltpu.VMEM((128, width), F32), pltpu.VMEM((128, width), F32), pltpu.VMEM((parts, prow, width), F32),
            pltpu.VMEM((5, parts, 4, prow, width), BF), pltpu.VMEM((5, parts, prow, dim), BF), pltpu.VMEM((5, parts, 3, prow, dim), BF),
            DMA((12,)), DMA((4, 8)), DMA((2, 2)), DMA((2, 2)), DMA((audios,)), DMA((audios,)), DMA((audios,)), DMA((audios,)), DMA((5, parts, 3)), DMA((5, parts, 3)),
        ],
        compiler_params=pltpu.CompilerParams(collective_id=0, has_side_effects=True, vmem_limit_bytes=REST_LIMIT),
        name="rest",
    )(*args)


def write_kernel(layer, beams, spot, kt, vt, sk_in, sv_in, ki_hbm, vi_hbm, ko_hbm, vo_hbm, sk, sv, kosem, vosem):
    rows, width, slots = sk.shape
    audios = rows // beams

    def k_out(a):
        r = pl.ds(a * beams, beams)
        return pltpu.make_async_copy(sk.at[r], ko_hbm.at[layer, r], kosem.at[a])

    def v_out(a):
        r = pl.ds(a * beams, beams)
        return pltpu.make_async_copy(sv.at[r], vo_hbm.at[layer, r], vosem.at[a])

    @pl.loop(0, audios)
    def _(a):
        hits = [iota((width, min(128, slots - t)), 1) + t == spot[a, 0:1, :min(128, slots - t)] for t in range(0, slots, 128)]
        for buf, cols, out in ((sk, kt, k_out), (sv, vt, v_out)):
            for i in range(beams):
                r = a * beams + i
                col = jnp.take_along_axis(cols[...], jnp.full((width, 128), r, jnp.int32), axis=1).astype(BF)
                for n, hit in enumerate(hits):
                    size = hit.shape[1]
                    span = (r, slice(None), slice(n * 128, n * 128 + size))
                    buf[span] = jnp.where(hit, col[:, :size], buf[span])
            out(a).start()

    @pl.loop(0, audios)
    def _(a):
        k_out(a).wait()
        v_out(a).wait()


def write_call(layer, beams, spot, kt, vt, sk, sv, ko, vo):
    audios = sk.shape[0] // beams
    return pl.pallas_call(
        functools.partial(write_kernel, layer, beams),
        out_shape=(jax.ShapeDtypeStruct(ko.shape, BF), jax.ShapeDtypeStruct(vo.shape, BF), pltpu.VMEM(sk.shape, BF), pltpu.VMEM(sv.shape, BF)),
        in_specs=[VM, VM, VM, VM, VM, ANY, ANY],
        out_specs=(ANY, ANY, VM, VM),
        input_output_aliases={3: 2, 4: 3, 5: 0, 6: 1},
        cost_estimate=pl.CostEstimate(flops=0, bytes_accessed=4 * sk.size, transcendentals=0),
        scratch_shapes=[DMA((audios,)), DMA((audios,))],
        compiler_params=pltpu.CompilerParams(vmem_limit_bytes=4 * 1024 * 1024),
        name="write",
    )(spot, kt, vt, sk, sv, ko, vo)[:2]


def solution(mesh):
    cache_spec = P(None, 'dp', None, 'tp', None)
    col_spec = P(None, None, 'tp')
    row_spec = P(None, 'tp', None)
    vec_spec = P(None, 'tp')
    in_specs = (P('dp', None), P('dp'), cache_spec, cache_spec, cache_spec, cache_spec,
                P(), P(), col_spec, vec_spec, col_spec, col_spec, vec_spec, row_spec, P(), col_spec, vec_spec, row_spec, P(), col_spec, vec_spec, row_spec, P())

    def heads_first(cache):
        cache = jnp.transpose(cache, (0, 1, 3, 4, 2))
        return cache.reshape(cache.shape[:2] + (-1, cache.shape[-1]))

    def heads_last(cache, like):
        layers, batch, slots, heads, dim = like.shape
        return jnp.transpose(cache.reshape(layers, batch, heads, dim, slots), (0, 1, 4, 2, 3))

    def local_step(hidden, positions, self_keys, self_vals, cross_keys, cross_vals, g, b, wq, bq, wk, wv, bv, wo, bo, wc, bc, wco, bco, w1, b1, w2, b2):
        beams = hidden.shape[0] // cross_keys.shape[1]
        sk, sv, ck, cv = (heads_first(x) for x in (self_keys, self_vals, cross_keys, cross_vals))
        wq, wk, wv, wc = (jnp.swapaxes(w, 1, 2) for w in (wq, wk, wv, wc))
        g, b = (jnp.swapaxes(x, 0, 1) for x in (g, b))
        def hop(x, flip):
            return lax.ppermute(x, 'tp', [(i, i ^ flip) for i in range(4)])

        parts = 2
        wo_far = pltpu.with_memory_space_constraint(hop(wo, 2), pltpu.VMEM)
        o, ko, vo = self_call(0, beams, parts, hidden, positions, g, b, wq, wk, wv, bq, bv, sk, sv)
        part, hidden, sk1, sv1, kt, vt, spot = rest_call(beams, parts, o, hidden, positions, g, b, wq, bq, wk, wv, bv, wo, bo, wc, bc, wco, bco, w1, b1, w2, b2, wo_far, sk, sv, ck, cv)
        ko, vo = write_call(1, beams, spot, kt, vt, sk1, sv1, ko, vo)
        here, mate, far, diag = (x.astype(F32) for x in (part, hop(part, 1), hop(part, 2), hop(part, 3)))
        hidden = (hidden.astype(F32) + ((here + mate) + (far + diag)) + b2[1].astype(F32)).astype(BF)
        return hidden, heads_last(ko, self_keys), heads_last(vo, self_vals)

    return jax.shard_map(local_step, mesh=mesh, in_specs=in_specs, out_specs=(P('dp', None), cache_spec, cache_spec), check_vma=False)
```

```python
import functools

import jax
import jax.numpy as jnp
from jax import lax
from jax.experimental import pallas as pl
from jax.experimental.pallas import tpu as pltpu
from jax.sharding import PartitionSpec as P

EPS = 1e-5
BF = jnp.bfloat16
F32 = jnp.float32
MESH = pl.DeviceIdType.MESH
ANY = pl.BlockSpec(memory_space=pl.ANY)
VM = pl.BlockSpec(memory_space=pltpu.VMEM)
SMEM = pl.BlockSpec(memory_space=pltpu.SMEM)
DMA = pltpu.SemaphoreType.DMA
NT = (((1,), (1,)), ((), ()))
VMEM_LIMIT = 60 * 1024 * 1024
REST_LIMIT = 38 * 1024 * 1024


def layer_norm(wide, gain_row, bias_row):
    center = wide - jnp.mean(wide, axis=-1, keepdims=True)
    var_est = jnp.mean(center * center, axis=-1, keepdims=True)
    return (center * lax.rsqrt(var_est + EPS) * gain_row.astype(F32) + bias_row.astype(F32)).astype(BF)


def dot(a, b):
    return jnp.dot(a, b, preferred_element_type=F32)


def dot_nt(a, b):
    return lax.dot_general(a, b, NT, preferred_element_type=F32)


def iota(shape, dim):
    return lax.broadcasted_iota(jnp.int32, shape, dim)


def insert_slot(places, row, beams, pos, slots):
    last = (slots // 128) * 128
    tile = pos // 128

    def insert(start, size):
        for buf, cols in places:
            width = cols.shape[0]
            hit = iota((width, size), 1) == pos - start
            for i in range(beams):
                col = jnp.take_along_axis(cols[...], jnp.full((width, 128), row + i, jnp.int32), axis=1)[:, :size]
                span = (row + i, slice(None), pl.ds(start, size))
                buf[span] = jnp.where(hit, col.astype(BF), buf[span])

    @pl.when(tile * 128 < last)
    def _():
        insert(pl.multiple_of(tile * 128, 128), 128)

    if slots > last:
        @pl.when(tile * 128 >= last)
        def _():
            insert(last, slots - last)


def as_columns(rows):
    pad = jnp.zeros((128 - rows.shape[0], rows.shape[1]), F32)
    return jnp.concatenate([rows, pad], axis=0).T


def copies(pairs, sem):
    return [pltpu.make_async_copy(s, d, sem.at[i]) for i, (s, d) in enumerate(pairs)]


def self_kernel(layer, beams, parts, h_hbm, pos_hbm, g_hbm, b_hbm, wq_hbm, wk_hbm, wv_hbm, bq_hbm, bv_hbm, k_hbm, v_hbm, o_hbm, ko_hbm, vo_hbm,
                h, pos_ref, g, b, wq, wk, wv, bq, bv, kbuf, vbuf, qs, kt, vt, os, o, psem, ksem, vsem, kosem, vosem):
    rows = h.shape[0]
    audios = rows // beams
    slots = kbuf.shape[-1]
    scale = 64 ** -0.25

    small = copies([(h_hbm, h), (g_hbm, g), (b_hbm, b), (wq_hbm.at[layer], wq), (wk_hbm.at[layer], wk), (wv_hbm.at[layer], wv), (bq_hbm, bq), (bv_hbm, bv), (pos_hbm, pos_ref)], psem)
    for c in small:
        c.start()

    def block(a, src, dst, sem):
        return pltpu.make_async_copy(src, dst, sem.at[a])

    def at(a):
        return pl.ds(a * beams, beams)

    def k_in(a):
        return block(a, k_hbm.at[layer, at(a)], kbuf.at[at(a)], ksem)

    def v_in(a):
        return block(a, v_hbm.at[layer, at(a)], vbuf.at[at(a)], vsem)

    def k_out(a):
        return block(a, kbuf.at[at(a)], ko_hbm.at[layer, at(a)], kosem)

    def v_out(a):
        return block(a, vbuf.at[at(a)], vo_hbm.at[layer, at(a)], vosem)

    @pl.loop(0, audios)
    def _(a):
        k_in(a).start()
        v_in(a).start()

    for c in small:
        c.wait()
    normed = layer_norm(h[...].astype(F32), g[0, layer:layer + 1, :], b[0, layer:layer + 1, :])
    qs[...] = ((dot_nt(normed, wq[...]) + bq[layer:layer + 1, :].astype(F32)) * scale).astype(BF).astype(F32)
    kt[...] = as_columns((dot_nt(normed, wk[...]) * scale).astype(BF).astype(F32))
    vt[...] = as_columns((dot_nt(normed, wv[...]) + bv[layer:layer + 1, :].astype(F32)).astype(BF).astype(F32))
    own = iota((8, qs.shape[1]), 1) // 64 == iota((8, qs.shape[1]), 0)
    pairs = audios // 2
    hold = pairs // 2

    def release(pair):
        for a in (pair * 2, pair * 2 + 1):
            k_out(a).start()
            v_out(a).start()

    @pl.loop(0, pairs)
    def _(pair):
        group = (pair * 2, pair * 2 + 1)
        for a in group:
            k_in(a).wait()
            v_in(a).wait()
        for a in group:
            insert_slot(((kbuf, kt), (vbuf, vt)), a * beams, beams, pos_ref[a * beams], slots)

        @pl.when(pair >= hold)
        def _():
            release(pair - hold)

        probs = []
        for a in group:
            scores = []
            for i in range(beams):
                q = jnp.broadcast_to(qs[pl.ds(a * beams + i, 1), :], own.shape)
                scores.append(dot(jnp.where(own, q, 0.0).astype(BF), kbuf[a * beams + i]))
            scores = jnp.concatenate(scores, axis=0)
            scores = jnp.where(iota(scores.shape, 1) <= pos_ref[a * beams], scores, -1e30)
            e = jnp.exp(scores - jnp.max(scores, axis=-1, keepdims=True))
            probs.append(e * (1.0 / jnp.sum(e, axis=-1, keepdims=True)))
        for a, p in zip(group, probs):
            for i in range(beams):
                r = a * beams + i
                out = dot_nt(p[i * 8:i * 8 + 8].astype(BF), vbuf[r])
                os[pl.ds(r, 1), :] = jnp.sum(jnp.where(own, out, 0.0), axis=0, keepdims=True)

    @pl.loop(pairs - hold, pairs)
    def _(pair):
        release(pair)

    for m in range(parts):
        o[m] = os[m * rows // parts:(m + 1) * rows // parts, :].astype(BF)
    last = pltpu.make_async_copy(o, o_hbm, psem.at[0])
    last.start()

    @pl.loop(0, audios)
    def _(a):
        k_out(a).wait()
        v_out(a).wait()

    last.wait()


def self_call(layer, beams, parts, h, pos, g, b, wq, wk, wv, bq, bv, k, v):
    rows = h.shape[0]
    audios = rows // beams
    _, _, width, slots = k.shape
    args = (h, pos, g, b, wq, wk, wv, bq, bv, k, v)
    return pl.pallas_call(
        functools.partial(self_kernel, layer, beams, parts),
        out_shape=(jax.ShapeDtypeStruct((parts, rows // parts, width), BF), jax.ShapeDtypeStruct(k.shape, BF), jax.ShapeDtypeStruct(v.shape, BF)),
        in_specs=[ANY] * 11,
        out_specs=(ANY, ANY, ANY),
        scratch_shapes=[
            pltpu.VMEM(h.shape, BF), pltpu.SMEM(pos.shape, jnp.int32), pltpu.VMEM(g.shape, BF), pltpu.VMEM(b.shape, BF),
            pltpu.VMEM(wq.shape[1:], BF), pltpu.VMEM(wk.shape[1:], BF), pltpu.VMEM(wv.shape[1:], BF),
            pltpu.VMEM(bq.shape, BF), pltpu.VMEM(bv.shape, BF),
            pltpu.VMEM((rows, width, slots), BF), pltpu.VMEM((rows, width, slots), BF),
            pltpu.VMEM((rows, width), F32), pltpu.VMEM((width, 128), F32), pltpu.VMEM((width, 128), F32), pltpu.VMEM((rows, width), F32), pltpu.VMEM((parts, rows // parts, width), BF),
            DMA((9,)), DMA((audios,)), DMA((audios,)), DMA((audios,)), DMA((audios,)),
        ],
        cost_estimate=pl.CostEstimate(flops=0, bytes_accessed=4 * k.size, transcendentals=0),
        compiler_params=pltpu.CompilerParams(vmem_limit_bytes=VMEM_LIMIT),
        name=f"self_{layer}",
    )(*args)


def rest_kernel(beams, parts, o_hbm, h_hbm, pos_hbm, g_hbm, b_hbm, wq_hbm, bq_hbm, wk_hbm, wv_hbm, bv_hbm, wo_hbm, bo_hbm, wc_hbm, bc_hbm, wco_hbm, bco_hbm, w1_hbm, b1_hbm, w2_hbm, b2_hbm,
                wo_far, sk_hbm, sv_hbm, ck_hbm, cv_hbm, part_ref, out_ref, sk, sv, kt, vt, spot,
                o, h, pos_ref, g, b, wq, bq, wk, wv, bv, wo, bo, wc, bc, wco, bco, w1, b1, w2, b2, ck, cv, hid, qr, kr, vr, kall, vall, os, got, snd, rcv,
                psem, wsem, msem, mrsem, skem, svem, ckem, cvem, ssem, rsem):
    rows = h.shape[0]
    audios = rows // beams
    group = audios // parts
    prow = rows // parts
    width = o.shape[-1]
    heads = width // 64
    scale = 64 ** -0.25
    dp = lax.axis_index('dp')
    me = lax.axis_index('tp')
    mate = me + 1 - 2 * (me % 2)
    peers = ((me + 2) % 4, (mate + 2) % 4, mate)

    small = copies([(o_hbm, o), (h_hbm, h), (g_hbm, g), (b_hbm, b), (bq_hbm, bq), (bv_hbm, bv), (bo_hbm, bo), (bc_hbm, bc), (bco_hbm, bco), (b1_hbm, b1), (b2_hbm, b2), (pos_hbm, pos_ref)], psem)
    def layer_copies(layer, arrays, sem):
        return copies([(x.at[layer], y.at[layer]) for x, y in arrays], sem)

    first = layer_copies(0, ((wc_hbm, wc), (wco_hbm, wco), (w1_hbm, w1), (w2_hbm, w2)), wsem.at[1])
    second = layer_copies(1, ((wc_hbm, wc), (wco_hbm, wco), (w1_hbm, w1), (w2_hbm, w2)), wsem.at[2])
    early = copies([(wo_hbm.at[i], wo.at[i, 0]) for i in range(2)], wsem.at[0])

    def shared(layer):
        return [pltpu.make_async_remote_copy(src.at[layer], wo.at[layer, 1 + j], msem.at[layer, j], mrsem.at[layer, j], device_id=(dp, mate), device_id_type=MESH) for j, src in enumerate((wo_hbm, wo_far))]

    extra = copies([(x.at[1], y) for x, y in ((wq_hbm, wq), (wk_hbm, wk), (wv_hbm, wv))], wsem.at[3])

    def cross_in(layer, a):
        return pltpu.make_async_copy(ck_hbm.at[layer, a], ck.at[a], ckem.at[a]), pltpu.make_async_copy(cv_hbm.at[layer, a], cv.at[a], cvem.at[a])

    def self_in(a):
        r = pl.ds(a * beams, beams)
        return pltpu.make_async_copy(sk_hbm.at[1, r], sk.at[r], skem.at[a]), pltpu.make_async_copy(sv_hbm.at[1, r], sv.at[r], svem.at[a])

    def start(pair):
        for c in pair:
            c.start()

    def wait(pair):
        for c in pair:
            c.wait()

    start(small)
    start(early)
    barrier = pltpu.get_barrier_semaphore()
    for peer in peers:
        pl.semaphore_signal(barrier, inc=1, device_id=(dp, peer), device_id_type=MESH)

    def sends(step, m):
        return [pltpu.make_async_remote_copy(snd.at[step, m], rcv.at[step, m, j], ssem.at[step, m, j], rsem.at[step, m, j], device_id=(dp, peer), device_id_type=MESH) for j, peer in enumerate(peers)]

    def push(step, m, part):
        snd[step, m] = part.astype(BF)
        start(sends(step, m))

    def total(step, m):
        wait(sends(step, m))
        mine = snd[step, m].astype(F32) + rcv[step, m, 2].astype(F32)
        return mine + (rcv[step, m, 0].astype(F32) + rcv[step, m, 1].astype(F32))

    def heads_sends(step, m):
        return [pltpu.make_async_remote_copy(got.at[step, m, 3], got.at[step, m, j], ssem.at[step, m, j], rsem.at[step, m, j], device_id=(dp, peer), device_id_type=MESH) for j, peer in enumerate(peers)]

    def push_heads(step, m, out):
        got[step, m, 3] = out
        start(heads_sends(step, m))

    def project(step, m, layer):
        wait(heads_sends(step, m))
        here = dot(got[step, m, 3], wo[layer, 0]) + dot(got[step, m, 2], wo[layer, 1])
        return here + (dot(got[step, m, 0], wo_far[layer]) + dot(got[step, m, 1], wo[layer, 2]))

    def settle(m, update, bias):
        new = (hid[m].astype(F32) + update + bias.astype(F32)).astype(BF)
        hid[m] = new
        return new.astype(F32)

    def flags(shape, rule):
        return rule(iota(shape, 0), iota(shape, 1)).astype(F32).astype(BF)

    def pick(m):
        return flags((prow, rows), lambda r, c: c == r + m * prow)

    def cross_half(layer, m, wide):
        normed = layer_norm(wide, g[1, layer:layer + 1, :], b[1, layer:layer + 1, :])
        q = ((dot_nt(normed, wc[layer]) + bc[layer:layer + 1, :].astype(F32)) * scale).astype(BF)
        qr[m, 0:prow, :] = q.astype(F32)

        @pl.loop(0, group)
        def _(n):
            wait(cross_in(layer, m * group + n))

        if layer == 0:
            @pl.loop(0, group)
            def _(n):
                start(self_in(m * group + n))

            start(first[2:] if m == 0 else extra if m == 1 else [])

        own = iota((heads * 8, width), 1) // 64 == iota((heads * 8, width), 0) // 8

        def probs_of(n):
            qa = jnp.concatenate([qr[m, n * beams:n * beams + 8, :]] * heads, axis=0)
            scores = dot(jnp.where(own, qa, 0.0).astype(BF), ck[m * group + n])
            e = jnp.exp(scores - jnp.max(scores, axis=-1, keepdims=True))
            return (e * (1.0 / jnp.sum(e, axis=-1, keepdims=True))).astype(BF)

        def mix(n, p):
            out = jnp.where(own, dot_nt(p, cv[m * group + n]), 0.0)
            acc = out[0:8]
            for j in range(1, heads):
                acc = acc + out[j * 8:j * 8 + 8]
            os[m, n * beams:(n + 1) * beams, :] = acc[0:beams]

        probs = [probs_of(n) for n in range(group)]
        for n in range(group):
            mix(n, probs[n])

        return dot(os[m].astype(BF), wco[layer])

    def mlp_half(layer, m, wide):
        normed = layer_norm(wide, g[2, layer:layer + 1, :], b[2, layer:layer + 1, :])
        inner = dot(normed, w1[layer]) + b1[layer:layer + 1, :].astype(F32)
        inner = (0.5 * inner * (1.0 + lax.erf(inner * (2.0 ** -0.5)))).astype(BF)
        return dot(inner, w2[layer])

    def self_half(m, wide):
        normed = layer_norm(wide, g[0, 1:1 + 1, :], b[0, 1:1 + 1, :])
        q = ((dot_nt(normed, wq[...]) + bq[1:2, :].astype(F32)) * scale).astype(BF)
        k = (dot_nt(normed, wk[...]) * scale).astype(BF)
        v = (dot_nt(normed, wv[...]) + bv[1:2, :].astype(F32)).astype(BF)
        kall[m * prow:(m + 1) * prow, :] = k.astype(F32)
        vall[m * prow:(m + 1) * prow, :] = v.astype(F32)
        qr[m, 0:prow, :] = q.astype(F32)
        kr[m] = k.astype(F32)
        vr[m] = v.astype(F32)
        own = iota((8, width), 1) // 64 == iota((8, width), 0)

        @pl.loop(0, group)
        def _(n):
            wait(self_in(m * group + n))

        if m == 0:
            start(second)

        @pl.loop(0, group)
        def _(n):
            start(cross_in(1, m * group + n))

        def row(ref, r):
            return jnp.where(own, jnp.broadcast_to(ref[m, r:r + 1, :], own.shape), 0.0)

        def probs_of(n):
            pos = pos_ref[(m * group + n) * beams]
            scores, fresh = [], []
            for j in range(beams):
                r = n * beams + j
                q8 = row(qr, r)
                scores.append(dot(q8.astype(BF), sk[m * prow + r]))
                fresh.append(jnp.sum(q8 * row(kr, r), axis=-1, keepdims=True))
            scores = jnp.concatenate(scores, axis=0)
            fresh = jnp.concatenate(fresh, axis=0)
            old = iota(scores.shape, 1) < pos
            scores = jnp.where(old, scores, -1e30)
            top = jnp.maximum(jnp.max(scores, axis=-1, keepdims=True), fresh)
            e = jnp.where(old, jnp.exp(scores - top), 0.0)
            e_new = jnp.exp(fresh - top)
            inv = 1.0 / (jnp.sum(e, axis=-1, keepdims=True) + e_new)
            return (e * inv), (e_new * inv).astype(BF).astype(F32)

        def mix(n, p, p_new):
            for j in range(beams):
                r = n * beams + j
                out = dot_nt(p[j * 8:j * 8 + 8].astype(BF), sv[m * prow + r])
                out = jnp.where(own, out, 0.0) + p_new[j * 8:j * 8 + 8] * row(vr, r)
                os[m, r:r + 1, :] = jnp.sum(out, axis=0, keepdims=True)

        probs = [probs_of(n) for n in range(group)]
        for n in range(group):
            mix(n, *probs[n])

        return os[m].astype(BF)

    wait(small)
    pl.semaphore_wait(barrier, 3)
    for m in range(parts):
        push_heads(0, m, o[m])
    start(shared(0))
    start(first[:2])

    @pl.loop(0, audios)
    def _(a):
        start(cross_in(0, a))

    start(shared(1))

    for m in range(parts):
        hid[m] = dot(pick(m), h[...]).astype(BF)
        qr[m, prow:, :] = jnp.zeros((qr.shape[1] - prow, width), F32)
    kall[rows:, :] = jnp.zeros((128 - rows, width), F32)
    vall[rows:, :] = jnp.zeros((128 - rows, width), F32)
    wait(early)
    wait(shared(0))
    wait(first[:2])
    for m in range(parts):
        push(1, m, cross_half(0, m, settle(m, project(0, m, 0), bo[0:1, :])))
    wait(first[2:])
    for m in range(parts):
        push(2, m, mlp_half(0, m, settle(m, total(1, m), bco[0:1, :])))
    wait(extra)
    for m in range(parts):
        push_heads(3, m, self_half(m, settle(m, total(2, m), b2[0:1, :])))
    kt[...] = kall[...].T
    vt[...] = vall[...].T
    for a in range(audios):
        spot[a] = jnp.full(spot.shape[1:], pos_ref[a * beams], jnp.int32)
    wait(second)
    wait(shared(1))
    for m in range(parts):
        push(4, m, cross_half(1, m, settle(m, project(3, m, 1), bo[1:2, :])))
    final = jnp.zeros((rows, h.shape[1]), F32)
    resid = jnp.zeros((rows, h.shape[1]), F32)
    for m in range(parts):
        place = flags((rows, prow), lambda r, c: r == c + m * prow)
        wide = settle(m, total(4, m), bco[1:2, :])
        final = final + dot(place, mlp_half(1, m, wide).astype(BF))
        resid = resid + dot(place, hid[m])
    part_ref[...] = final.astype(BF)
    out_ref[...] = resid.astype(BF)


def rest_call(beams, parts, o, h, pos, g, b, wq, bq, wk, wv, bv, wo, bo, wc, bc, wco, bco, w1, b1, w2, b2, wo_far, sk, sv, ck, cv):
    rows, dim = h.shape
    _, audios, width, frames = ck.shape
    slots = sk.shape[-1]
    prow = rows // parts
    args = (o, h, pos, g, b, wq, bq, wk, wv, bv, wo, bo, wc, bc, wco, bco, w1, b1, w2, b2, wo_far, sk, sv, ck, cv)

    def whole(x):
        return pltpu.VMEM(x.shape, BF)

    def one(x):
        return pltpu.VMEM(x.shape[1:], BF)

    return pl.pallas_call(
        functools.partial(rest_kernel, beams, parts),
        out_shape=(pltpu.VMEM(h.shape, BF), pltpu.VMEM(h.shape, BF), pltpu.VMEM((rows, width, slots), BF), pltpu.VMEM((rows, width, slots), BF), pltpu.VMEM((width, 128), F32), pltpu.VMEM((width, 128), F32), pltpu.VMEM((audios, 8, 128), jnp.int32)),
        in_specs=[ANY] * (len(args) - 5) + [VM] + [ANY] * 4,
        out_specs=(VM,) * 7,
        scratch_shapes=[
            whole(o), whole(h), pltpu.SMEM(pos.shape, jnp.int32), whole(g), whole(b), one(wq), whole(bq), one(wk), one(wv), whole(bv), pltpu.VMEM((2, 3, width, dim), BF), whole(bo), whole(wc), whole(bc), whole(wco), whole(bco), whole(w1), whole(b1), whole(w2), whole(b2), one(ck), one(cv),
            pltpu.VMEM((parts, prow, dim), BF),
            pltpu.VMEM((parts, prow + 8, width), F32), pltpu.VMEM((parts, prow, width), F32), pltpu.VMEM((parts, prow, width), F32),
            pltpu.VMEM((128, width), F32), pltpu.VMEM((128, width), F32), pltpu.VMEM((parts, prow, width), F32),
            pltpu.VMEM((5, parts, 4, prow, width), BF), pltpu.VMEM((5, parts, prow, dim), BF), pltpu.VMEM((5, parts, 3, prow, dim), BF),
            DMA((12,)), DMA((4, 8)), DMA((2, 2)), DMA((2, 2)), DMA((audios,)), DMA((audios,)), DMA((audios,)), DMA((audios,)), DMA((5, parts, 3)), DMA((5, parts, 3)),
        ],
        compiler_params=pltpu.CompilerParams(collective_id=0, has_side_effects=True, vmem_limit_bytes=REST_LIMIT),
        name="rest",
    )(*args)


def write_kernel(layer, beams, spot, kt, vt, sk_in, sv_in, ki_hbm, vi_hbm, ko_hbm, vo_hbm, sk, sv, kosem, vosem):
    rows, width, slots = sk.shape
    audios = rows // beams

    def k_out(a):
        r = pl.ds(a * beams, beams)
        return pltpu.make_async_copy(sk.at[r], ko_hbm.at[layer, r], kosem.at[a])

    def v_out(a):
        r = pl.ds(a * beams, beams)
        return pltpu.make_async_copy(sv.at[r], vo_hbm.at[layer, r], vosem.at[a])

    @pl.loop(0, audios)
    def _(a):
        hits = [iota((width, min(128, slots - t)), 1) + t == spot[a, 0:1, :min(128, slots - t)] for t in range(0, slots, 128)]
        for buf, cols, out in ((sk, kt, k_out), (sv, vt, v_out)):
            for i in range(beams):
                r = a * beams + i
                col = jnp.take_along_axis(cols[...], jnp.full((width, 128), r, jnp.int32), axis=1).astype(BF)
                for n, hit in enumerate(hits):
                    size = hit.shape[1]
                    span = (r, slice(None), slice(n * 128, n * 128 + size))
                    buf[span] = jnp.where(hit, col[:, :size], buf[span])
            out(a).start()

    @pl.loop(0, audios)
    def _(a):
        k_out(a).wait()
        v_out(a).wait()


def write_call(layer, beams, spot, kt, vt, sk, sv, ko, vo):
    audios = sk.shape[0] // beams
    return pl.pallas_call(
        functools.partial(write_kernel, layer, beams),
        out_shape=(jax.ShapeDtypeStruct(ko.shape, BF), jax.ShapeDtypeStruct(vo.shape, BF), pltpu.VMEM(sk.shape, BF), pltpu.VMEM(sv.shape, BF)),
        in_specs=[VM, VM, VM, VM, VM, ANY, ANY],
        out_specs=(ANY, ANY, VM, VM),
        input_output_aliases={3: 2, 4: 3, 5: 0, 6: 1},
        cost_estimate=pl.CostEstimate(flops=0, bytes_accessed=4 * sk.size, transcendentals=0),
        scratch_shapes=[DMA((audios,)), DMA((audios,))],
        compiler_params=pltpu.CompilerParams(vmem_limit_bytes=4 * 1024 * 1024),
        name="write",
    )(spot, kt, vt, sk, sv, ko, vo)[:2]


def solution(mesh):
    cache_spec = P(None, 'dp', None, 'tp', None)
    col_spec = P(None, None, 'tp')
    row_spec = P(None, 'tp', None)
    vec_spec = P(None, 'tp')
    in_specs = (P('dp', None), P('dp'), cache_spec, cache_spec, cache_spec, cache_spec,
                P(), P(), col_spec, vec_spec, col_spec, col_spec, vec_spec, row_spec, P(), col_spec, vec_spec, row_spec, P(), col_spec, vec_spec, row_spec, P())

    def heads_first(cache):
        cache = jnp.transpose(cache, (0, 1, 3, 4, 2))
        return cache.reshape(cache.shape[:2] + (-1, cache.shape[-1]))

    def heads_last(cache, like):
        layers, batch, slots, heads, dim = like.shape
        return jnp.transpose(cache.reshape(layers, batch, heads, dim, slots), (0, 1, 4, 2, 3))

    def local_step(hidden, positions, self_keys, self_vals, cross_keys, cross_vals, g, b, wq, bq, wk, wv, bv, wo, bo, wc, bc, wco, bco, w1, b1, w2, b2):
        beams = hidden.shape[0] // cross_keys.shape[1]
        sk, sv, ck, cv = (heads_first(x) for x in (self_keys, self_vals, cross_keys, cross_vals))
        wq, wk, wv, wc = (jnp.swapaxes(w, 1, 2) for w in (wq, wk, wv, wc))
        g, b = (jnp.swapaxes(x, 0, 1) for x in (g, b))
        def hop(x, flip):
            return lax.ppermute(x, 'tp', [(i, i ^ flip) for i in range(4)])

        parts = 2
        wo_far = pltpu.with_memory_space_constraint(hop(wo, 2), pltpu.VMEM)
        o, ko, vo = self_call(0, beams, parts, hidden, positions, g, b, wq, wk, wv, bq, bv, sk, sv)
        part, hidden, sk1, sv1, kt, vt, spot = rest_call(beams, parts, o, hidden, positions, g, b, wq, bq, wk, wv, bv, wo, bo, wc, bc, wco, bco, w1, b1, w2, b2, wo_far, sk, sv, ck, cv)
        ko, vo = write_call(1, beams, spot, kt, vt, sk1, sv1, ko, vo)
        here, mate, far, diag = (x.astype(F32) for x in (part, hop(part, 1), hop(part, 2), hop(part, 3)))
        hidden = (hidden.astype(F32) + ((here + mate) + (far + diag)) + b2[1].astype(F32)).astype(BF)
        return hidden, heads_last(ko, self_keys), heads_last(vo, self_vals)

    return jax.shard_map(local_step, mesh=mesh, in_specs=in_specs, out_specs=(P('dp', None), cache_spec, cache_spec), check_vma=False)
```

```python
import functools

import jax
import jax.numpy as jnp
from jax import lax
from jax.experimental import pallas as pl
from jax.experimental.pallas import tpu as pltpu
from jax.sharding import PartitionSpec as P

EPS = 1e-5
BF = jnp.bfloat16
F32 = jnp.float32
MESH = pl.DeviceIdType.MESH
ANY = pl.BlockSpec(memory_space=pl.ANY)
VM = pl.BlockSpec(memory_space=pltpu.VMEM)
SMEM = pl.BlockSpec(memory_space=pltpu.SMEM)
DMA = pltpu.SemaphoreType.DMA
NT = (((1,), (1,)), ((), ()))
VMEM_LIMIT = 60 * 1024 * 1024
REST_LIMIT = 38 * 1024 * 1024


def layer_norm(wide, gain_row, bias_row):
    center = wide - jnp.mean(wide, axis=-1, keepdims=True)
    var_est = jnp.mean(center * center, axis=-1, keepdims=True)
    return (center * lax.rsqrt(var_est + EPS) * gain_row.astype(F32) + bias_row.astype(F32)).astype(BF)


def dot(a, b):
    return jnp.dot(a, b, preferred_element_type=F32)


def dot_nt(a, b):
    return lax.dot_general(a, b, NT, preferred_element_type=F32)


def iota(shape, dim):
    return lax.broadcasted_iota(jnp.int32, shape, dim)


def insert_slot(places, row, beams, pos, slots):
    last = (slots // 128) * 128
    tile = pos // 128

    def insert(start, size):
        for buf, cols in places:
            width = cols.shape[0]
            hit = iota((width, size), 1) == pos - start
            for i in range(beams):
                col = jnp.take_along_axis(cols[...], jnp.full((width, 128), row + i, jnp.int32), axis=1)[:, :size]
                span = (row + i, slice(None), pl.ds(start, size))
                buf[span] = jnp.where(hit, col.astype(BF), buf[span])

    @pl.when(tile * 128 < last)
    def _():
        insert(pl.multiple_of(tile * 128, 128), 128)

    if slots > last:
        @pl.when(tile * 128 >= last)
        def _():
            insert(last, slots - last)


def as_columns(rows):
    pad = jnp.zeros((128 - rows.shape[0], rows.shape[1]), F32)
    return jnp.concatenate([rows, pad], axis=0).T


def copies(pairs, sem):
    return [pltpu.make_async_copy(s, d, sem.at[i]) for i, (s, d) in enumerate(pairs)]


def self_kernel(layer, beams, parts, h_hbm, pos_hbm, g_hbm, b_hbm, wq_hbm, wk_hbm, wv_hbm, bq_hbm, bv_hbm, k_hbm, v_hbm, o_hbm, ko_hbm, vo_hbm,
                h, pos_ref, g, b, wq, wk, wv, bq, bv, kbuf, vbuf, qs, kt, vt, os, o, psem, ksem, vsem, kosem, vosem):
    rows = h.shape[0]
    audios = rows // beams
    slots = kbuf.shape[-1]
    scale = 64 ** -0.25

    small = copies([(h_hbm, h), (g_hbm, g), (b_hbm, b), (wq_hbm.at[layer], wq), (wk_hbm.at[layer], wk), (wv_hbm.at[layer], wv), (bq_hbm, bq), (bv_hbm, bv), (pos_hbm, pos_ref)], psem)
    for c in small:
        c.start()

    def block(a, src, dst, sem):
        return pltpu.make_async_copy(src, dst, sem.at[a])

    def at(a):
        return pl.ds(a * beams, beams)

    def k_in(a):
        return block(a, k_hbm.at[layer, at(a)], kbuf.at[at(a)], ksem)

    def v_in(a):
        return block(a, v_hbm.at[layer, at(a)], vbuf.at[at(a)], vsem)

    def k_out(a):
        return block(a, kbuf.at[at(a)], ko_hbm.at[layer, at(a)], kosem)

    def v_out(a):
        return block(a, vbuf.at[at(a)], vo_hbm.at[layer, at(a)], vosem)

    @pl.loop(0, audios)
    def _(a):
        k_in(a).start()
        v_in(a).start()

    for c in small:
        c.wait()
    normed = layer_norm(h[...].astype(F32), g[0, layer:layer + 1, :], b[0, layer:layer + 1, :])
    qs[...] = ((dot_nt(normed, wq[...]) + bq[layer:layer + 1, :].astype(F32)) * scale).astype(BF).astype(F32)
    kt[...] = as_columns((dot_nt(normed, wk[...]) * scale).astype(BF).astype(F32))
    vt[...] = as_columns((dot_nt(normed, wv[...]) + bv[layer:layer + 1, :].astype(F32)).astype(BF).astype(F32))
    own = iota((8, qs.shape[1]), 1) // 64 == iota((8, qs.shape[1]), 0)
    pairs = audios // 2
    hold = pairs // 2

    def release(pair):
        for a in (pair * 2, pair * 2 + 1):
            k_out(a).start()
            v_out(a).start()

    @pl.loop(0, pairs)
    def _(pair):
        group = (pair * 2, pair * 2 + 1)
        for a in group:
            k_in(a).wait()
            v_in(a).wait()
        for a in group:
            insert_slot(((kbuf, kt), (vbuf, vt)), a * beams, beams, pos_ref[a * beams], slots)

        @pl.when(pair >= hold)
        def _():
            release(pair - hold)

        probs = []
        for a in group:
            scores = []
            for i in range(beams):
                q = jnp.broadcast_to(qs[pl.ds(a * beams + i, 1), :], own.shape)
                scores.append(dot(jnp.where(own, q, 0.0).astype(BF), kbuf[a * beams + i]))
            scores = jnp.concatenate(scores, axis=0)
            scores = jnp.where(iota(scores.shape, 1) <= pos_ref[a * beams], scores, -1e30)
            e = jnp.exp(scores - jnp.max(scores, axis=-1, keepdims=True))
            probs.append(e * (1.0 / jnp.sum(e, axis=-1, keepdims=True)))
        for a, p in zip(group, probs):
            for i in range(beams):
                r = a * beams + i
                out = dot_nt(p[i * 8:i * 8 + 8].astype(BF), vbuf[r])
                os[pl.ds(r, 1), :] = jnp.sum(jnp.where(own, out, 0.0), axis=0, keepdims=True)

    @pl.loop(pairs - hold, pairs)
    def _(pair):
        release(pair)

    for m in range(parts):
        o[m] = os[m * rows // parts:(m + 1) * rows // parts, :].astype(BF)
    last = pltpu.make_async_copy(o, o_hbm, psem.at[0])
    last.start()

    @pl.loop(0, audios)
    def _(a):
        k_out(a).wait()
        v_out(a).wait()

    last.wait()


def self_call(layer, beams, parts, h, pos, g, b, wq, wk, wv, bq, bv, k, v):
    rows = h.shape[0]
    audios = rows // beams
    _, _, width, slots = k.shape
    args = (h, pos, g, b, wq, wk, wv, bq, bv, k, v)
    return pl.pallas_call(
        functools.partial(self_kernel, layer, beams, parts),
        out_shape=(jax.ShapeDtypeStruct((parts, rows // parts, width), BF), jax.ShapeDtypeStruct(k.shape, BF), jax.ShapeDtypeStruct(v.shape, BF)),
        in_specs=[ANY] * 11,
        out_specs=(ANY, ANY, ANY),
        scratch_shapes=[
            pltpu.VMEM(h.shape, BF), pltpu.SMEM(pos.shape, jnp.int32), pltpu.VMEM(g.shape, BF), pltpu.VMEM(b.shape, BF),
            pltpu.VMEM(wq.shape[1:], BF), pltpu.VMEM(wk.shape[1:], BF), pltpu.VMEM(wv.shape[1:], BF),
            pltpu.VMEM(bq.shape, BF), pltpu.VMEM(bv.shape, BF),
            pltpu.VMEM((rows, width, slots), BF), pltpu.VMEM((rows, width, slots), BF),
            pltpu.VMEM((rows, width), F32), pltpu.VMEM((width, 128), F32), pltpu.VMEM((width, 128), F32), pltpu.VMEM((rows, width), F32), pltpu.VMEM((parts, rows // parts, width), BF),
            DMA((9,)), DMA((audios,)), DMA((audios,)), DMA((audios,)), DMA((audios,)),
        ],
        cost_estimate=pl.CostEstimate(flops=0, bytes_accessed=4 * k.size, transcendentals=0),
        compiler_params=pltpu.CompilerParams(vmem_limit_bytes=VMEM_LIMIT),
        name=f"self_{layer}",
    )(*args)


def rest_kernel(beams, parts, o_hbm, h_hbm, pos_hbm, g_hbm, b_hbm, wq_hbm, bq_hbm, wk_hbm, wv_hbm, bv_hbm, wo_hbm, bo_hbm, wc_hbm, bc_hbm, wco_hbm, bco_hbm, w1_hbm, b1_hbm, w2_hbm, b2_hbm,
                wo_far, sk_hbm, sv_hbm, ck_hbm, cv_hbm, part_ref, out_ref, sk, sv, kt, vt, spot,
                o, h, pos_ref, g, b, wq, bq, wk, wv, bv, wo, bo, wc, bc, wco, bco, w1, b1, w2, b2, ck, cv, hid, qr, kr, vr, kall, vall, os, got, snd, rcv, wcx,
                psem, wsem, msem, mrsem, xsem, xrsem, skem, svem, ckem, cvem, ssem, rsem):
    rows = h.shape[0]
    audios = rows // beams
    group = audios // parts
    prow = rows // parts
    width = o.shape[-1]
    heads = width // 64
    scale = 64 ** -0.25
    dp = lax.axis_index('dp')
    me = lax.axis_index('tp')
    mate = me + 1 - 2 * (me % 2)
    peers = ((me + 2) % 4, (mate + 2) % 4, mate)

    small = copies([(o_hbm, o), (h_hbm, h), (g_hbm, g), (b_hbm, b), (bq_hbm, bq), (bv_hbm, bv), (bo_hbm, bo), (bc_hbm, bc), (bco_hbm, bco), (b1_hbm, b1), (b2_hbm, b2), (pos_hbm, pos_ref)], psem)
    def layer_copies(layer, arrays, sem):
        return copies([(x.at[layer], y.at[layer]) for x, y in arrays], sem)

    first = layer_copies(0, ((wc_hbm, wc), (wco_hbm, wco), (w1_hbm, w1), (w2_hbm, w2)), wsem.at[1])
    second = layer_copies(1, ((wc_hbm, wc), (wco_hbm, wco), (w1_hbm, w1), (w2_hbm, w2)), wsem.at[2])
    early = copies([(wo_hbm.at[i], wo.at[i, 0]) for i in range(2)], wsem.at[0])

    def shared(layer):
        return [pltpu.make_async_remote_copy(src.at[layer], wo.at[layer, 1 + j], msem.at[layer, j], mrsem.at[layer, j], device_id=(dp, mate), device_id_type=MESH) for j, src in enumerate((wo_hbm, wo_far))]

    extra = copies([(x.at[1], y) for x, y in ((wq_hbm, wq), (wk_hbm, wk), (wv_hbm, wv))], wsem.at[3])

    def cross_in(layer, a):
        return pltpu.make_async_copy(ck_hbm.at[layer, a], ck.at[a], ckem.at[a]), pltpu.make_async_copy(cv_hbm.at[layer, a], cv.at[a], cvem.at[a])

    def self_in(a):
        r = pl.ds(a * beams, beams)
        return pltpu.make_async_copy(sk_hbm.at[1, r], sk.at[r], skem.at[a]), pltpu.make_async_copy(sv_hbm.at[1, r], sv.at[r], svem.at[a])

    def start(pair):
        for c in pair:
            c.start()

    def wait(pair):
        for c in pair:
            c.wait()

    start(small)
    start(early)
    barrier = pltpu.get_barrier_semaphore()
    for peer in peers:
        pl.semaphore_signal(barrier, inc=1, device_id=(dp, peer), device_id_type=MESH)

    def sends(step, m):
        return [pltpu.make_async_remote_copy(snd.at[step, m], rcv.at[step, m, j], ssem.at[step, m, j], rsem.at[step, m, j], device_id=(dp, peer), device_id_type=MESH) for j, peer in enumerate(peers)]

    def push(step, m, part):
        snd[step, m] = part.astype(BF)
        start(sends(step, m))

    def total(step, m):
        wait(sends(step, m))
        mine = snd[step, m].astype(F32) + rcv[step, m, 2].astype(F32)
        return mine + (rcv[step, m, 0].astype(F32) + rcv[step, m, 1].astype(F32))

    def heads_sends(step, m):
        return [pltpu.make_async_remote_copy(got.at[step, m, 3], got.at[step, m, j], ssem.at[step, m, j], rsem.at[step, m, j], device_id=(dp, peer), device_id_type=MESH) for j, peer in enumerate(peers)]

    def push_heads(step, m, out):
        got[step, m, 3] = out
        start(heads_sends(step, m))

    def project(step, m, layer):
        wait(heads_sends(step, m))
        here = dot(got[step, m, 3], wo[layer, 0]) + dot(got[step, m, 2], wo[layer, 1])
        return here + (dot(got[step, m, 0], wo_far[layer]) + dot(got[step, m, 1], wo[layer, 2]))

    band = width // 2

    def over_link(i):
        r = pl.ds(i * band, band)
        return pltpu.make_async_remote_copy(wco_hbm.at[1, r], wcx.at[0, r], xsem.at[i], xrsem.at[i], device_id=(dp, peers[0]), device_id_type=MESH)

    def to_mate(i):
        if i == 2:
            return pltpu.make_async_remote_copy(wco_hbm.at[1], wcx.at[1], xsem.at[4], xrsem.at[4], device_id=(dp, mate), device_id_type=MESH)
        r = pl.ds(i * band, band)
        return pltpu.make_async_remote_copy(wcx.at[0, r], wcx.at[2, r], xsem.at[2 + i], xrsem.at[2 + i], device_id=(dp, mate), device_id_type=MESH)

    def project_cross(m):
        wait(heads_sends(4, m))
        here = dot(got[4, m, 3], wco[1]) + dot(got[4, m, 2], wcx[1])
        return here + (dot(got[4, m, 0], wcx[0]) + dot(got[4, m, 1], wcx[2]))

    def settle(m, update, bias):
        new = (hid[m].astype(F32) + update + bias.astype(F32)).astype(BF)
        hid[m] = new
        return new.astype(F32)

    def flags(shape, rule):
        return rule(iota(shape, 0), iota(shape, 1)).astype(F32).astype(BF)

    def pick(m):
        return flags((prow, rows), lambda r, c: c == r + m * prow)

    def cross_half(layer, m, wide):
        normed = layer_norm(wide, g[1, layer:layer + 1, :], b[1, layer:layer + 1, :])
        q = ((dot_nt(normed, wc[layer]) + bc[layer:layer + 1, :].astype(F32)) * scale).astype(BF)
        qr[m, 0:prow, :] = q.astype(F32)

        @pl.loop(0, group)
        def _(n):
            wait(cross_in(layer, m * group + n))

        if layer == 0:
            @pl.loop(0, group)
            def _(n):
                start(self_in(m * group + n))

            start(first[2:] if m == 0 else extra if m == 1 else [])

        own = iota((heads * 8, width), 1) // 64 == iota((heads * 8, width), 0) // 8

        def probs_of(n):
            qa = jnp.concatenate([qr[m, n * beams:n * beams + 8, :]] * heads, axis=0)
            scores = dot(jnp.where(own, qa, 0.0).astype(BF), ck[m * group + n])
            e = jnp.exp(scores - jnp.max(scores, axis=-1, keepdims=True))
            return (e * (1.0 / jnp.sum(e, axis=-1, keepdims=True))).astype(BF)

        def mix(n, p):
            out = jnp.where(own, dot_nt(p, cv[m * group + n]), 0.0)
            acc = out[0:8]
            for j in range(1, heads):
                acc = acc + out[j * 8:j * 8 + 8]
            os[m, n * beams:(n + 1) * beams, :] = acc[0:beams]

        probs = [probs_of(n) for n in range(group)]
        for n in range(group):
            mix(n, probs[n])

        return os[m].astype(BF)

    def mlp_half(layer, m, wide):
        normed = layer_norm(wide, g[2, layer:layer + 1, :], b[2, layer:layer + 1, :])
        inner = dot(normed, w1[layer]) + b1[layer:layer + 1, :].astype(F32)
        inner = (0.5 * inner * (1.0 + lax.erf(inner * (2.0 ** -0.5)))).astype(BF)
        return dot(inner, w2[layer])

    def self_half(m, wide):
        normed = layer_norm(wide, g[0, 1:1 + 1, :], b[0, 1:1 + 1, :])
        q = ((dot_nt(normed, wq[...]) + bq[1:2, :].astype(F32)) * scale).astype(BF)
        k = (dot_nt(normed, wk[...]) * scale).astype(BF)
        v = (dot_nt(normed, wv[...]) + bv[1:2, :].astype(F32)).astype(BF)
        kall[m * prow:(m + 1) * prow, :] = k.astype(F32)
        vall[m * prow:(m + 1) * prow, :] = v.astype(F32)
        qr[m, 0:prow, :] = q.astype(F32)
        kr[m] = k.astype(F32)
        vr[m] = v.astype(F32)
        own = iota((8, width), 1) // 64 == iota((8, width), 0)

        @pl.loop(0, group)
        def _(n):
            wait(self_in(m * group + n))

        if m == 0:
            start(second)

        @pl.loop(0, group)
        def _(n):
            start(cross_in(1, m * group + n))

        def row(ref, r):
            return jnp.where(own, jnp.broadcast_to(ref[m, r:r + 1, :], own.shape), 0.0)

        def probs_of(n):
            pos = pos_ref[(m * group + n) * beams]
            scores, fresh = [], []
            for j in range(beams):
                r = n * beams + j
                q8 = row(qr, r)
                scores.append(dot(q8.astype(BF), sk[m * prow + r]))
                fresh.append(jnp.sum(q8 * row(kr, r), axis=-1, keepdims=True))
            scores = jnp.concatenate(scores, axis=0)
            fresh = jnp.concatenate(fresh, axis=0)
            old = iota(scores.shape, 1) < pos
            scores = jnp.where(old, scores, -1e30)
            top = jnp.maximum(jnp.max(scores, axis=-1, keepdims=True), fresh)
            e = jnp.where(old, jnp.exp(scores - top), 0.0)
            e_new = jnp.exp(fresh - top)
            inv = 1.0 / (jnp.sum(e, axis=-1, keepdims=True) + e_new)
            return (e * inv), (e_new * inv).astype(BF).astype(F32)

        def mix(n, p, p_new):
            for j in range(beams):
                r = n * beams + j
                out = dot_nt(p[j * 8:j * 8 + 8].astype(BF), sv[m * prow + r])
                out = jnp.where(own, out, 0.0) + p_new[j * 8:j * 8 + 8] * row(vr, r)
                os[m, r:r + 1, :] = jnp.sum(out, axis=0, keepdims=True)

        probs = [probs_of(n) for n in range(group)]
        for n in range(group):
            mix(n, *probs[n])

        return os[m].astype(BF)

    wait(small)
    pl.semaphore_wait(barrier, 3)
    for m in range(parts):
        push_heads(0, m, o[m])
    start(shared(0))
    start(first[:2])

    @pl.loop(0, audios)
    def _(a):
        start(cross_in(0, a))

    start(shared(1))

    for m in range(parts):
        hid[m] = dot(pick(m), h[...]).astype(BF)
        qr[m, prow:, :] = jnp.zeros((qr.shape[1] - prow, width), F32)
    kall[rows:, :] = jnp.zeros((128 - rows, width), F32)
    vall[rows:, :] = jnp.zeros((128 - rows, width), F32)
    wait(early)
    wait(shared(0))
    wait(first[:2])
    for m in range(parts):
        push(1, m, dot(cross_half(0, m, settle(m, project(0, m, 0), bo[0:1, :])), wco[0]))
    wait(first[2:])
    for m in range(parts):
        push(2, m, mlp_half(0, m, settle(m, total(1, m), bco[0:1, :])))
    wait(extra)
    for m in range(parts):
        wide = settle(m, total(2, m), b2[0:1, :])
        if m == 0:
            over_link(0).start()
            to_mate(2).start()
        push_heads(3, m, self_half(m, wide))
        if m == 0:
            over_link(1).start()
    kt[...] = kall[...].T
    vt[...] = vall[...].T
    for a in range(audios):
        spot[a] = jnp.full(spot.shape[1:], pos_ref[a * beams], jnp.int32)
    wait(second)
    wait(shared(1))
    for m in range(parts):
        wide = settle(m, project(3, m, 1), bo[1:2, :])
        if m < 2:
            over_link(m).wait()
            to_mate(m).start()
        push_heads(4, m, cross_half(1, m, wide))
    wait([to_mate(i) for i in range(3)])
    final = jnp.zeros((rows, h.shape[1]), F32)
    resid = jnp.zeros((rows, h.shape[1]), F32)
    for m in range(parts):
        place = flags((rows, prow), lambda r, c: r == c + m * prow)
        wide = settle(m, project_cross(m), bco[1:2, :])
        final = final + dot(place, mlp_half(1, m, wide).astype(BF))
        resid = resid + dot(place, hid[m])
    part_ref[...] = final.astype(BF)
    out_ref[...] = resid.astype(BF)


def rest_call(beams, parts, o, h, pos, g, b, wq, bq, wk, wv, bv, wo, bo, wc, bc, wco, bco, w1, b1, w2, b2, wo_far, sk, sv, ck, cv):
    rows, dim = h.shape
    _, audios, width, frames = ck.shape
    slots = sk.shape[-1]
    prow = rows // parts
    args = (o, h, pos, g, b, wq, bq, wk, wv, bv, wo, bo, wc, bc, wco, bco, w1, b1, w2, b2, wo_far, sk, sv, ck, cv)

    def whole(x):
        return pltpu.VMEM(x.shape, BF)

    def one(x):
        return pltpu.VMEM(x.shape[1:], BF)

    return pl.pallas_call(
        functools.partial(rest_kernel, beams, parts),
        out_shape=(pltpu.VMEM(h.shape, BF), pltpu.VMEM(h.shape, BF), pltpu.VMEM((rows, width, slots), BF), pltpu.VMEM((rows, width, slots), BF), pltpu.VMEM((width, 128), F32), pltpu.VMEM((width, 128), F32), pltpu.VMEM((audios, 8, 128), jnp.int32)),
        in_specs=[ANY] * (len(args) - 5) + [VM] + [ANY] * 4,
        out_specs=(VM,) * 7,
        scratch_shapes=[
            whole(o), whole(h), pltpu.SMEM(pos.shape, jnp.int32), whole(g), whole(b), one(wq), whole(bq), one(wk), one(wv), whole(bv), pltpu.VMEM((2, 3, width, dim), BF), whole(bo), whole(wc), whole(bc), whole(wco), whole(bco), whole(w1), whole(b1), whole(w2), whole(b2), one(ck), one(cv),
            pltpu.VMEM((parts, prow, dim), BF),
            pltpu.VMEM((parts, prow + 8, width), F32), pltpu.VMEM((parts, prow, width), F32), pltpu.VMEM((parts, prow, width), F32),
            pltpu.VMEM((128, width), F32), pltpu.VMEM((128, width), F32), pltpu.VMEM((parts, prow, width), F32),
            pltpu.VMEM((5, parts, 4, prow, width), BF), pltpu.VMEM((5, parts, prow, dim), BF), pltpu.VMEM((5, parts, 3, prow, dim), BF), pltpu.VMEM((3, width, dim), BF),
            DMA((12,)), DMA((4, 8)), DMA((2, 2)), DMA((2, 2)), DMA((5,)), DMA((5,)), DMA((audios,)), DMA((audios,)), DMA((audios,)), DMA((audios,)), DMA((5, parts, 3)), DMA((5, parts, 3)),
        ],
        compiler_params=pltpu.CompilerParams(collective_id=0, has_side_effects=True, vmem_limit_bytes=REST_LIMIT),
        name="rest",
    )(*args)


def write_kernel(layer, beams, spot, kt, vt, sk_in, sv_in, ki_hbm, vi_hbm, ko_hbm, vo_hbm, sk, sv, kosem, vosem):
    rows, width, slots = sk.shape
    audios = rows // beams

    def k_out(a):
        r = pl.ds(a * beams, beams)
        return pltpu.make_async_copy(sk.at[r], ko_hbm.at[layer, r], kosem.at[a])

    def v_out(a):
        r = pl.ds(a * beams, beams)
        return pltpu.make_async_copy(sv.at[r], vo_hbm.at[layer, r], vosem.at[a])

    @pl.loop(0, audios)
    def _(a):
        hits = [iota((width, min(128, slots - t)), 1) + t == spot[a, 0:1, :min(128, slots - t)] for t in range(0, slots, 128)]
        for buf, cols, out in ((sk, kt, k_out), (sv, vt, v_out)):
            for i in range(beams):
                r = a * beams + i
                col = jnp.take_along_axis(cols[...], jnp.full((width, 128), r, jnp.int32), axis=1).astype(BF)
                for n, hit in enumerate(hits):
                    size = hit.shape[1]
                    span = (r, slice(None), slice(n * 128, n * 128 + size))
                    buf[span] = jnp.where(hit, col[:, :size], buf[span])
            out(a).start()

    @pl.loop(0, audios)
    def _(a):
        k_out(a).wait()
        v_out(a).wait()


def write_call(layer, beams, spot, kt, vt, sk, sv, ko, vo):
    audios = sk.shape[0] // beams
    return pl.pallas_call(
        functools.partial(write_kernel, layer, beams),
        out_shape=(jax.ShapeDtypeStruct(ko.shape, BF), jax.ShapeDtypeStruct(vo.shape, BF), pltpu.VMEM(sk.shape, BF), pltpu.VMEM(sv.shape, BF)),
        in_specs=[VM, VM, VM, VM, VM, ANY, ANY],
        out_specs=(ANY, ANY, VM, VM),
        input_output_aliases={3: 2, 4: 3, 5: 0, 6: 1},
        cost_estimate=pl.CostEstimate(flops=0, bytes_accessed=4 * sk.size, transcendentals=0),
        scratch_shapes=[DMA((audios,)), DMA((audios,))],
        compiler_params=pltpu.CompilerParams(vmem_limit_bytes=4 * 1024 * 1024),
        name="write",
    )(spot, kt, vt, sk, sv, ko, vo)[:2]


def solution(mesh):
    cache_spec = P(None, 'dp', None, 'tp', None)
    col_spec = P(None, None, 'tp')
    row_spec = P(None, 'tp', None)
    vec_spec = P(None, 'tp')
    in_specs = (P('dp', None), P('dp'), cache_spec, cache_spec, cache_spec, cache_spec,
                P(), P(), col_spec, vec_spec, col_spec, col_spec, vec_spec, row_spec, P(), col_spec, vec_spec, row_spec, P(), col_spec, vec_spec, row_spec, P())

    def heads_first(cache):
        cache = jnp.transpose(cache, (0, 1, 3, 4, 2))
        return cache.reshape(cache.shape[:2] + (-1, cache.shape[-1]))

    def heads_last(cache, like):
        layers, batch, slots, heads, dim = like.shape
        return jnp.transpose(cache.reshape(layers, batch, heads, dim, slots), (0, 1, 4, 2, 3))

    def local_step(hidden, positions, self_keys, self_vals, cross_keys, cross_vals, g, b, wq, bq, wk, wv, bv, wo, bo, wc, bc, wco, bco, w1, b1, w2, b2):
        beams = hidden.shape[0] // cross_keys.shape[1]
        sk, sv, ck, cv = (heads_first(x) for x in (self_keys, self_vals, cross_keys, cross_vals))
        wq, wk, wv, wc = (jnp.swapaxes(w, 1, 2) for w in (wq, wk, wv, wc))
        g, b = (jnp.swapaxes(x, 0, 1) for x in (g, b))
        def hop(x, flip):
            return lax.ppermute(x, 'tp', [(i, i ^ flip) for i in range(4)])

        parts = 2
        wo_far = pltpu.with_memory_space_constraint(hop(wo, 2), pltpu.VMEM)
        o, ko, vo = self_call(0, beams, parts, hidden, positions, g, b, wq, wk, wv, bq, bv, sk, sv)
        part, hidden, sk1, sv1, kt, vt, spot = rest_call(beams, parts, o, hidden, positions, g, b, wq, bq, wk, wv, bv, wo, bo, wc, bc, wco, bco, w1, b1, w2, b2, wo_far, sk, sv, ck, cv)
        ko, vo = write_call(1, beams, spot, kt, vt, sk1, sv1, ko, vo)
        here, mate, far, diag = (x.astype(F32) for x in (part, hop(part, 1), hop(part, 2), hop(part, 3)))
        hidden = (hidden.astype(F32) + ((here + mate) + (far + diag)) + b2[1].astype(F32)).astype(BF)
        return hidden, heads_last(ko, self_keys), heads_last(vo, self_vals)

    return jax.shard_map(local_step, mesh=mesh, in_specs=in_specs, out_specs=(P('dp', None), cache_spec, cache_spec), check_vma=False)
```

```python
import functools

import jax
import jax.numpy as jnp
from jax import lax
from jax.experimental import pallas as pl
from jax.experimental.pallas import tpu as pltpu
from jax.sharding import PartitionSpec as P

EPS = 1e-5
BF = jnp.bfloat16
F32 = jnp.float32
MESH = pl.DeviceIdType.MESH
ANY = pl.BlockSpec(memory_space=pl.ANY)
VM = pl.BlockSpec(memory_space=pltpu.VMEM)
SMEM = pl.BlockSpec(memory_space=pltpu.SMEM)
DMA = pltpu.SemaphoreType.DMA
NT = (((1,), (1,)), ((), ()))
VMEM_LIMIT = 60 * 1024 * 1024
REST_LIMIT = 38 * 1024 * 1024


def layer_norm(wide, gain_row, bias_row):
    center = wide - jnp.mean(wide, axis=-1, keepdims=True)
    var_est = jnp.mean(center * center, axis=-1, keepdims=True)
    return (center * lax.rsqrt(var_est + EPS) * gain_row.astype(F32) + bias_row.astype(F32)).astype(BF)


def dot(a, b):
    return jnp.dot(a, b, preferred_element_type=F32)


def dot_nt(a, b):
    return lax.dot_general(a, b, NT, preferred_element_type=F32)


def iota(shape, dim):
    return lax.broadcasted_iota(jnp.int32, shape, dim)


def insert_slot(places, row, beams, pos, slots):
    last = (slots // 128) * 128
    tile = pos // 128

    def insert(start, size):
        for buf, cols in places:
            width = cols.shape[0]
            hit = iota((width, size), 1) == pos - start
            for i in range(beams):
                col = jnp.take_along_axis(cols[...], jnp.full((width, 128), row + i, jnp.int32), axis=1)[:, :size]
                span = (row + i, slice(None), pl.ds(start, size))
                buf[span] = jnp.where(hit, col.astype(BF), buf[span])

    @pl.when(tile * 128 < last)
    def _():
        insert(pl.multiple_of(tile * 128, 128), 128)

    if slots > last:
        @pl.when(tile * 128 >= last)
        def _():
            insert(last, slots - last)


def as_columns(rows):
    pad = jnp.zeros((128 - rows.shape[0], rows.shape[1]), F32)
    return jnp.concatenate([rows, pad], axis=0).T


def copies(pairs, sem):
    return [pltpu.make_async_copy(s, d, sem.at[i]) for i, (s, d) in enumerate(pairs)]


def self_kernel(layer, beams, parts, h_hbm, pos_hbm, g_hbm, b_hbm, wq_hbm, wk_hbm, wv_hbm, bq_hbm, bv_hbm, k_hbm, v_hbm, o_hbm, ko_hbm, vo_hbm,
                h, pos_ref, g, b, wq, wk, wv, bq, bv, kbuf, vbuf, qs, kt, vt, os, o, psem, ksem, vsem, kosem, vosem):
    rows = h.shape[0]
    audios = rows // beams
    slots = kbuf.shape[-1]
    scale = 64 ** -0.25

    small = copies([(h_hbm, h), (g_hbm, g), (b_hbm, b), (wq_hbm.at[layer], wq), (wk_hbm.at[layer], wk), (wv_hbm.at[layer], wv), (bq_hbm, bq), (bv_hbm, bv), (pos_hbm, pos_ref)], psem)
    for c in small:
        c.start()

    def block(a, src, dst, sem):
        return pltpu.make_async_copy(src, dst, sem.at[a])

    def at(a):
        return pl.ds(a * beams, beams)

    def k_in(a):
        return block(a, k_hbm.at[layer, at(a)], kbuf.at[at(a)], ksem)

    def v_in(a):
        return block(a, v_hbm.at[layer, at(a)], vbuf.at[at(a)], vsem)

    def k_out(a):
        return block(a, kbuf.at[at(a)], ko_hbm.at[layer, at(a)], kosem)

    def v_out(a):
        return block(a, vbuf.at[at(a)], vo_hbm.at[layer, at(a)], vosem)

    @pl.loop(0, audios)
    def _(a):
        k_in(a).start()
        v_in(a).start()

    for c in small:
        c.wait()
    normed = layer_norm(h[...].astype(F32), g[0, layer:layer + 1, :], b[0, layer:layer + 1, :])
    qs[...] = ((dot_nt(normed, wq[...]) + bq[layer:layer + 1, :].astype(F32)) * scale).astype(BF).astype(F32)
    kt[...] = as_columns((dot_nt(normed, wk[...]) * scale).astype(BF).astype(F32))
    vt[...] = as_columns((dot_nt(normed, wv[...]) + bv[layer:layer + 1, :].astype(F32)).astype(BF).astype(F32))
    own = iota((8, qs.shape[1]), 1) // 64 == iota((8, qs.shape[1]), 0)
    pairs = audios // 2
    hold = pairs // 2

    def release(pair):
        for a in (pair * 2, pair * 2 + 1):
            k_out(a).start()
            v_out(a).start()

    @pl.loop(0, pairs)
    def _(pair):
        group = (pair * 2, pair * 2 + 1)
        @pl.when(pair >= hold)
        def _():
            release(pair - hold)

        for a in group:
            k_in(a).wait()
            v_in(a).wait()
        for a in group:
            insert_slot(((kbuf, kt), (vbuf, vt)), a * beams, beams, pos_ref[a * beams], slots)

        probs = []
        for a in group:
            scores = []
            for i in range(beams):
                q = jnp.broadcast_to(qs[pl.ds(a * beams + i, 1), :], own.shape)
                scores.append(dot(jnp.where(own, q, 0.0).astype(BF), kbuf[a * beams + i]))
            scores = jnp.concatenate(scores, axis=0)
            scores = jnp.where(iota(scores.shape, 1) <= pos_ref[a * beams], scores, -1e30)
            e = jnp.exp(scores - jnp.max(scores, axis=-1, keepdims=True))
            probs.append(e * (1.0 / jnp.sum(e, axis=-1, keepdims=True)))
        for a, p in zip(group, probs):
            for i in range(beams):
                r = a * beams + i
                out = dot_nt(p[i * 8:i * 8 + 8].astype(BF), vbuf[r])
                os[pl.ds(r, 1), :] = jnp.sum(jnp.where(own, out, 0.0), axis=0, keepdims=True)

    @pl.loop(pairs - hold, pairs)
    def _(pair):
        release(pair)

    for m in range(parts):
        o[m] = os[m * rows // parts:(m + 1) * rows // parts, :].astype(BF)
    last = pltpu.make_async_copy(o, o_hbm, psem.at[0])
    last.start()

    @pl.loop(0, audios)
    def _(a):
        k_out(a).wait()
        v_out(a).wait()

    last.wait()


def self_call(layer, beams, parts, h, pos, g, b, wq, wk, wv, bq, bv, k, v):
    rows = h.shape[0]
    audios = rows // beams
    _, _, width, slots = k.shape
    args = (h, pos, g, b, wq, wk, wv, bq, bv, k, v)
    return pl.pallas_call(
        functools.partial(self_kernel, layer, beams, parts),
        out_shape=(jax.ShapeDtypeStruct((parts, rows // parts, width), BF), jax.ShapeDtypeStruct(k.shape, BF), jax.ShapeDtypeStruct(v.shape, BF)),
        in_specs=[ANY] * 11,
        out_specs=(ANY, ANY, ANY),
        scratch_shapes=[
            pltpu.VMEM(h.shape, BF), pltpu.SMEM(pos.shape, jnp.int32), pltpu.VMEM(g.shape, BF), pltpu.VMEM(b.shape, BF),
            pltpu.VMEM(wq.shape[1:], BF), pltpu.VMEM(wk.shape[1:], BF), pltpu.VMEM(wv.shape[1:], BF),
            pltpu.VMEM(bq.shape, BF), pltpu.VMEM(bv.shape, BF),
            pltpu.VMEM((rows, width, slots), BF), pltpu.VMEM((rows, width, slots), BF),
            pltpu.VMEM((rows, width), F32), pltpu.VMEM((width, 128), F32), pltpu.VMEM((width, 128), F32), pltpu.VMEM((rows, width), F32), pltpu.VMEM((parts, rows // parts, width), BF),
            DMA((9,)), DMA((audios,)), DMA((audios,)), DMA((audios,)), DMA((audios,)),
        ],
        cost_estimate=pl.CostEstimate(flops=0, bytes_accessed=4 * k.size, transcendentals=0),
        compiler_params=pltpu.CompilerParams(vmem_limit_bytes=VMEM_LIMIT),
        name=f"self_{layer}",
    )(*args)


def rest_kernel(beams, parts, o_hbm, h_hbm, pos_hbm, g_hbm, b_hbm, wq_hbm, bq_hbm, wk_hbm, wv_hbm, bv_hbm, wo_hbm, bo_hbm, wc_hbm, bc_hbm, wco_hbm, bco_hbm, w1_hbm, b1_hbm, w2_hbm, b2_hbm,
                wo_far, sk_hbm, sv_hbm, ck_hbm, cv_hbm, part_ref, out_ref, sk, sv, kt, vt, spot,
                o, h, pos_ref, g, b, wq, bq, wk, wv, bv, wo, bo, wc, bc, wco, bco, w1, b1, w2, b2, ck, cv, hid, qr, kr, vr, kall, vall, os, got, snd, rcv, wcx,
                psem, wsem, msem, mrsem, xsem, xrsem, skem, svem, ckem, cvem, ssem, rsem):
    rows = h.shape[0]
    audios = rows // beams
    group = audios // parts
    prow = rows // parts
    width = o.shape[-1]
    heads = width // 64
    scale = 64 ** -0.25
    dp = lax.axis_index('dp')
    me = lax.axis_index('tp')
    mate = me + 1 - 2 * (me % 2)
    peers = ((me + 2) % 4, (mate + 2) % 4, mate)

    small = copies([(o_hbm, o), (h_hbm, h), (g_hbm, g), (b_hbm, b), (bq_hbm, bq), (bv_hbm, bv), (bo_hbm, bo), (bc_hbm, bc), (bco_hbm, bco), (b1_hbm, b1), (b2_hbm, b2), (pos_hbm, pos_ref)], psem)
    def layer_copies(layer, arrays, sem):
        return copies([(x.at[layer], y.at[layer]) for x, y in arrays], sem)

    first = layer_copies(0, ((wc_hbm, wc), (wco_hbm, wco), (w1_hbm, w1), (w2_hbm, w2)), wsem.at[1])
    second = layer_copies(1, ((wc_hbm, wc), (wco_hbm, wco), (w1_hbm, w1), (w2_hbm, w2)), wsem.at[2])
    early = copies([(wo_hbm.at[i], wo.at[i, 0]) for i in range(2)], wsem.at[0])

    def shared(layer):
        return [pltpu.make_async_remote_copy(src.at[layer], wo.at[layer, 1 + j], msem.at[layer, j], mrsem.at[layer, j], device_id=(dp, mate), device_id_type=MESH) for j, src in enumerate((wo_hbm, wo_far))]

    extra = copies([(x.at[1], y) for x, y in ((wq_hbm, wq), (wk_hbm, wk), (wv_hbm, wv))], wsem.at[3])

    def cross_in(layer, a):
        return pltpu.make_async_copy(ck_hbm.at[layer, a], ck.at[a], ckem.at[a]), pltpu.make_async_copy(cv_hbm.at[layer, a], cv.at[a], cvem.at[a])

    def self_in(a):
        r = pl.ds(a * beams, beams)
        return pltpu.make_async_copy(sk_hbm.at[1, r], sk.at[r], skem.at[a]), pltpu.make_async_copy(sv_hbm.at[1, r], sv.at[r], svem.at[a])

    def start(pair):
        for c in pair:
            c.start()

    def wait(pair):
        for c in pair:
            c.wait()

    start(small)
    start(early)
    barrier = pltpu.get_barrier_semaphore()
    for peer in peers:
        pl.semaphore_signal(barrier, inc=1, device_id=(dp, peer), device_id_type=MESH)

    def sends(step, m):
        return [pltpu.make_async_remote_copy(snd.at[step, m], rcv.at[step, m, j], ssem.at[step, m, j], rsem.at[step, m, j], device_id=(dp, peer), device_id_type=MESH) for j, peer in enumerate(peers)]

    def push(step, m, part):
        snd[step, m] = part.astype(BF)
        start(sends(step, m))

    def total(step, m):
        wait(sends(step, m))
        mine = snd[step, m].astype(F32) + rcv[step, m, 2].astype(F32)
        return mine + (rcv[step, m, 0].astype(F32) + rcv[step, m, 1].astype(F32))

    def heads_sends(step, m):
        return [pltpu.make_async_remote_copy(got.at[step, m, 3], got.at[step, m, j], ssem.at[step, m, j], rsem.at[step, m, j], device_id=(dp, peer), device_id_type=MESH) for j, peer in enumerate(peers)]

    def push_heads(step, m, out):
        got[step, m, 3] = out
        start(heads_sends(step, m))

    def project(step, m, layer):
        wait(heads_sends(step, m))
        here = dot(got[step, m, 3], wo[layer, 0]) + dot(got[step, m, 2], wo[layer, 1])
        return here + (dot(got[step, m, 0], wo_far[layer]) + dot(got[step, m, 1], wo[layer, 2]))

    band = width // 2

    def over_link(i):
        r = pl.ds(i * band, band)
        return pltpu.make_async_remote_copy(wco_hbm.at[1, r], wcx.at[0, r], xsem.at[i], xrsem.at[i], device_id=(dp, peers[0]), device_id_type=MESH)

    def to_mate(i):
        if i == 2:
            return pltpu.make_async_remote_copy(wco_hbm.at[1], wcx.at[1], xsem.at[4], xrsem.at[4], device_id=(dp, mate), device_id_type=MESH)
        r = pl.ds(i * band, band)
        return pltpu.make_async_remote_copy(wcx.at[0, r], wcx.at[2, r], xsem.at[2 + i], xrsem.at[2 + i], device_id=(dp, mate), device_id_type=MESH)

    def project_cross(m):
        wait(heads_sends(4, m))
        here = dot(got[4, m, 3], wco[1]) + dot(got[4, m, 2], wcx[1])
        return here + (dot(got[4, m, 0], wcx[0]) + dot(got[4, m, 1], wcx[2]))

    def settle(m, update, bias):
        new = (hid[m].astype(F32) + update + bias.astype(F32)).astype(BF)
        hid[m] = new
        return new.astype(F32)

    def flags(shape, rule):
        return rule(iota(shape, 0), iota(shape, 1)).astype(F32).astype(BF)

    def pick(m):
        return flags((prow, rows), lambda r, c: c == r + m * prow)

    def cross_half(layer, m, wide):
        normed = layer_norm(wide, g[1, layer:layer + 1, :], b[1, layer:layer + 1, :])
        q = ((dot_nt(normed, wc[layer]) + bc[layer:layer + 1, :].astype(F32)) * scale).astype(BF)
        qr[m, 0:prow, :] = q.astype(F32)

        @pl.loop(0, group)
        def _(n):
            wait(cross_in(layer, m * group + n))

        if layer == 0:
            @pl.loop(0, group)
            def _(n):
                start(self_in(m * group + n))

            start(first[2:] if m == 0 else extra if m == 1 else [])

        own = iota((heads * 8, width), 1) // 64 == iota((heads * 8, width), 0) // 8

        def probs_of(n):
            qa = jnp.concatenate([qr[m, n * beams:n * beams + 8, :]] * heads, axis=0)
            scores = dot(jnp.where(own, qa, 0.0).astype(BF), ck[m * group + n])
            e = jnp.exp(scores - jnp.max(scores, axis=-1, keepdims=True))
            return (e * (1.0 / jnp.sum(e, axis=-1, keepdims=True))).astype(BF)

        def mix(n, p):
            out = jnp.where(own, dot_nt(p, cv[m * group + n]), 0.0)
            acc = out[0:8]
            for j in range(1, heads):
                acc = acc + out[j * 8:j * 8 + 8]
            os[m, n * beams:(n + 1) * beams, :] = acc[0:beams]

        probs = [probs_of(n) for n in range(group)]
        for n in range(group):
            mix(n, probs[n])

        return os[m].astype(BF)

    def mlp_half(layer, m, wide):
        normed = layer_norm(wide, g[2, layer:layer + 1, :], b[2, layer:layer + 1, :])
        inner = dot(normed, w1[layer]) + b1[layer:layer + 1, :].astype(F32)
        inner = (0.5 * inner * (1.0 + lax.erf(inner * (2.0 ** -0.5)))).astype(BF)
        return dot(inner, w2[layer])

    def self_half(m, wide):
        normed = layer_norm(wide, g[0, 1:1 + 1, :], b[0, 1:1 + 1, :])
        q = ((dot_nt(normed, wq[...]) + bq[1:2, :].astype(F32)) * scale).astype(BF)
        k = (dot_nt(normed, wk[...]) * scale).astype(BF)
        v = (dot_nt(normed, wv[...]) + bv[1:2, :].astype(F32)).astype(BF)
        kall[m * prow:(m + 1) * prow, :] = k.astype(F32)
        vall[m * prow:(m + 1) * prow, :] = v.astype(F32)
        qr[m, 0:prow, :] = q.astype(F32)
        kr[m] = k.astype(F32)
        vr[m] = v.astype(F32)
        own = iota((8, width), 1) // 64 == iota((8, width), 0)

        @pl.loop(0, group)
        def _(n):
            wait(self_in(m * group + n))

        if m == 0:
            start(second)

        @pl.loop(0, group)
        def _(n):
            start(cross_in(1, m * group + n))

        def row(ref, r):
            return jnp.where(own, jnp.broadcast_to(ref[m, r:r + 1, :], own.shape), 0.0)

        def probs_of(n):
            pos = pos_ref[(m * group + n) * beams]
            scores, fresh = [], []
            for j in range(beams):
                r = n * beams + j
                q8 = row(qr, r)
                scores.append(dot(q8.astype(BF), sk[m * prow + r]))
                fresh.append(jnp.sum(q8 * row(kr, r), axis=-1, keepdims=True))
            scores = jnp.concatenate(scores, axis=0)
            fresh = jnp.concatenate(fresh, axis=0)
            old = iota(scores.shape, 1) < pos
            scores = jnp.where(old, scores, -1e30)
            top = jnp.maximum(jnp.max(scores, axis=-1, keepdims=True), fresh)
            e = jnp.where(old, jnp.exp(scores - top), 0.0)
            e_new = jnp.exp(fresh - top)
            inv = 1.0 / (jnp.sum(e, axis=-1, keepdims=True) + e_new)
            return (e * inv), (e_new * inv).astype(BF).astype(F32)

        def mix(n, p, p_new):
            for j in range(beams):
                r = n * beams + j
                out = dot_nt(p[j * 8:j * 8 + 8].astype(BF), sv[m * prow + r])
                out = jnp.where(own, out, 0.0) + p_new[j * 8:j * 8 + 8] * row(vr, r)
                os[m, r:r + 1, :] = jnp.sum(out, axis=0, keepdims=True)

        probs = [probs_of(n) for n in range(group)]
        for n in range(group):
            mix(n, *probs[n])

        return os[m].astype(BF)

    wait(small)
    pl.semaphore_wait(barrier, 3)
    for m in range(parts):
        push_heads(0, m, o[m])
    start(shared(0))
    start(first[:2])

    @pl.loop(0, audios)
    def _(a):
        start(cross_in(0, a))

    start(shared(1))

    for m in range(parts):
        hid[m] = dot(pick(m), h[...]).astype(BF)
        qr[m, prow:, :] = jnp.zeros((qr.shape[1] - prow, width), F32)
    kall[rows:, :] = jnp.zeros((128 - rows, width), F32)
    vall[rows:, :] = jnp.zeros((128 - rows, width), F32)
    wait(early)
    wait(shared(0))
    wait(first[:2])
    for m in range(parts):
        push(1, m, dot(cross_half(0, m, settle(m, project(0, m, 0), bo[0:1, :])), wco[0]))
    wait(first[2:])
    for m in range(parts):
        push(2, m, mlp_half(0, m, settle(m, total(1, m), bco[0:1, :])))
    wait(extra)
    for m in range(parts):
        wide = settle(m, total(2, m), b2[0:1, :])
        if m == 0:
            over_link(0).start()
            to_mate(2).start()
        push_heads(3, m, self_half(m, wide))
        if m == 0:
            over_link(1).start()
    kt[...] = kall[...].T
    vt[...] = vall[...].T
    for a in range(audios):
        spot[a] = jnp.full(spot.shape[1:], pos_ref[a * beams], jnp.int32)
    wait(second)
    wait(shared(1))
    for m in range(parts):
        wide = settle(m, project(3, m, 1), bo[1:2, :])
        if m < 2:
            over_link(m).wait()
            to_mate(m).start()
        push_heads(4, m, cross_half(1, m, wide))
    wait([to_mate(i) for i in range(3)])
    final = jnp.zeros((rows, h.shape[1]), F32)
    resid = jnp.zeros((rows, h.shape[1]), F32)
    for m in range(parts):
        place = flags((rows, prow), lambda r, c: r == c + m * prow)
        wide = settle(m, project_cross(m), bco[1:2, :])
        final = final + dot(place, mlp_half(1, m, wide).astype(BF))
        resid = resid + dot(place, hid[m])
    part_ref[...] = final.astype(BF)
    out_ref[...] = resid.astype(BF)


def rest_call(beams, parts, o, h, pos, g, b, wq, bq, wk, wv, bv, wo, bo, wc, bc, wco, bco, w1, b1, w2, b2, wo_far, sk, sv, ck, cv):
    rows, dim = h.shape
    _, audios, width, frames = ck.shape
    slots = sk.shape[-1]
    prow = rows // parts
    args = (o, h, pos, g, b, wq, bq, wk, wv, bv, wo, bo, wc, bc, wco, bco, w1, b1, w2, b2, wo_far, sk, sv, ck, cv)

    def whole(x):
        return pltpu.VMEM(x.shape, BF)

    def one(x):
        return pltpu.VMEM(x.shape[1:], BF)

    return pl.pallas_call(
        functools.partial(rest_kernel, beams, parts),
        out_shape=(pltpu.VMEM(h.shape, BF), pltpu.VMEM(h.shape, BF), pltpu.VMEM((rows, width, slots), BF), pltpu.VMEM((rows, width, slots), BF), pltpu.VMEM((width, 128), F32), pltpu.VMEM((width, 128), F32), pltpu.VMEM((audios, 8, 128), jnp.int32)),
        in_specs=[ANY] * (len(args) - 5) + [VM] + [ANY] * 4,
        out_specs=(VM,) * 7,
        scratch_shapes=[
            whole(o), whole(h), pltpu.SMEM(pos.shape, jnp.int32), whole(g), whole(b), one(wq), whole(bq), one(wk), one(wv), whole(bv), pltpu.VMEM((2, 3, width, dim), BF), whole(bo), whole(wc), whole(bc), whole(wco), whole(bco), whole(w1), whole(b1), whole(w2), whole(b2), one(ck), one(cv),
            pltpu.VMEM((parts, prow, dim), BF),
            pltpu.VMEM((parts, prow + 8, width), F32), pltpu.VMEM((parts, prow, width), F32), pltpu.VMEM((parts, prow, width), F32),
            pltpu.VMEM((128, width), F32), pltpu.VMEM((128, width), F32), pltpu.VMEM((parts, prow, width), F32),
            pltpu.VMEM((5, parts, 4, prow, width), BF), pltpu.VMEM((5, parts, prow, dim), BF), pltpu.VMEM((5, parts, 3, prow, dim), BF), pltpu.VMEM((3, width, dim), BF),
            DMA((12,)), DMA((4, 8)), DMA((2, 2)), DMA((2, 2)), DMA((5,)), DMA((5,)), DMA((audios,)), DMA((audios,)), DMA((audios,)), DMA((audios,)), DMA((5, parts, 3)), DMA((5, parts, 3)),
        ],
        compiler_params=pltpu.CompilerParams(collective_id=0, has_side_effects=True, vmem_limit_bytes=REST_LIMIT),
        name="rest",
    )(*args)


def write_kernel(layer, beams, spot, kt, vt, sk_in, sv_in, ki_hbm, vi_hbm, ko_hbm, vo_hbm, sk, sv, kosem, vosem):
    rows, width, slots = sk.shape
    audios = rows // beams

    def k_out(a):
        r = pl.ds(a * beams, beams)
        return pltpu.make_async_copy(sk.at[r], ko_hbm.at[layer, r], kosem.at[a])

    def v_out(a):
        r = pl.ds(a * beams, beams)
        return pltpu.make_async_copy(sv.at[r], vo_hbm.at[layer, r], vosem.at[a])

    @pl.loop(0, audios)
    def _(a):
        hits = [iota((width, min(128, slots - t)), 1) + t == spot[a, 0:1, :min(128, slots - t)] for t in range(0, slots, 128)]
        for buf, cols, out in ((sk, kt, k_out), (sv, vt, v_out)):
            for i in range(beams):
                r = a * beams + i
                col = jnp.take_along_axis(cols[...], jnp.full((width, 128), r, jnp.int32), axis=1).astype(BF)
                for n, hit in enumerate(hits):
                    size = hit.shape[1]
                    span = (r, slice(None), slice(n * 128, n * 128 + size))
                    buf[span] = jnp.where(hit, col[:, :size], buf[span])
            out(a).start()

    @pl.loop(0, audios)
    def _(a):
        k_out(a).wait()
        v_out(a).wait()


def write_call(layer, beams, spot, kt, vt, sk, sv, ko, vo):
    audios = sk.shape[0] // beams
    return pl.pallas_call(
        functools.partial(write_kernel, layer, beams),
        out_shape=(jax.ShapeDtypeStruct(ko.shape, BF), jax.ShapeDtypeStruct(vo.shape, BF), pltpu.VMEM(sk.shape, BF), pltpu.VMEM(sv.shape, BF)),
        in_specs=[VM, VM, VM, VM, VM, ANY, ANY],
        out_specs=(ANY, ANY, VM, VM),
        input_output_aliases={3: 2, 4: 3, 5: 0, 6: 1},
        cost_estimate=pl.CostEstimate(flops=0, bytes_accessed=4 * sk.size, transcendentals=0),
        scratch_shapes=[DMA((audios,)), DMA((audios,))],
        compiler_params=pltpu.CompilerParams(vmem_limit_bytes=4 * 1024 * 1024),
        name="write",
    )(spot, kt, vt, sk, sv, ko, vo)[:2]


def solution(mesh):
    cache_spec = P(None, 'dp', None, 'tp', None)
    col_spec = P(None, None, 'tp')
    row_spec = P(None, 'tp', None)
    vec_spec = P(None, 'tp')
    in_specs = (P('dp', None), P('dp'), cache_spec, cache_spec, cache_spec, cache_spec,
                P(), P(), col_spec, vec_spec, col_spec, col_spec, vec_spec, row_spec, P(), col_spec, vec_spec, row_spec, P(), col_spec, vec_spec, row_spec, P())

    def heads_first(cache):
        cache = jnp.transpose(cache, (0, 1, 3, 4, 2))
        return cache.reshape(cache.shape[:2] + (-1, cache.shape[-1]))

    def heads_last(cache, like):
        layers, batch, slots, heads, dim = like.shape
        return jnp.transpose(cache.reshape(layers, batch, heads, dim, slots), (0, 1, 4, 2, 3))

    def local_step(hidden, positions, self_keys, self_vals, cross_keys, cross_vals, g, b, wq, bq, wk, wv, bv, wo, bo, wc, bc, wco, bco, w1, b1, w2, b2):
        beams = hidden.shape[0] // cross_keys.shape[1]
        sk, sv, ck, cv = (heads_first(x) for x in (self_keys, self_vals, cross_keys, cross_vals))
        wq, wk, wv, wc = (jnp.swapaxes(w, 1, 2) for w in (wq, wk, wv, wc))
        g, b = (jnp.swapaxes(x, 0, 1) for x in (g, b))
        def hop(x, flip):
            return lax.ppermute(x, 'tp', [(i, i ^ flip) for i in range(4)])

        parts = 2
        wo_far = pltpu.with_memory_space_constraint(hop(wo, 2), pltpu.VMEM)
        o, ko, vo = self_call(0, beams, parts, hidden, positions, g, b, wq, wk, wv, bq, bv, sk, sv)
        part, hidden, sk1, sv1, kt, vt, spot = rest_call(beams, parts, o, hidden, positions, g, b, wq, bq, wk, wv, bv, wo, bo, wc, bc, wco, bco, w1, b1, w2, b2, wo_far, sk, sv, ck, cv)
        ko, vo = write_call(1, beams, spot, kt, vt, sk1, sv1, ko, vo)
        here, mate, far, diag = (x.astype(F32) for x in (part, hop(part, 1), hop(part, 2), hop(part, 3)))
        hidden = (hidden.astype(F32) + ((here + mate) + (far + diag)) + b2[1].astype(F32)).astype(BF)
        return hidden, heads_last(ko, self_keys), heads_last(vo, self_vals)

    return jax.shard_map(local_step, mesh=mesh, in_specs=in_specs, out_specs=(P('dp', None), cache_spec, cache_spec), check_vma=False)
```

```python
import functools

import jax
import jax.numpy as jnp
from jax import lax
from jax.experimental import pallas as pl
from jax.experimental.pallas import tpu as pltpu
from jax.sharding import PartitionSpec as P

EPS = 1e-5
BF = jnp.bfloat16
F32 = jnp.float32
MESH = pl.DeviceIdType.MESH
ANY = pl.BlockSpec(memory_space=pl.ANY)
VM = pl.BlockSpec(memory_space=pltpu.VMEM)
SMEM = pl.BlockSpec(memory_space=pltpu.SMEM)
DMA = pltpu.SemaphoreType.DMA
NT = (((1,), (1,)), ((), ()))
VMEM_LIMIT = 60 * 1024 * 1024
REST_LIMIT = 38 * 1024 * 1024


def layer_norm(wide, gain_row, bias_row):
    center = wide - jnp.mean(wide, axis=-1, keepdims=True)
    var_est = jnp.mean(center * center, axis=-1, keepdims=True)
    return (center * lax.rsqrt(var_est + EPS) * gain_row.astype(F32) + bias_row.astype(F32)).astype(BF)


def dot(a, b):
    return jnp.dot(a, b, preferred_element_type=F32)


def dot_nt(a, b):
    return lax.dot_general(a, b, NT, preferred_element_type=F32)


def iota(shape, dim):
    return lax.broadcasted_iota(jnp.int32, shape, dim)


def insert_slot(places, row, beams, pos, slots):
    last = (slots // 128) * 128
    tile = pos // 128

    def insert(start, size):
        for buf, cols in places:
            width = cols.shape[0]
            hit = iota((width, size), 1) == pos - start
            for i in range(beams):
                col = jnp.take_along_axis(cols[...], jnp.full((width, 128), row + i, jnp.int32), axis=1)[:, :size]
                span = (row + i, slice(None), pl.ds(start, size))
                buf[span] = jnp.where(hit, col.astype(BF), buf[span])

    @pl.when(tile * 128 < last)
    def _():
        insert(pl.multiple_of(tile * 128, 128), 128)

    if slots > last:
        @pl.when(tile * 128 >= last)
        def _():
            insert(last, slots - last)


def as_columns(rows):
    pad = jnp.zeros((128 - rows.shape[0], rows.shape[1]), F32)
    return jnp.concatenate([rows, pad], axis=0).T


def copies(pairs, sem):
    return [pltpu.make_async_copy(s, d, sem.at[i]) for i, (s, d) in enumerate(pairs)]


def self_kernel(layer, beams, parts, h_hbm, pos_hbm, g_hbm, b_hbm, wq_hbm, wk_hbm, wv_hbm, bq_hbm, bv_hbm, k_hbm, v_hbm, o_hbm, ko_hbm, vo_hbm,
                h, pos_ref, g, b, wq, wk, wv, bq, bv, kbuf, vbuf, qs, kt, vt, os, o, psem, ksem, vsem, kosem, vosem):
    rows = h.shape[0]
    audios = rows // beams
    slots = kbuf.shape[-1]
    scale = 64 ** -0.25

    small = copies([(h_hbm, h), (g_hbm, g), (b_hbm, b), (wq_hbm.at[layer], wq), (wk_hbm.at[layer], wk), (wv_hbm.at[layer], wv), (bq_hbm, bq), (bv_hbm, bv), (pos_hbm, pos_ref)], psem)
    for c in small:
        c.start()

    def block(a, src, dst, sem):
        return pltpu.make_async_copy(src, dst, sem.at[a])

    def at(a):
        return pl.ds(a * beams, beams)

    def k_in(a):
        return block(a, k_hbm.at[layer, at(a)], kbuf.at[at(a)], ksem)

    def v_in(a):
        return block(a, v_hbm.at[layer, at(a)], vbuf.at[at(a)], vsem)

    def k_out(a):
        return block(a, kbuf.at[at(a)], ko_hbm.at[layer, at(a)], kosem)

    def v_out(a):
        return block(a, vbuf.at[at(a)], vo_hbm.at[layer, at(a)], vosem)

    @pl.loop(0, audios)
    def _(a):
        k_in(a).start()
        v_in(a).start()

    for c in small:
        c.wait()
    normed = layer_norm(h[...].astype(F32), g[0, layer:layer + 1, :], b[0, layer:layer + 1, :])
    qs[...] = ((dot_nt(normed, wq[...]) + bq[layer:layer + 1, :].astype(F32)) * scale).astype(BF).astype(F32)
    kt[...] = as_columns((dot_nt(normed, wk[...]) * scale).astype(BF).astype(F32))
    vt[...] = as_columns((dot_nt(normed, wv[...]) + bv[layer:layer + 1, :].astype(F32)).astype(BF).astype(F32))
    own = iota((8, qs.shape[1]), 1) // 64 == iota((8, qs.shape[1]), 0)
    pairs = audios // 2
    hold = pairs // 2

    def release(pair):
        for a in (pair * 2, pair * 2 + 1):
            k_out(a).start()
            v_out(a).start()

    @pl.loop(0, pairs)
    def _(pair):
        group = (pair * 2, pair * 2 + 1)
        @pl.when(pair >= hold)
        def _():
            release(pair - hold)

        for a in group:
            k_in(a).wait()
            v_in(a).wait()
        for a in group:
            insert_slot(((kbuf, kt), (vbuf, vt)), a * beams, beams, pos_ref[a * beams], slots)

        probs = []
        for a in group:
            scores = []
            for i in range(beams):
                q = jnp.broadcast_to(qs[pl.ds(a * beams + i, 1), :], own.shape)
                scores.append(dot(jnp.where(own, q, 0.0).astype(BF), kbuf[a * beams + i]))
            scores = jnp.concatenate(scores, axis=0)
            scores = jnp.where(iota(scores.shape, 1) <= pos_ref[a * beams], scores, -1e30)
            e = jnp.exp(scores - jnp.max(scores, axis=-1, keepdims=True))
            probs.append(e * (1.0 / jnp.sum(e, axis=-1, keepdims=True)))
        for a, p in zip(group, probs):
            for i in range(beams):
                r = a * beams + i
                out = dot_nt(p[i * 8:i * 8 + 8].astype(BF), vbuf[r])
                os[pl.ds(r, 1), :] = jnp.sum(jnp.where(own, out, 0.0), axis=0, keepdims=True)

    @pl.loop(pairs - hold, pairs)
    def _(pair):
        release(pair)

    for m in range(parts):
        o[m] = os[m * rows // parts:(m + 1) * rows // parts, :].astype(BF)
    last = pltpu.make_async_copy(o, o_hbm, psem.at[0])
    last.start()

    @pl.loop(0, audios)
    def _(a):
        k_out(a).wait()
        v_out(a).wait()

    last.wait()


def self_call(layer, beams, parts, h, pos, g, b, wq, wk, wv, bq, bv, k, v):
    rows = h.shape[0]
    audios = rows // beams
    _, _, width, slots = k.shape
    args = (h, pos, g, b, wq, wk, wv, bq, bv, k, v)
    return pl.pallas_call(
        functools.partial(self_kernel, layer, beams, parts),
        out_shape=(jax.ShapeDtypeStruct((parts, rows // parts, width), BF), jax.ShapeDtypeStruct(k.shape, BF), jax.ShapeDtypeStruct(v.shape, BF)),
        in_specs=[ANY] * 11,
        out_specs=(ANY, ANY, ANY),
        scratch_shapes=[
            pltpu.VMEM(h.shape, BF), pltpu.SMEM(pos.shape, jnp.int32), pltpu.VMEM(g.shape, BF), pltpu.VMEM(b.shape, BF),
            pltpu.VMEM(wq.shape[1:], BF), pltpu.VMEM(wk.shape[1:], BF), pltpu.VMEM(wv.shape[1:], BF),
            pltpu.VMEM(bq.shape, BF), pltpu.VMEM(bv.shape, BF),
            pltpu.VMEM((rows, width, slots), BF), pltpu.VMEM((rows, width, slots), BF),
            pltpu.VMEM((rows, width), F32), pltpu.VMEM((width, 128), F32), pltpu.VMEM((width, 128), F32), pltpu.VMEM((rows, width), F32), pltpu.VMEM((parts, rows // parts, width), BF),
            DMA((9,)), DMA((audios,)), DMA((audios,)), DMA((audios,)), DMA((audios,)),
        ],
        cost_estimate=pl.CostEstimate(flops=0, bytes_accessed=4 * k.size, transcendentals=0),
        compiler_params=pltpu.CompilerParams(vmem_limit_bytes=VMEM_LIMIT),
        name=f"self_{layer}",
    )(*args)


def rest_kernel(beams, parts, o_hbm, h_hbm, pos_hbm, g_hbm, b_hbm, wq_hbm, bq_hbm, wk_hbm, wv_hbm, bv_hbm, wo_hbm, bo_hbm, wc_hbm, bc_hbm, wco_hbm, bco_hbm, w1_hbm, b1_hbm, w2_hbm, b2_hbm,
                wo_far, sk_hbm, sv_hbm, ck_hbm, cv_hbm, part_ref, out_ref, sk, sv, kt, vt, spot,
                o, h, pos_ref, g, b, wq, bq, wk, wv, bv, wo, bo, wc, bc, wco, bco, w1, b1, w2, b2, ck, cv, hid, qr, kr, vr, kall, vall, os, got, snd, rcv, wcx,
                psem, wsem, msem, mrsem, xsem, xrsem, skem, svem, ckem, cvem, ssem, rsem):
    rows = h.shape[0]
    audios = rows // beams
    group = audios // parts
    prow = rows // parts
    width = o.shape[-1]
    heads = width // 64
    scale = 64 ** -0.25
    dp = lax.axis_index('dp')
    me = lax.axis_index('tp')
    mate = me + 1 - 2 * (me % 2)
    peers = ((me + 2) % 4, (mate + 2) % 4, mate)

    small = copies([(o_hbm, o), (h_hbm, h), (g_hbm, g), (b_hbm, b), (bq_hbm, bq), (bv_hbm, bv), (bo_hbm, bo), (bc_hbm, bc), (bco_hbm, bco), (b1_hbm, b1), (b2_hbm, b2), (pos_hbm, pos_ref)], psem)
    def layer_copies(layer, arrays, sem):
        return copies([(x.at[layer], y.at[layer]) for x, y in arrays], sem)

    first = layer_copies(0, ((wc_hbm, wc), (wco_hbm, wco), (w1_hbm, w1), (w2_hbm, w2)), wsem.at[1])
    second = layer_copies(1, ((wc_hbm, wc), (wco_hbm, wco), (w1_hbm, w1), (w2_hbm, w2)), wsem.at[2])
    early = copies([(wo_hbm.at[i], wo.at[i, 0]) for i in range(2)], wsem.at[0])

    def shared(layer):
        return [pltpu.make_async_remote_copy(src.at[layer], wo.at[layer, 1 + j], msem.at[layer, j], mrsem.at[layer, j], device_id=(dp, mate), device_id_type=MESH) for j, src in enumerate((wo_hbm, wo_far))]

    extra = copies([(x.at[1], y) for x, y in ((wq_hbm, wq), (wk_hbm, wk), (wv_hbm, wv))], wsem.at[3])

    def cross_in(layer, a):
        return pltpu.make_async_copy(ck_hbm.at[layer, a], ck.at[a], ckem.at[a]), pltpu.make_async_copy(cv_hbm.at[layer, a], cv.at[a], cvem.at[a])

    def self_in(a):
        r = pl.ds(a * beams, beams)
        return pltpu.make_async_copy(sk_hbm.at[1, r], sk.at[r], skem.at[a]), pltpu.make_async_copy(sv_hbm.at[1, r], sv.at[r], svem.at[a])

    def start(pair):
        for c in pair:
            c.start()

    def wait(pair):
        for c in pair:
            c.wait()

    start(small)
    start(early)
    barrier = pltpu.get_barrier_semaphore()
    for peer in peers:
        pl.semaphore_signal(barrier, inc=1, device_id=(dp, peer), device_id_type=MESH)

    def sends(step, m):
        return [pltpu.make_async_remote_copy(snd.at[step, m], rcv.at[step, m, j], ssem.at[step, m, j], rsem.at[step, m, j], device_id=(dp, peer), device_id_type=MESH) for j, peer in enumerate(peers)]

    def push(step, m, part):
        snd[step, m] = part.astype(BF)
        start(sends(step, m))

    def total(step, m):
        wait(sends(step, m))
        mine = snd[step, m].astype(F32) + rcv[step, m, 2].astype(F32)
        return mine + (rcv[step, m, 0].astype(F32) + rcv[step, m, 1].astype(F32))

    def heads_sends(step, m):
        return [pltpu.make_async_remote_copy(got.at[step, m, 3], got.at[step, m, j], ssem.at[step, m, j], rsem.at[step, m, j], device_id=(dp, peer), device_id_type=MESH) for j, peer in enumerate(peers)]

    def push_heads(step, m, out):
        got[step, m, 3] = out
        start(heads_sends(step, m))

    def project(step, m, layer):
        wait(heads_sends(step, m))
        here = dot(got[step, m, 3], wo[layer, 0]) + dot(got[step, m, 2], wo[layer, 1])
        return here + (dot(got[step, m, 0], wo_far[layer]) + dot(got[step, m, 1], wo[layer, 2]))

    band = width // 2

    def over_link(i):
        r = pl.ds(i * band, band)
        return pltpu.make_async_remote_copy(wco_hbm.at[1, r], wcx.at[0, r], xsem.at[i], xrsem.at[i], device_id=(dp, peers[0]), device_id_type=MESH)

    def to_mate(i):
        if i == 2:
            return pltpu.make_async_remote_copy(wco_hbm.at[1], wcx.at[1], xsem.at[4], xrsem.at[4], device_id=(dp, mate), device_id_type=MESH)
        r = pl.ds(i * band, band)
        return pltpu.make_async_remote_copy(wcx.at[0, r], wcx.at[2, r], xsem.at[2 + i], xrsem.at[2 + i], device_id=(dp, mate), device_id_type=MESH)

    def project_cross(m):
        wait(heads_sends(4, m))
        here = dot(got[4, m, 3], wco[1]) + dot(got[4, m, 2], wcx[1])
        return here + (dot(got[4, m, 0], wcx[0]) + dot(got[4, m, 1], wcx[2]))

    def settle(m, update, bias):
        new = (hid[m].astype(F32) + update + bias.astype(F32)).astype(BF)
        hid[m] = new
        return new.astype(F32)

    def flags(shape, rule):
        return rule(iota(shape, 0), iota(shape, 1)).astype(F32).astype(BF)

    def pick(m):
        return flags((prow, rows), lambda r, c: c == r + m * prow)

    def cross_half(layer, m, wide):
        normed = layer_norm(wide, g[1, layer:layer + 1, :], b[1, layer:layer + 1, :])
        q = ((dot_nt(normed, wc[layer]) + bc[layer:layer + 1, :].astype(F32)) * scale).astype(BF)
        qr[m, 0:prow, :] = q.astype(F32)

        @pl.loop(0, group)
        def _(n):
            wait(cross_in(layer, m * group + n))

        if layer == 0:
            @pl.loop(0, group)
            def _(n):
                start(self_in(m * group + n))

            start(first[2:] if m == 0 else extra if m == 1 else [])

        own = iota((heads * 8, width), 1) // 64 == iota((heads * 8, width), 0) // 8

        def probs_of(n):
            qa = jnp.concatenate([qr[m, n * beams:n * beams + 8, :]] * heads, axis=0)
            scores = dot(jnp.where(own, qa, 0.0).astype(BF), ck[m * group + n])
            e = jnp.exp(scores - jnp.max(scores, axis=-1, keepdims=True))
            return (e * (1.0 / jnp.sum(e, axis=-1, keepdims=True))).astype(BF)

        def mix(n, p):
            out = jnp.where(own, dot_nt(p, cv[m * group + n]), 0.0)
            acc = out[0:8]
            for j in range(1, heads):
                acc = acc + out[j * 8:j * 8 + 8]
            os[m, n * beams:(n + 1) * beams, :] = acc[0:beams]

        probs = [probs_of(n) for n in range(group)]
        for n in range(group):
            mix(n, probs[n])

        return os[m].astype(BF)

    def mlp_half(layer, m, wide):
        normed = layer_norm(wide, g[2, layer:layer + 1, :], b[2, layer:layer + 1, :])
        inner = dot(normed, w1[layer]) + b1[layer:layer + 1, :].astype(F32)
        inner = (0.5 * inner * (1.0 + lax.erf(inner * (2.0 ** -0.5)))).astype(BF)
        return dot(inner, w2[layer])

    def self_half(m, wide):
        normed = layer_norm(wide, g[0, 1:1 + 1, :], b[0, 1:1 + 1, :])
        q = ((dot_nt(normed, wq[...]) + bq[1:2, :].astype(F32)) * scale).astype(BF)
        k = (dot_nt(normed, wk[...]) * scale).astype(BF)
        v = (dot_nt(normed, wv[...]) + bv[1:2, :].astype(F32)).astype(BF)
        kall[m * prow:(m + 1) * prow, :] = k.astype(F32)
        vall[m * prow:(m + 1) * prow, :] = v.astype(F32)
        qr[m, 0:prow, :] = q.astype(F32)
        kr[m] = k.astype(F32)
        vr[m] = v.astype(F32)
        own = iota((8, width), 1) // 64 == iota((8, width), 0)

        @pl.loop(0, group)
        def _(n):
            wait(self_in(m * group + n))

        if m == 0:
            start(second)

        @pl.loop(0, group)
        def _(n):
            start(cross_in(1, m * group + n))

        def row(ref, r):
            return jnp.where(own, jnp.broadcast_to(ref[m, r:r + 1, :], own.shape), 0.0)

        def probs_of(n):
            pos = pos_ref[(m * group + n) * beams]
            scores, fresh = [], []
            for j in range(beams):
                r = n * beams + j
                q8 = row(qr, r)
                scores.append(dot(q8.astype(BF), sk[m * prow + r]))
                fresh.append(jnp.sum(q8 * row(kr, r), axis=-1, keepdims=True))
            scores = jnp.concatenate(scores, axis=0)
            fresh = jnp.concatenate(fresh, axis=0)
            old = iota(scores.shape, 1) < pos
            scores = jnp.where(old, scores, -1e30)
            top = jnp.maximum(jnp.max(scores, axis=-1, keepdims=True), fresh)
            e = jnp.where(old, jnp.exp(scores - top), 0.0)
            e_new = jnp.exp(fresh - top)
            inv = 1.0 / (jnp.sum(e, axis=-1, keepdims=True) + e_new)
            return (e * inv), (e_new * inv).astype(BF).astype(F32)

        def mix(n, p, p_new):
            for j in range(beams):
                r = n * beams + j
                out = dot_nt(p[j * 8:j * 8 + 8].astype(BF), sv[m * prow + r])
                out = jnp.where(own, out, 0.0) + p_new[j * 8:j * 8 + 8] * row(vr, r)
                os[m, r:r + 1, :] = jnp.sum(out, axis=0, keepdims=True)

        probs = [probs_of(n) for n in range(group)]
        for n in range(group):
            mix(n, *probs[n])

        return os[m].astype(BF)

    wait(small)
    pl.semaphore_wait(barrier, 3)
    for m in range(parts):
        push_heads(0, m, o[m])
    start(shared(0))
    start(first[:2])

    @pl.loop(0, audios)
    def _(a):
        start(cross_in(0, a))

    start(shared(1))

    for m in range(parts):
        hid[m] = dot(pick(m), h[...]).astype(BF)
        qr[m, prow:, :] = jnp.zeros((qr.shape[1] - prow, width), F32)
    kall[rows:, :] = jnp.zeros((128 - rows, width), F32)
    vall[rows:, :] = jnp.zeros((128 - rows, width), F32)
    wait(early)
    wait(shared(0))
    wait(first[:2])
    for m in range(parts):
        push(1, m, dot(cross_half(0, m, settle(m, project(0, m, 0), bo[0:1, :])), wco[0]))
    wait(first[2:])
    for m in range(parts):
        push(2, m, mlp_half(0, m, settle(m, total(1, m), bco[0:1, :])))
    wait(extra)
    for m in range(parts):
        wide = settle(m, total(2, m), b2[0:1, :])
        if m == 0:
            over_link(0).start()
            to_mate(2).start()
        push_heads(3, m, self_half(m, wide))
        if m == 0:
            over_link(1).start()
    wait(second)
    wait(shared(1))
    for m in range(parts):
        wide = settle(m, project(3, m, 1), bo[1:2, :])
        if m < 2:
            over_link(m).wait()
            to_mate(m).start()
        push_heads(4, m, cross_half(1, m, wide))
    wait([to_mate(i) for i in range(3)])
    final = jnp.zeros((rows, h.shape[1]), F32)
    resid = jnp.zeros((rows, h.shape[1]), F32)
    for m in range(parts):
        place = flags((rows, prow), lambda r, c: r == c + m * prow)
        wide = settle(m, project_cross(m), bco[1:2, :])
        final = final + dot(place, mlp_half(1, m, wide).astype(BF))
        resid = resid + dot(place, hid[m])
        if m == 0:
            kt[...] = kall[...].T
            vt[...] = vall[...].T
            for a in range(audios):
                spot[a] = jnp.full(spot.shape[1:], pos_ref[a * beams], jnp.int32)
    part_ref[...] = final.astype(BF)
    out_ref[...] = resid.astype(BF)


def rest_call(beams, parts, o, h, pos, g, b, wq, bq, wk, wv, bv, wo, bo, wc, bc, wco, bco, w1, b1, w2, b2, wo_far, sk, sv, ck, cv):
    rows, dim = h.shape
    _, audios, width, frames = ck.shape
    slots = sk.shape[-1]
    prow = rows // parts
    args = (o, h, pos, g, b, wq, bq, wk, wv, bv, wo, bo, wc, bc, wco, bco, w1, b1, w2, b2, wo_far, sk, sv, ck, cv)

    def whole(x):
        return pltpu.VMEM(x.shape, BF)

    def one(x):
        return pltpu.VMEM(x.shape[1:], BF)

    return pl.pallas_call(
        functools.partial(rest_kernel, beams, parts),
        out_shape=(pltpu.VMEM(h.shape, BF), pltpu.VMEM(h.shape, BF), pltpu.VMEM((rows, width, slots), BF), pltpu.VMEM((rows, width, slots), BF), pltpu.VMEM((width, 128), F32), pltpu.VMEM((width, 128), F32), pltpu.VMEM((audios, 8, 128), jnp.int32)),
        in_specs=[ANY] * (len(args) - 5) + [VM] + [ANY] * 4,
        out_specs=(VM,) * 7,
        scratch_shapes=[
            whole(o), whole(h), pltpu.SMEM(pos.shape, jnp.int32), whole(g), whole(b), one(wq), whole(bq), one(wk), one(wv), whole(bv), pltpu.VMEM((2, 3, width, dim), BF), whole(bo), whole(wc), whole(bc), whole(wco), whole(bco), whole(w1), whole(b1), whole(w2), whole(b2), one(ck), one(cv),
            pltpu.VMEM((parts, prow, dim), BF),
            pltpu.VMEM((parts, prow + 8, width), F32), pltpu.VMEM((parts, prow, width), F32), pltpu.VMEM((parts, prow, width), F32),
            pltpu.VMEM((128, width), F32), pltpu.VMEM((128, width), F32), pltpu.VMEM((parts, prow, width), F32),
            pltpu.VMEM((5, parts, 4, prow, width), BF), pltpu.VMEM((5, parts, prow, dim), BF), pltpu.VMEM((5, parts, 3, prow, dim), BF), pltpu.VMEM((3, width, dim), BF),
            DMA((12,)), DMA((4, 8)), DMA((2, 2)), DMA((2, 2)), DMA((5,)), DMA((5,)), DMA((audios,)), DMA((audios,)), DMA((audios,)), DMA((audios,)), DMA((5, parts, 3)), DMA((5, parts, 3)),
        ],
        compiler_params=pltpu.CompilerParams(collective_id=0, has_side_effects=True, vmem_limit_bytes=REST_LIMIT),
        name="rest",
    )(*args)


def write_kernel(layer, beams, spot, kt, vt, sk_in, sv_in, ki_hbm, vi_hbm, ko_hbm, vo_hbm, sk, sv, kosem, vosem):
    rows, width, slots = sk.shape
    audios = rows // beams

    def k_out(a):
        r = pl.ds(a * beams, beams)
        return pltpu.make_async_copy(sk.at[r], ko_hbm.at[layer, r], kosem.at[a])

    def v_out(a):
        r = pl.ds(a * beams, beams)
        return pltpu.make_async_copy(sv.at[r], vo_hbm.at[layer, r], vosem.at[a])

    @pl.loop(0, audios)
    def _(a):
        hits = [iota((width, min(128, slots - t)), 1) + t == spot[a, 0:1, :min(128, slots - t)] for t in range(0, slots, 128)]
        for buf, cols, out in ((sk, kt, k_out), (sv, vt, v_out)):
            for i in range(beams):
                r = a * beams + i
                col = jnp.take_along_axis(cols[...], jnp.full((width, 128), r, jnp.int32), axis=1).astype(BF)
                for n, hit in enumerate(hits):
                    size = hit.shape[1]
                    span = (r, slice(None), slice(n * 128, n * 128 + size))
                    buf[span] = jnp.where(hit, col[:, :size], buf[span])
            out(a).start()

    @pl.loop(0, audios)
    def _(a):
        k_out(a).wait()
        v_out(a).wait()


def write_call(layer, beams, spot, kt, vt, sk, sv, ko, vo):
    audios = sk.shape[0] // beams
    return pl.pallas_call(
        functools.partial(write_kernel, layer, beams),
        out_shape=(jax.ShapeDtypeStruct(ko.shape, BF), jax.ShapeDtypeStruct(vo.shape, BF), pltpu.VMEM(sk.shape, BF), pltpu.VMEM(sv.shape, BF)),
        in_specs=[VM, VM, VM, VM, VM, ANY, ANY],
        out_specs=(ANY, ANY, VM, VM),
        input_output_aliases={3: 2, 4: 3, 5: 0, 6: 1},
        cost_estimate=pl.CostEstimate(flops=0, bytes_accessed=4 * sk.size, transcendentals=0),
        scratch_shapes=[DMA((audios,)), DMA((audios,))],
        compiler_params=pltpu.CompilerParams(vmem_limit_bytes=4 * 1024 * 1024),
        name="write",
    )(spot, kt, vt, sk, sv, ko, vo)[:2]


def solution(mesh):
    cache_spec = P(None, 'dp', None, 'tp', None)
    col_spec = P(None, None, 'tp')
    row_spec = P(None, 'tp', None)
    vec_spec = P(None, 'tp')
    in_specs = (P('dp', None), P('dp'), cache_spec, cache_spec, cache_spec, cache_spec,
                P(), P(), col_spec, vec_spec, col_spec, col_spec, vec_spec, row_spec, P(), col_spec, vec_spec, row_spec, P(), col_spec, vec_spec, row_spec, P())

    def heads_first(cache):
        cache = jnp.transpose(cache, (0, 1, 3, 4, 2))
        return cache.reshape(cache.shape[:2] + (-1, cache.shape[-1]))

    def heads_last(cache, like):
        layers, batch, slots, heads, dim = like.shape
        return jnp.transpose(cache.reshape(layers, batch, heads, dim, slots), (0, 1, 4, 2, 3))

    def local_step(hidden, positions, self_keys, self_vals, cross_keys, cross_vals, g, b, wq, bq, wk, wv, bv, wo, bo, wc, bc, wco, bco, w1, b1, w2, b2):
        beams = hidden.shape[0] // cross_keys.shape[1]
        sk, sv, ck, cv = (heads_first(x) for x in (self_keys, self_vals, cross_keys, cross_vals))
        wq, wk, wv, wc = (jnp.swapaxes(w, 1, 2) for w in (wq, wk, wv, wc))
        g, b = (jnp.swapaxes(x, 0, 1) for x in (g, b))
        def hop(x, flip):
            return lax.ppermute(x, 'tp', [(i, i ^ flip) for i in range(4)])

        parts = 2
        wo_far = pltpu.with_memory_space_constraint(hop(wo, 2), pltpu.VMEM)
        o, ko, vo = self_call(0, beams, parts, hidden, positions, g, b, wq, wk, wv, bq, bv, sk, sv)
        part, hidden, sk1, sv1, kt, vt, spot = rest_call(beams, parts, o, hidden, positions, g, b, wq, bq, wk, wv, bv, wo, bo, wc, bc, wco, bco, w1, b1, w2, b2, wo_far, sk, sv, ck, cv)
        ko, vo = write_call(1, beams, spot, kt, vt, sk1, sv1, ko, vo)
        here, mate, far, diag = (x.astype(F32) for x in (part, hop(part, 1), hop(part, 2), hop(part, 3)))
        hidden = (hidden.astype(F32) + ((here + mate) + (far + diag)) + b2[1].astype(F32)).astype(BF)
        return hidden, heads_last(ko, self_keys), heads_last(vo, self_vals)

    return jax.shard_map(local_step, mesh=mesh, in_specs=in_specs, out_specs=(P('dp', None), cache_spec, cache_spec), check_vma=False)
```
